256 devices in a mesh: gx: 32 (over z, y), gy: 8 (over x, core).
Axes of the slice: x: 4, y: 4, z: 8, core: 2. Of those that a mesh axis runs over, the one named last changes fastest.
Arguments:
- populations: float32 [19, 256, 512, 128], P(None, 'gx', 'gy'), may hold values from 0.5 to 2
- solid_flags: int32 [256, 512, 128], P('gx', 'gy'), may hold values 0 or 1
- point_cells: int32 [3, 4608], replicated, may hold values from 0 to 511, as said below
- point_turbine: int32 [4608], replicated, may hold values from 0 to 23, as said below
- blade_speed: float32 [3, 4608], replicated, may hold values from -0.3 to 0.3
- chord: float32 [4608], replicated, may hold values from 0.3 to 3
- turbine_gain: float32 [24], replicated, may hold values from 0.5 to 2
Outputs:
- read: float32 [19, 256, 512, 128], P(None, 'gx', 'gy')
- point_force: float32 [3, 4608], replicated
The draws below stay inside these ranges and needn't reach their ends.
Inputs may be any that keep to these rules, and one draw needn't show every extreme that they name: `point_cells`: row 0 and row 1 are a point's streamwise and spanwise cell, row 2 its height, which lies in [4, 124]; all points of one turbine share the streamwise cell. `point_turbine`: each turbine has exactly 192 points.
All inputs are finite; a program needn't handle non-finite values. No bound on the sum of `solid_flags` on one device may be relied on, other than what follows from the above.
Results may differ from the reference program's by a relative error of at most 0.00007.
Values sent between devices are 32-bit elements; how exact they have to be, the bound alone decides.
No kernel may reach another device: no remote copies, remote signals or barrier semaphores. Data moves between devices by JAX's collectives and lax.ppermute only.
A program may use at most 128 MiB of HBM per device.

```python
import math
import jax
import jax.numpy as jnp
from jax import lax

CX = 8
CY = 64
NZ = 128
TURB = 24
BLADES = 3
BLADE_PTS = 64
SMEAR = 3
POINTS = 4608
NX = 256
NY = 512


def place_points(key):
    base = jax.random.fold_in(key, 11)
    keys = jax.random.split(base, 5)
    hub_x = jax.random.randint(keys[0], (TURB,), 0, NX, dtype=jnp.int32)
    hub_y = jax.random.randint(keys[1], (TURB,), 0, NY, dtype=jnp.int32)
    within_x = jax.random.randint(jax.random.fold_in(base, 21), (2,), 0, CX, dtype=jnp.int32)
    within_y = jax.random.randint(jax.random.fold_in(base, 22), (2,), 0, CY, dtype=jnp.int32)
    hub_x = hub_x.at[0].set(NX // 2 + within_x[0]).at[1].set(within_x[1])
    hub_y = hub_y.at[0].set(within_y[0]).at[1].set(within_y[1])
    owner = jax.random.permutation(keys[2], jnp.repeat(jnp.arange(TURB, dtype=jnp.int32), BLADES * BLADE_PTS))
    reach = NZ // 2 - SMEAR - 1
    off_y = jax.random.randint(keys[3], (POINTS,), -reach, reach + 1, dtype=jnp.int32)
    off_z = jax.random.randint(keys[4], (POINTS,), -reach, reach + 1, dtype=jnp.int32)
    pos_x = hub_x[owner]
    pos_y = (hub_y[owner] + off_y) % NY
    pos_z = NZ // 2 + off_z
    return (jnp.stack([pos_x, pos_y, pos_z], axis=0).astype(jnp.int32), owner.astype(jnp.int32))


def draw_point_cells(key, part):
    return place_points(key)[0]


def draw_point_turbine(key, part):
    return place_points(key)[1]


def set_ends(values, own_key, low, top_value):
    dims = values.shape
    index_at = [jax.random.randint(jax.random.fold_in(own_key, axis), (), 0, dims[axis]) for axis in range(len(dims))]
    values = values.at[tuple(index_at)].set(low)
    longest = dims.index(max(dims))
    index_at[longest] = (index_at[longest] + 1) % dims[longest]
    return values.at[tuple(index_at)].set(top_value)


def block_levels(rng, shape, shards, smallest, top_value):
    loudness = 1.0
    for dim, parts in shards:
        draws = jax.random.uniform(jax.random.fold_in(jax.random.fold_in(rng, 6), dim), (parts,), jnp.float32, smallest / len(shards), top_value / len(shards))
        loudness = loudness * jnp.repeat(jnp.exp(draws), shape[dim] // parts).reshape((-1,) + (1,) * (len(shape) - 1 - dim))
    return loudness


def gaussian(key, extent, scale, most, held_as=jnp.bfloat16):
    return jnp.clip(scale * jax.random.normal(key, extent, jnp.float32), -most, most).astype(held_as)


def setup_inputs(seed: int = 0) -> dict:
    arg_keys = jax.random.split(jax.random.key(seed), 8)
    populations = jnp.clip(jnp.exp(math.log(2.0) - 1.3862944 * jax.random.uniform(arg_keys[0], (19, NX, NY, NZ), jnp.float32) ** block_levels(arg_keys[0], (19, NX, NY, NZ), ((1, 32), (2, 8)), -0.2, 0.2)), 0.5, 2.0)
    solid_flags = set_ends((jax.random.randint(arg_keys[1], (NX, NY, NZ), 0, 16) < 1).astype(jnp.int32), jax.random.fold_in(arg_keys[1], 1), 0, 1)
    point_cells = draw_point_cells(jax.random.fold_in(arg_keys[7], 71), 0)
    point_turbine = draw_point_turbine(jax.random.fold_in(arg_keys[7], 71), 0)
    blade_speed = gaussian(arg_keys[4], (3, POINTS), 0.05, 0.3, jnp.float32)
    chord = jnp.clip(jnp.exp(jax.random.uniform(arg_keys[5], (POINTS,), jnp.float32, math.log(0.3), math.log(3.0))), 0.3, 3.0)
    turbine_gain = jnp.clip(jnp.exp(jax.random.uniform(arg_keys[6], (TURB,), jnp.float32, math.log(0.5), math.log(2.0))), 0.5, 2.0)
    return {"populations": populations, "solid_flags": solid_flags, "point_cells": point_cells, "point_turbine": point_turbine, "blade_speed": blade_speed, "chord": chord, "turbine_gain": turbine_gain}


lattice_dirs = [(0, 0, 0), (1, 0, 0), (-1, 0, 0), (0, 1, 0), (0, -1, 0), (0, 0, 1), (0, 0, -1), (1, 1, 0), (-1, -1, 0), (1, -1, 0), (-1, 1, 0), (1, 0, 1), (-1, 0, -1), (1, 0, -1), (-1, 0, 1), (0, 1, 1), (0, -1, -1), (0, 1, -1), (0, -1, 1)]
opposite_dir = [0, 2, 1, 4, 3, 6, 5, 8, 7, 10, 9, 12, 11, 14, 13, 16, 15, 18, 17]
lattice_wts = [1.0 / 3.0] + [1.0 / 18.0] * 6 + [1.0 / 36.0] * 12
relax_time = 0.8
kernel_scale = 1.5
high = lax.Precision.HIGHEST

def kernel_value(offset):
    dist = offset.astype(jnp.float32)
    return jnp.where(jnp.abs(offset) <= SMEAR, jnp.exp(-(dist / kernel_scale) ** 2), jnp.float32(0.0))

def collide(pops, rho, mom, force, solid_flags):
    cvec = jnp.array(lattice_dirs, jnp.float32).T
    vel = (mom + 0.5 * force) / rho
    cu = jnp.einsum('ci,cxyz->ixyz', cvec, vel, precision=high)
    cf = jnp.einsum('ci,cxyz->ixyz', cvec, force, precision=high)
    usq = lax.optimization_barrier(jnp.sum(vel * vel, axis=0))
    uf = lax.optimization_barrier(jnp.sum(vel * force, axis=0))
    geq = rho * (1.0 + 3.0 * cu + 4.5 * cu * cu - 1.5 * usq)
    source = (1.0 - 0.5 / relax_time) * (3.0 * (cf - uf) + 9.0 * cu * cf)
    post = pops - (pops - geq) / relax_time + source
    bounce = pops[jnp.array(opposite_dir, jnp.int32)]
    return jnp.where(solid_flags[None] != 0, bounce, post)

def reference(populations, solid_flags, point_cells, point_turbine, blade_speed, chord, turbine_gain):
    wts = jnp.array(lattice_wts, jnp.float32)
    cvec = jnp.array(lattice_dirs, jnp.float32).T
    rho = jnp.einsum('i,ixyz->xyz', wts, populations, precision=high)
    mom = jnp.einsum('ci,ixyz->cxyz', cvec * wts[None], populations, precision=high)
    vel_raw = mom / rho[None]
    pos_x, pos_y, pos_z = (point_cells[0], point_cells[1], point_cells[2])
    sampled = vel_raw[:, pos_x, pos_y, pos_z]
    rel = sampled - blade_speed
    coef = chord * turbine_gain[point_turbine]
    speed = jnp.sqrt(lax.optimization_barrier(jnp.sum(rel * rel, axis=0)) + 0.0001)
    point_force = -(coef * speed)[None] * rel
    span = jnp.arange(-SMEAR, SMEAR + 1, dtype=jnp.int32)
    off_x, off_y, off_z = jnp.meshgrid(span, span, span, indexing='ij')
    off_x, off_y, off_z = (off_x.reshape(-1), off_y.reshape(-1), off_z.reshape(-1))
    kern = kernel_value(off_x) * kernel_value(off_y) * kernel_value(off_z)
    cell_x = (pos_x[:, None] + off_x[None]) % NX
    cell_y = (pos_y[:, None] + off_y[None]) % NY
    cell_z = pos_z[:, None] + off_z[None]
    values = point_force[:, :, None] * kern[None, None]
    force = jnp.zeros((3, NX, NY, NZ), jnp.float32).at[:, cell_x, cell_y, cell_z].add(values)
    post = collide(populations, rho[None], mom, force, solid_flags)
    outs = []
    for index in range(19):
        step_x, step_y, step_z = lattice_dirs[index]
        moved = jnp.roll(post[index], (step_x, step_y), axis=(0, 1))
        mirror = post[opposite_dir[index]]
        if step_z == 1:
            moved = jnp.concatenate([mirror[:, :, :1], moved[:, :, :-1]], axis=2)
        elif step_z == -1:
            moved = jnp.concatenate([moved[:, :, 1:], mirror[:, :, -1:]], axis=2)
        outs.append(moved)
    return (jnp.stack(outs, axis=0), point_force)
```

```python
import functools

import jax
import jax.numpy as jnp
from jax import lax
from jax.experimental import pallas as pl
from jax.experimental.pallas import tpu as pltpu
from jax.sharding import PartitionSpec as P

SMEAR = 3
RELAX = 0.8
SCALE = 1.5
CHUNK = 256
LANES = 128
DIRS = [
    (0, 0, 0),
    (1, 0, 0),
    (-1, 0, 0),
    (0, 1, 0),
    (0, -1, 0),
    (0, 0, 1),
    (0, 0, -1),
    (1, 1, 0),
    (-1, -1, 0),
    (1, -1, 0),
    (-1, 1, 0),
    (1, 0, 1),
    (-1, 0, -1),
    (1, 0, -1),
    (-1, 0, 1),
    (0, 1, 1),
    (0, -1, -1),
    (0, 1, -1),
    (0, -1, 1),
]
OPP = [0, 2, 1, 4, 3, 6, 5, 8, 7, 10, 9, 12, 11, 14, 13, 16, 15, 18, 17]
EAST = [i for i in range(19) if DIRS[i][0] == 1]
WEST = [i for i in range(19) if DIRS[i][0] == -1]
NORTH = [i for i in range(19) if DIRS[i][1] == 1]
SOUTH = [i for i in range(19) if DIRS[i][1] == -1]
CX, CY = 8, 64
F32, BF16 = jnp.float32, jnp.bfloat16
ANY = pl.BlockSpec(memory_space=pl.ANY)
SMEM = pl.BlockSpec(memory_space=pltpu.SMEM)
VMEM = pl.BlockSpec(memory_space=pltpu.VMEM)
NT = (((1,), (1,)), ((), ()))
NN = (((1,), (0,)), ((), ()))


def dot(a, b, dims=NN):
    return lax.dot_general(a, b, dims, preferred_element_type=F32)


def split3(v):
    high = v.astype(BF16)
    rest = v - high.astype(F32)
    mid = rest.astype(BF16)
    low = (rest - mid.astype(F32)).astype(BF16)
    return high, mid, low


def moments(g):
    s = [None] * 19
    d = [None] * 19
    for k in range(1, 19, 2):
        s[k] = g[k] + g[k + 1]
        d[k] = g[k] - g[k + 1]
    w1, w2 = 1.0 / 18.0, 1.0 / 36.0
    rho = (
        g[0] * (1.0 / 3.0)
        + (s[1] + s[3] + s[5]) * w1
        + ((s[7] + s[9]) + (s[11] + s[13]) + (s[15] + s[17])) * w2
    )
    mx = d[1] * w1 + ((d[7] + d[9]) + (d[11] + d[13])) * w2
    my = d[3] * w1 + ((d[7] - d[9]) + (d[15] + d[17])) * w2
    mz = d[5] * w1 + ((d[11] - d[13]) + (d[15] - d[17])) * w2
    return rho, (mx, my, mz)


def along(c, v):
    total = None
    for comp, part in zip(c, v):
        if comp == 0:
            continue
        if total is None:
            total = part if comp > 0 else -part
        else:
            total = total + part if comp > 0 else total - part
    return total


class Collision:
    def __init__(self, rho, mom, force):
        inv = 1.0 / rho
        amp = 1.0 - 0.5 / RELAX
        vel = [(m + 0.5 * f) * inv for m, f in zip(mom, force)]
        usq = vel[0] * vel[0] + vel[1] * vel[1] + vel[2] * vel[2]
        uf = vel[0] * force[0] + vel[1] * force[1] + vel[2] * force[2]
        heavy = rho * (1.0 / RELAX)
        self.base = heavy - 1.5 * heavy * usq - 3.0 * amp * uf
        self.vel = vel
        rho3, rho45 = 3.0 * heavy, 4.5 * heavy
        self.odd_vec = [rho3 * u + (3.0 * amp) * f for u, f in zip(vel, force)]
        self.even_vec = [rho45 * u + (9.0 * amp) * f for u, f in zip(vel, force)]

    def terms(self, k):
        if k == 0:
            return self.base, None
        c = DIRS[k]
        return self.base + along(c, self.vel) * along(c, self.even_vec), along(c, self.odd_vec)

    def one(self, k):
        first = k if k % 2 == 1 else k - 1
        even, odd = self.terms(first)
        return even + odd if first == k else even - odd


KEEP = 1.0 - 1.0 / RELAX


def sample_kernel(
    pos, gain, pops_hbm, flags, cells, turb, chord, blade,
    north, south, east, west,
    pops, vh, vm, vl, sel, fld, m128, r128, dense, sems,
):
    for x in range(CX):
        pltpu.make_async_copy(pops_hbm.at[:, x], pops.at[:, x], sems.at[x]).start()
    points = cells.shape[1]
    tiles = points // LANES
    start_x, start_y = pos[0], pos[1]
    px = cells[0:1, :] - start_x
    py = cells[1:2, :] - start_y
    own = (px >= 0) & (px < CX) & (py >= 0) & (py < CY)
    own = jnp.where(own, 1.0, 0.0)
    m128[...] = jnp.zeros_like(m128)
    for j in range(tiles):
        m128[j : j + 1, :] = own[:, j * LANES : (j + 1) * LANES]
    mask = m128[...]
    maskb = mask.astype(BF16)
    rows = lax.broadcasted_iota(jnp.int32, (LANES, LANES), 0)
    cols = lax.broadcasted_iota(jnp.int32, (LANES, LANES), 1)
    before = jnp.where(rows < cols, 1.0, 0.0).astype(BF16)
    above = jnp.where(rows > cols, 1.0, 0.0).astype(BF16)
    inside = dot(maskb, before)
    ahead = jnp.sum(dot(above, maskb), axis=1, keepdims=True)
    r128[...] = jnp.where(mask > 0.0, inside + ahead, -1.0)
    count = jnp.sum(mask).astype(jnp.int32)

    fld[0:1, :] = px.astype(F32)
    fld[1:2, :] = py.astype(F32)
    fld[2:3, :] = cells[2:3, :].astype(F32)
    fld[3:4, :] = turb[...].astype(F32)
    ch = split3(chord[...])
    bl = split3(blade[...])
    for k in range(3):
        fld[4 + k : 5 + k, :] = ch[k].astype(F32)
        fld[7 + 3 * k : 10 + 3 * k, :] = bl[k].astype(F32)
    dense[...] = jnp.zeros_like(dense)

    def plane(x, carry):
        pltpu.make_async_copy(pops_hbm.at[:, x], pops.at[:, x], sems.at[x]).wait()
        for yb in range(CY // 16):
            g = [pops[i, x, yb * 16 : yb * 16 + 16, :] for i in range(19)]
            rho, mom = moments(g)
            for c in range(3):
                at = pl.multiple_of(c * CX * CY + x * CY + yb * 16, 16)
                high, mid, low = split3(mom[c] / rho)
                vh[pl.ds(at, 16), :] = high
                vm[pl.ds(at, 16), :] = mid
                vl[pl.ds(at, 16), :] = low
        return carry

    lax.fori_loop(0, CX, plane, 0)

    def pack(ids, g, flag):
        rho, mom = moments(g)
        solid = flag != 0
        held = [jnp.where(solid, g[OPP[i]], g[i]) for i in ids]
        return held + [rho, *mom, flag.astype(F32)]

    for ids, x, out in ((EAST, CX - 1, east), (WEST, 0, west)):
        for yb in range(CY // 8):
            at = slice(yb * 8, yb * 8 + 8)
            parts = pack(ids, [pops[i, x, at, :] for i in range(19)], flags[x, at, :])
            for k, part in enumerate(parts):
                out[k, at, :] = part
    for ids, y, out in ((NORTH, CY - 1, north), (SOUTH, 0, south)):
        parts = pack(ids, [pops[i, :, y, :] for i in range(19)], flags[:, y, :])
        for k, part in enumerate(parts):
            out[112 + 8 * k : 120 + 8 * k, :] = part

    spots = lax.broadcasted_iota(jnp.int32, (CHUNK, LANES), 0).astype(F32)
    levels = lax.broadcasted_iota(jnp.int32, (LANES, CHUNK), 0).astype(F32)
    cell_ids = lax.broadcasted_iota(jnp.int32, (CX * CY, CHUNK), 0).astype(F32)

    def chunk(turn, carry):
        base = (turn * CHUNK).astype(F32)
        for j in range(tiles):
            hit = r128[j : j + 1, :] - base == spots
            sel[:, j * LANES : (j + 1) * LANES] = jnp.where(hit, 1.0, 0.0).astype(BF16)
        got = dot(fld[...].astype(BF16), sel[...], NT)
        cell = got[0:1] * CY + got[1:2]
        onez = jnp.where(levels == got[2:3], 1.0, 0.0).astype(BF16)
        factor = jnp.zeros((1, CHUNK), F32)
        for t in range(gain.shape[0]):
            factor = jnp.where(got[3:4] == t, gain[t], factor)
        factor = factor * (got[4:5] + got[5:6] + got[6:7])
        rel = []
        for c in range(3):
            at = slice(c * CX * CY, (c + 1) * CX * CY)
            lines = dot(vh[at, :], onez) + dot(vm[at, :], onez) + dot(vl[at, :], onez)
            sampled = jnp.sum(jnp.where(cell_ids == cell, lines, 0.0), axis=0, keepdims=True)
            speed = got[7 + c : 8 + c] + got[10 + c : 11 + c] + got[13 + c : 14 + c]
            rel.append(sampled - speed)
        size = jnp.sqrt(rel[0] * rel[0] + rel[1] * rel[1] + rel[2] * rel[2] + 0.0001)
        size = -(factor * size)
        pieces = [split3(size * r) for r in rel]
        stack = [pieces[c][k].astype(F32) for k in range(3) for c in range(3)]
        stack = jnp.concatenate(stack + [jnp.zeros((7, CHUNK), F32)], axis=0).astype(BF16)
        spread = dot(stack, sel[...])
        dense[...] += spread[0:3] + spread[3:6] + spread[6:9]
        return carry

    lax.fori_loop(0, (count + CHUNK - 1) // CHUNK, chunk, 0)
    for c in range(3):
        for j in range(tiles):
            north[c * tiles + j : c * tiles + j + 1, :] = dense[
                c : c + 1, j * LANES : (j + 1) * LANES
            ]
    north[3 * tiles : 112, :] = jnp.zeros((112 - 3 * tiles, LANES), F32)
    south[0:112, :] = north[0:112, :]


def known(a, b):
    return jnp.where(a != 0.0, a, b)


def join_kernel(north, south_in, north_in, out):
    out[0:112, :] = known(north[0:112, :], known(south_in[0:112, :], north_in[0:112, :]))
    at = 112
    for x, first, second in ((CX - 1, 7, 9), (0, 10, 8)):
        for ids, src, wanted in ((NORTH, south_in, first), (SOUTH, north_in, second)):
            for k in [ids.index(wanted), 5, 6, 7, 8, 9]:
                row = 112 + 8 * k + x
                out[at : at + 1, :] = src[row : row + 1, :]
                at += 1


FY = 72


def force_kernel(pos, cells, points_in, out, sel, fld, m128, r128, *, total_x, total_y):
    points = cells.shape[1]
    tiles = points // LANES

    def wrapped(v, total):
        v = jnp.where(v < -(total // 2), v + total, v)
        return jnp.where(v >= total // 2, v - total, v)

    px = wrapped(cells[0:1, :] - pos[0], total_x)
    py = wrapped(cells[1:2, :] - pos[1], total_y)
    reach = SMEAR + 1
    near = (px >= -reach) & (px < CX + reach) & (py >= -reach) & (py < CY + reach)
    near = jnp.where(near, 1.0, 0.0)
    m128[...] = jnp.zeros_like(m128)
    for j in range(tiles):
        m128[j : j + 1, :] = near[:, j * LANES : (j + 1) * LANES]
    mask = m128[...]
    maskb = mask.astype(BF16)
    rows = lax.broadcasted_iota(jnp.int32, (LANES, LANES), 0)
    cols = lax.broadcasted_iota(jnp.int32, (LANES, LANES), 1)
    before = jnp.where(rows < cols, 1.0, 0.0).astype(BF16)
    above = jnp.where(rows > cols, 1.0, 0.0).astype(BF16)
    inside = dot(maskb, before)
    ahead = jnp.sum(dot(above, maskb), axis=1, keepdims=True)
    r128[...] = jnp.where(mask > 0.0, inside + ahead, -1.0)
    count = jnp.sum(mask).astype(jnp.int32)

    fld[0:1, :] = px.astype(F32)
    fld[1:2, :] = py.astype(F32)
    fld[2:3, :] = cells[2:3, :].astype(F32)
    pieces = split3(points_in[0:112, :])
    for k in range(3):
        piece = pieces[k].astype(F32)
        for c in range(3):
            for j in range(tiles):
                fld[3 + 3 * k + c : 4 + 3 * k + c, j * LANES : (j + 1) * LANES] = piece[
                    c * tiles + j : c * tiles + j + 1, :
                ]
    fld[12:16, :] = jnp.zeros((4, points), F32)
    out[...] = jnp.zeros_like(out)
    spots = lax.broadcasted_iota(jnp.int32, (CHUNK, LANES), 0).astype(F32)

    def kernel_value(cell, point):
        dist = cell - point
        return jnp.where(
            jnp.abs(dist) <= SMEAR, jnp.exp(-((dist / SCALE) * (dist / SCALE))), 0.0
        )

    def iota(size):
        return lax.broadcasted_iota(jnp.int32, (size, CHUNK), 0).astype(F32)

    def chunk(turn, carry):
        base = (turn * CHUNK).astype(F32)
        for j in range(tiles):
            hit = r128[j : j + 1, :] - base == spots
            sel[:, j * LANES : (j + 1) * LANES] = jnp.where(hit, 1.0, 0.0).astype(BF16)
        got = dot(fld[...].astype(BF16), sel[...], NT)
        kx = kernel_value(iota(16) - 1.0, got[0:1])
        ky = kernel_value(iota(FY) - 1.0, got[1:2])
        kz = kernel_value(iota(LANES), got[2:3])
        left = jnp.concatenate(
            [(got[3 + c : 4 + c] + got[6 + c : 7 + c] + got[9 + c : 10 + c]) * ky for c in range(3)],
            axis=0,
        )
        left_high = left.astype(BF16)
        left_low = (left - left_high.astype(F32)).astype(BF16)
        for x in range(CX + 2):
            right = kx[x : x + 1] * kz
            right_high = right.astype(BF16)
            right_low = (right - right_high.astype(F32)).astype(BF16)
            field = dot(left_high, right_high, NT) + (
                dot(left_high, right_low, NT) + dot(left_low, right_high, NT)
            )
            for c in range(3):
                out[c, x, :, :] += field[c * FY : (c + 1) * FY]
        return carry

    lax.fori_loop(0, (count + CHUNK - 1) // CHUNK, chunk, 0)


OY = 8


def step_kernel(
    pops_hbm, flags, force, from_west, from_east, from_south, from_north, west_pts, east_pts,
    out_hbm, pops, out, sems, out_sems,
):
    for x in range(CX):
        pltpu.make_async_copy(pops_hbm.at[:, x], pops.at[:, x], sems.at[x]).start()
    lane = lax.broadcasted_iota(jnp.int32, (8, LANES), 1)
    not_first, not_last = lane > 0, lane < LANES - 1
    first, last = lane == 0, lane == LANES - 1

    def put(i, x, row, val, mask=True):
        cx, cy, cz = DIRS[i]
        dst = out.at[i, x + 1 + cx, pl.ds(OY + row + cy, val.shape[0]), :]
        if cz == 0:
            dst[...] = val
        elif cz == 1:
            pltpu.store(dst, pltpu.roll(val, 1, 1), mask=not_first[: val.shape[0]])
        else:
            pltpu.store(dst, pltpu.roll(val, LANES - 1, 1), mask=not_last[: val.shape[0]])

    for ids, x, src in ((EAST, -1, from_west), (WEST, CX, from_east)):
        for yb in range(CY // 8):
            at = slice(yb * 8, yb * 8 + 8)
            frc = [force[c, x + 1, yb * 8 + 1 : yb * 8 + 9, :] for c in range(3)]
            rho, mom, solid = src[5, at, :], [src[6 + c, at, :] for c in range(3)], src[9, at, :] != 0.0
            hit = Collision(rho, mom, frc)
            for k, i in enumerate(ids):
                held = src[k, at, :]
                put(i, x, yb * 8, jnp.where(solid, held, KEEP * held + hit.one(i)))
    for ids, y, src in ((NORTH, -1, from_south), (SOUTH, CY, from_north)):
        part = [src[112 + 8 * k : 120 + 8 * k, :] for k in range(10)]
        frc = [force[c, 1 : CX + 1, y + 1, :] for c in range(3)]
        hit = Collision(part[5], part[6:9], frc)
        solid = part[9] != 0.0
        for k, i in enumerate(ids):
            val = jnp.where(solid, part[k], KEEP * part[k] + hit.one(i))
            cx, cy, cz = DIRS[i]
            if cz != 0:
                val = pltpu.roll(val, 1 if cz == 1 else LANES - 1, 1)
            for x in range(CX):
                dst = out.at[i, x + 1 + cx, OY + y + cy : OY + y + cy + 1, :]
                if cz == 0:
                    dst[...] = val[x : x + 1]
                else:
                    keep = (not_first if cz == 1 else not_last)[0:1]
                    pltpu.store(dst, val[x : x + 1], mask=keep)
    for src, at, i, x, y in (
        (west_pts, 112, 7, -1, -1),
        (west_pts, 118, 9, -1, CY),
        (east_pts, 124, 10, CX, -1),
        (east_pts, 130, 8, CX, CY),
    ):
        held, rho = src[at : at + 1, :], src[at + 1 : at + 2, :]
        mom = [src[at + 2 + c : at + 3 + c, :] for c in range(3)]
        solid = src[at + 5 : at + 6, :] != 0.0
        frc = [force[c, x + 1, y + 1 : y + 2, :] for c in range(3)]
        hit = Collision(rho, mom, frc)
        put(i, x, y, jnp.where(solid, held, KEEP * held + hit.one(i)))

    def send(x):
        return pltpu.make_async_copy(
            out.at[:, x + 1, OY : OY + CY, :], out_hbm.at[:, x], out_sems.at[x]
        )

    def plane(x, carry):
        pltpu.make_async_copy(pops_hbm.at[:, x], pops.at[:, x], sems.at[x]).wait()
        for yb in range(CY // 8):
            at = slice(yb * 8, yb * 8 + 8)
            g = [pops[i, x, at, :] for i in range(19)]
            solid = flags[x, at, :] != 0
            rho, mom = moments(g)
            frc = [force[c, x + 1, yb * 8 + 1 : yb * 8 + 9, :] for c in range(3)]
            hit = Collision(rho, mom, frc)
            put(0, x, yb * 8, jnp.where(solid, g[0], KEEP * g[0] + hit.base))
            for k in range(1, 19, 2):
                even, odd = hit.terms(k)
                ahead = jnp.where(solid, g[k + 1], KEEP * g[k] + (even + odd))
                back = jnp.where(solid, g[k], KEEP * g[k + 1] + (even - odd))
                put(k, x, yb * 8, ahead)
                put(k + 1, x, yb * 8, back)
                if DIRS[k][2] != 0:
                    up, down = (k, k + 1) if DIRS[k][2] == 1 else (k + 1, k)
                    rising, falling = (ahead, back) if up == k else (back, ahead)
                    rows = pl.ds(OY + yb * 8, 8)
                    pltpu.store(out.at[up, x + 1, rows, :], falling, mask=first)
                    pltpu.store(out.at[down, x + 1, rows, :], rising, mask=last)

        @pl.when(x > 0)
        def _():
            send(x - 1).start()

        return carry

    lax.fori_loop(0, CX, plane, 0)
    send(CX - 1).start()
    for x in range(CX):
        send(x).wait()


def from_behind(block, axis, distance):
    count = lax.axis_size(axis)
    return lax.ppermute(block, axis, [((i - distance) % count, i) for i in range(count)])


def body(populations, solid_flags, point_cells, point_turbine, blade_speed, chord, turbine_gain):
    points = point_cells.shape[1]
    total_x = CX * lax.axis_size("gx")
    total_y = CY * lax.axis_size("gy")
    pos = jnp.stack([lax.axis_index("gx") * CX, lax.axis_index("gy") * CY]).astype(jnp.int32)
    sds = jax.ShapeDtypeStruct
    params = pltpu.CompilerParams(vmem_limit_bytes=48 * 1024 * 1024)
    compact = [
        pltpu.VMEM((CHUNK, points), BF16),
        pltpu.VMEM((16, points), F32),
        pltpu.VMEM((LANES, LANES), F32),
        pltpu.VMEM((LANES, LANES), F32),
    ]
    plane_block = pltpu.VMEM((19, CX, CY, LANES), F32)
    north, south, east, west = pl.pallas_call(
        sample_kernel,
        out_shape=(
            sds((192, LANES), F32),
            sds((192, LANES), F32),
            sds((10, CY, LANES), F32),
            sds((10, CY, LANES), F32),
        ),
        in_specs=[SMEM, SMEM, ANY, VMEM, VMEM, VMEM, VMEM, VMEM],
        out_specs=(VMEM, VMEM, VMEM, VMEM),
        scratch_shapes=[
            plane_block,
            *[pltpu.VMEM((3 * CX * CY, LANES), BF16)] * 3,
            *compact,
            pltpu.VMEM((3, points), F32),
            pltpu.SemaphoreType.DMA((CX,)),
        ],
        compiler_params=params,
        name="sample",
    )(
        pos, turbine_gain, populations, solid_flags, point_cells,
        point_turbine.reshape(1, points), chord.reshape(1, points), blade_speed,
    )
    from_south = from_behind(north, "gy", 1)
    from_north = from_behind(south, "gy", -1)
    from_west = from_behind(east, "gx", 1)
    from_east = from_behind(west, "gx", -1)
    joined = pl.pallas_call(
        join_kernel,
        out_shape=sds((136, LANES), F32),
        in_specs=[VMEM] * 3,
        out_specs=VMEM,
        name="join",
    )(north, from_south, from_north)
    west_pts = from_behind(joined, "gx", 1)
    east_pts = from_behind(joined, "gx", -1)
    near = known(joined[:112], known(west_pts[:112], east_pts[:112]))
    force = pl.pallas_call(
        functools.partial(force_kernel, total_x=total_x, total_y=total_y),
        out_shape=sds((3, CX + 2, FY, LANES), F32),
        in_specs=[SMEM, VMEM, VMEM],
        out_specs=VMEM,
        scratch_shapes=compact,
        compiler_params=params,
        name="force",
    )(pos, point_cells, near)
    read = pl.pallas_call(
        step_kernel,
        out_shape=sds(populations.shape, F32),
        in_specs=[ANY] + [VMEM] * 8,
        out_specs=ANY,
        scratch_shapes=[
            plane_block,
            pltpu.VMEM((19, CX + 2, CY + 16, LANES), F32),
            pltpu.SemaphoreType.DMA((CX,)),
            pltpu.SemaphoreType.DMA((CX,)),
        ],
        compiler_params=params,
        name="step",
    )(
        populations, solid_flags, force, from_west, from_east, from_south, from_north,
        west_pts, east_pts,
    )
    row = known(near, known(from_behind(near, "gy", 3), from_behind(near, "gy", -3)))
    wide = known(
        known(row, from_behind(row, "gx", 3)),
        known(from_behind(row, "gx", -3), from_behind(row, "gx", -6)),
    )
    whole = known(wide, known(from_behind(wide, "gx", 12), from_behind(wide, "gx", -12)))
    point_force = whole[: 3 * points // LANES].reshape(3, points)
    return read, point_force


def solution(mesh):
    in_specs = (P(None, "gx", "gy", None), P("gx", "gy", None), P(), P(), P(), P(), P())
    out_specs = (P(None, "gx", "gy", None), P())
    return jax.shard_map(body, mesh=mesh, in_specs=in_specs, out_specs=out_specs, check_vma=False)
```

```python
import functools

import jax
import jax.numpy as jnp
from jax import lax
from jax.experimental import pallas as pl
from jax.experimental.pallas import tpu as pltpu
from jax.sharding import PartitionSpec as P


SMEAR = 3
RELAX = 0.8
SCALE = 1.5
CHUNK = 256
LANES = 128
DIRS = [
    (0, 0, 0),
    (1, 0, 0),
    (-1, 0, 0),
    (0, 1, 0),
    (0, -1, 0),
    (0, 0, 1),
    (0, 0, -1),
    (1, 1, 0),
    (-1, -1, 0),
    (1, -1, 0),
    (-1, 1, 0),
    (1, 0, 1),
    (-1, 0, -1),
    (1, 0, -1),
    (-1, 0, 1),
    (0, 1, 1),
    (0, -1, -1),
    (0, 1, -1),
    (0, -1, 1),
]
OPP = [0, 2, 1, 4, 3, 6, 5, 8, 7, 10, 9, 12, 11, 14, 13, 16, 15, 18, 17]
EAST = [i for i in range(19) if DIRS[i][0] == 1]
WEST = [i for i in range(19) if DIRS[i][0] == -1]
NORTH = [i for i in range(19) if DIRS[i][1] == 1]
SOUTH = [i for i in range(19) if DIRS[i][1] == -1]
CX, CY = 8, 64
F32, BF16 = jnp.float32, jnp.bfloat16
FORCE_FLOPS = 40_000_000
STEP_FLOPS = 60_000_000
HBM = pl.BlockSpec(memory_space=pltpu.HBM)
VMEM = pl.BlockSpec(memory_space=pltpu.VMEM)
NT = (((1,), (1,)), ((), ()))
NN = (((1,), (0,)), ((), ()))


def dot(a, b, dims=NN):
    return lax.dot_general(a, b, dims, preferred_element_type=F32)


def split3(v):
    high = v.astype(BF16)
    rest = v - high.astype(F32)
    mid = rest.astype(BF16)
    low = (rest - mid.astype(F32)).astype(BF16)
    return high, mid, low


def moments(g):
    s = [None] * 19
    d = [None] * 19
    for k in range(1, 19, 2):
        s[k] = g[k] + g[k + 1]
        d[k] = g[k] - g[k + 1]
    w1, w2 = 1.0 / 18.0, 1.0 / 36.0
    rho = (
        g[0] * (1.0 / 3.0)
        + (s[1] + s[3] + s[5]) * w1
        + ((s[7] + s[9]) + (s[11] + s[13]) + (s[15] + s[17])) * w2
    )
    mx = d[1] * w1 + ((d[7] + d[9]) + (d[11] + d[13])) * w2
    my = d[3] * w1 + ((d[7] - d[9]) + (d[15] + d[17])) * w2
    mz = d[5] * w1 + ((d[11] - d[13]) + (d[15] - d[17])) * w2
    return rho, (mx, my, mz)


def along(c, v):
    total = None
    for comp, part in zip(c, v):
        if comp == 0:
            continue
        if total is None:
            total = part if comp > 0 else -part
        else:
            total = total + part if comp > 0 else total - part
    return total


class Collision:
    def __init__(self, rho, mom, force):
        inv = 1.0 / rho
        amp = 1.0 - 0.5 / RELAX
        vel = [(m + 0.5 * f) * inv for m, f in zip(mom, force)]
        usq = vel[0] * vel[0] + vel[1] * vel[1] + vel[2] * vel[2]
        uf = vel[0] * force[0] + vel[1] * force[1] + vel[2] * force[2]
        heavy = rho * (1.0 / RELAX)
        self.base = heavy - 1.5 * heavy * usq - 3.0 * amp * uf
        self.vel = vel
        rho3, rho45 = 3.0 * heavy, 4.5 * heavy
        self.odd_vec = [rho3 * u + (3.0 * amp) * f for u, f in zip(vel, force)]
        self.even_vec = [rho45 * u + (9.0 * amp) * f for u, f in zip(vel, force)]

    def terms(self, k):
        if k == 0:
            return self.base, None
        c = DIRS[k]
        return self.base + along(c, self.vel) * along(c, self.even_vec), along(c, self.odd_vec)

    def one(self, k):
        first = k if k % 2 == 1 else k - 1
        even, odd = self.terms(first)
        return even + odd if first == k else even - odd


KEEP = 1.0 - 1.0 / RELAX


def sample_kernel(
    gain_hbm, pops_hbm, flags_hbm, cells_hbm, turb_hbm, chord_hbm, blade_hbm,
    sibling, across, east, west, pops,
    vh, vm, vl, sel, fld, m128, r128, dense, got_ref,
    gain, flags, cells, turb, chord, blade, sems, in_sems,
):
    small = [
        pltpu.make_async_copy(src, dst, in_sems.at[k])
        for k, (src, dst) in enumerate(
            (
                (cells_hbm, cells),
                (turb_hbm, turb.at[0]),
                (chord_hbm, chord.at[0]),
                (blade_hbm, blade),
                (gain_hbm, gain),
                (flags_hbm, flags),
            )
        )
    ]
    for copy in small:
        copy.start()
    for x in range(CX):
        pltpu.make_async_copy(pops_hbm.at[:, x], pops.at[:, x], sems.at[x]).start()
    points = cells.shape[1]
    tiles = points // LANES
    start_x, start_y = lax.axis_index("gx") * CX, lax.axis_index("gy") * CY
    even = lax.axis_index("gy") % 2 == 0
    for copy in small[:5]:
        copy.wait()
    px = cells[0:1, :] - start_x
    py = cells[1:2, :] - start_y
    own = (px >= 0) & (px < CX) & (py >= 0) & (py < CY)
    own = jnp.where(own, 1.0, 0.0)
    m128[...] = jnp.zeros_like(m128)
    for j in range(tiles):
        m128[j : j + 1, :] = own[:, j * LANES : (j + 1) * LANES]
    mask = m128[...]
    maskb = mask.astype(BF16)
    rows = lax.broadcasted_iota(jnp.int32, (LANES, LANES), 0)
    cols = lax.broadcasted_iota(jnp.int32, (LANES, LANES), 1)
    before = jnp.where(rows < cols, 1.0, 0.0).astype(BF16)
    above = jnp.where(rows > cols, 1.0, 0.0).astype(BF16)
    inside = dot(maskb, before)
    ahead = jnp.sum(dot(above, maskb), axis=1, keepdims=True)
    r128[...] = jnp.where(mask > 0.0, inside + ahead, -1.0)
    count = jnp.sum(mask).astype(jnp.int32)

    fld[0:1, :] = px.astype(F32)
    fld[1:2, :] = py.astype(F32)
    fld[2:3, :] = cells[2:3, :].astype(F32)
    fld[3:4, :] = turb[...].astype(F32)
    ch = split3(chord[...])
    bl = split3(blade[...])
    for k in range(3):
        fld[4 + k : 5 + k, :] = ch[k].astype(F32)
        fld[7 + 3 * k : 10 + 3 * k, :] = bl[k].astype(F32)
    dense[...] = jnp.zeros_like(dense)
    spots = lax.broadcasted_iota(jnp.int32, (CHUNK, LANES), 0).astype(F32)

    def choose(turn):
        base = (turn * CHUNK).astype(F32) if not isinstance(turn, int) else 0.0
        for j in range(tiles):
            hit = r128[j : j + 1, :] - base == spots
            sel[:, j * LANES : (j + 1) * LANES] = jnp.where(hit, 1.0, 0.0).astype(BF16)
        got_ref[...] = dot(fld[...].astype(BF16), sel[...], NT)

    @pl.when(count > 0)
    def _():
        choose(0)

    small[5].wait()

    def plane(x, carry):
        pltpu.make_async_copy(pops_hbm.at[:, x], pops.at[:, x], sems.at[x]).wait()
        for yb in range(CY // 16):
            g = [pops[i, x, yb * 16 : yb * 16 + 16, :] for i in range(19)]
            rho, mom = moments(g)
            for c in range(3):
                at = pl.multiple_of(c * CX * CY + x * CY + yb * 16, 16)
                high, mid, low = split3(mom[c] / rho)
                vh[pl.ds(at, 16), :] = high
                vm[pl.ds(at, 16), :] = mid
                vl[pl.ds(at, 16), :] = low
        return carry

    lax.fori_loop(0, CX, plane, 0)

    def pack(ids, g, flag):
        rho, mom = moments(g)
        solid = flag != 0
        held = [jnp.where(solid, g[OPP[i]], g[i]) for i in ids]
        return held + [rho, *mom, flag.astype(F32)]

    for ids, x, out in ((EAST, CX - 1, east), (WEST, 0, west)):
        for yb in range(CY // 8):
            at = slice(yb * 8, yb * 8 + 8)
            parts = pack(ids, [pops[i, x, at, :] for i in range(19)], flags[x, at, :])
            for k, part in enumerate(parts):
                out[k, at, :] = part
    up = pack(NORTH, [pops[i, :, CY - 1, :] for i in range(19)], flags[:, CY - 1, :])
    down = pack(SOUTH, [pops[i, :, 0, :] for i in range(19)], flags[:, 0, :])
    for k, (a, b) in enumerate(zip(up, down)):
        sibling[112 + 8 * k : 120 + 8 * k, :] = jnp.where(even, a, b)
        across[112 + 8 * k : 120 + 8 * k, :] = jnp.where(even, b, a)

    levels = lax.broadcasted_iota(jnp.int32, (LANES, CHUNK), 0).astype(F32)
    cell_ids = lax.broadcasted_iota(jnp.int32, (CX * CY, CHUNK), 0).astype(F32)

    def chunk(turn, carry):
        @pl.when(turn > 0)
        def _():
            choose(turn)

        got = got_ref[...]
        cell = got[0:1] * CY + got[1:2]
        onez = jnp.where(levels == got[2:3], 1.0, 0.0).astype(BF16)
        factor = jnp.zeros((1, CHUNK), F32)
        for t in range(gain.shape[0]):
            factor = jnp.where(got[3:4] == t, gain[t], factor)
        factor = factor * (got[4:5] + got[5:6] + got[6:7])
        rel = []
        for c in range(3):
            at = slice(c * CX * CY, (c + 1) * CX * CY)
            lines = dot(vh[at, :], onez) + dot(vm[at, :], onez) + dot(vl[at, :], onez)
            sampled = jnp.sum(jnp.where(cell_ids == cell, lines, 0.0), axis=0, keepdims=True)
            speed = got[7 + c : 8 + c] + got[10 + c : 11 + c] + got[13 + c : 14 + c]
            rel.append(sampled - speed)
        size = jnp.sqrt(rel[0] * rel[0] + rel[1] * rel[1] + rel[2] * rel[2] + 0.0001)
        size = -(factor * size)
        pieces = [split3(size * r) for r in rel]
        stack = [pieces[c][k].astype(F32) for k in range(3) for c in range(3)]
        stack = jnp.concatenate(stack + [jnp.zeros((7, CHUNK), F32)], axis=0).astype(BF16)
        spread = dot(stack, sel[...])
        dense[...] += spread[0:3] + spread[3:6] + spread[6:9]
        return carry

    lax.fori_loop(0, (count + CHUNK - 1) // CHUNK, chunk, 0)
    for c in range(3):
        for j in range(tiles):
            sibling[c * tiles + j : c * tiles + j + 1, :] = dense[
                c : c + 1, j * LANES : (j + 1) * LANES
            ]
    sibling[3 * tiles : 112, :] = jnp.zeros((112 - 3 * tiles, LANES), F32)
    across[0:112, :] = sibling[0:112, :]


def known(a, b):
    return jnp.where(a != 0.0, a, b)


def join_kernel(own, beside, beyond, out):
    even = lax.axis_index("gy") % 2 == 0
    out[0:112, :] = known(own[0:112, :], known(beside[0:112, :], beyond[0:112, :]))
    at = 112
    for x, first, second in ((CX - 1, 7, 9), (0, 10, 8)):
        for ids, wanted, south in ((NORTH, first, True), (SOUTH, second, False)):
            for k in [ids.index(wanted), 5, 6, 7, 8, 9]:
                row = slice(112 + 8 * k + x, 113 + 8 * k + x)
                a, b = beside[row, :], beyond[row, :]
                out[at : at + 1, :] = jnp.where(even, b, a) if south else jnp.where(even, a, b)
                at += 1


def finish_kernel(mine, other, out):
    whole = known(mine[...], other[...])
    tiles = out.shape[1] // LANES
    for c in range(3):
        for j in range(tiles):
            row = c * tiles + j
            out[c : c + 1, j * LANES : (j + 1) * LANES] = whole[row : row + 1, :]


FY = 72


def force_kernel(cells, points_in, out, sel, fld, m128, r128, *, total_x, total_y):
    points = cells.shape[1]
    tiles = points // LANES

    def wrapped(v, total):
        v = jnp.where(v < -(total // 2), v + total, v)
        return jnp.where(v >= total // 2, v - total, v)

    px = wrapped(cells[0:1, :] - lax.axis_index("gx") * CX, total_x)
    py = wrapped(cells[1:2, :] - lax.axis_index("gy") * CY, total_y)
    reach = SMEAR + 1
    near = (px >= -reach) & (px < CX + reach) & (py >= -reach) & (py < CY + reach)
    near = jnp.where(near, 1.0, 0.0)
    m128[...] = jnp.zeros_like(m128)
    for j in range(tiles):
        m128[j : j + 1, :] = near[:, j * LANES : (j + 1) * LANES]
    mask = m128[...]
    maskb = mask.astype(BF16)
    rows = lax.broadcasted_iota(jnp.int32, (LANES, LANES), 0)
    cols = lax.broadcasted_iota(jnp.int32, (LANES, LANES), 1)
    before = jnp.where(rows < cols, 1.0, 0.0).astype(BF16)
    above = jnp.where(rows > cols, 1.0, 0.0).astype(BF16)
    inside = dot(maskb, before)
    ahead = jnp.sum(dot(above, maskb), axis=1, keepdims=True)
    r128[...] = jnp.where(mask > 0.0, inside + ahead, -1.0)
    count = jnp.sum(mask).astype(jnp.int32)

    fld[0:1, :] = px.astype(F32)
    fld[1:2, :] = py.astype(F32)
    fld[2:3, :] = cells[2:3, :].astype(F32)
    pieces = split3(points_in[0:112, :])
    for k in range(3):
        piece = pieces[k].astype(F32)
        for c in range(3):
            for j in range(tiles):
                fld[3 + 3 * k + c : 4 + 3 * k + c, j * LANES : (j + 1) * LANES] = piece[
                    c * tiles + j : c * tiles + j + 1, :
                ]
    fld[12:16, :] = jnp.zeros((4, points), F32)
    out[...] = jnp.zeros_like(out)
    spots = lax.broadcasted_iota(jnp.int32, (CHUNK, LANES), 0).astype(F32)

    def kernel_value(cell, point):
        dist = cell - point
        return jnp.where(
            jnp.abs(dist) <= SMEAR, jnp.exp(-((dist / SCALE) * (dist / SCALE))), 0.0
        )

    def iota(size):
        return lax.broadcasted_iota(jnp.int32, (size, CHUNK), 0).astype(F32)

    def chunk(turn, carry):
        base = (turn * CHUNK).astype(F32)
        for j in range(tiles):
            hit = r128[j : j + 1, :] - base == spots
            sel[:, j * LANES : (j + 1) * LANES] = jnp.where(hit, 1.0, 0.0).astype(BF16)
        got = dot(fld[...].astype(BF16), sel[...], NT)
        kx = kernel_value(iota(16) - 1.0, got[0:1])
        ky = kernel_value(iota(FY) - 1.0, got[1:2])
        kz = kernel_value(iota(LANES), got[2:3])
        left = jnp.concatenate(
            [(got[3 + c : 4 + c] + got[6 + c : 7 + c] + got[9 + c : 10 + c]) * ky for c in range(3)],
            axis=0,
        )
        left_high = left.astype(BF16)
        left_low = (left - left_high.astype(F32)).astype(BF16)
        for x in range(CX + 2):
            right = kx[x : x + 1] * kz
            right_high = right.astype(BF16)
            right_low = (right - right_high.astype(F32)).astype(BF16)
            field = dot(left_high, right_high, NT) + (
                dot(left_high, right_low, NT) + dot(left_low, right_high, NT)
            )
            for c in range(3):
                out[c, x, :, :] += field[c * FY : (c + 1) * FY]
        return carry

    lax.fori_loop(0, (count + CHUNK - 1) // CHUNK, chunk, 0)


OY = 8


def step_kernel(
    pops, flags, force, from_west, from_east, beside, beyond, west_pts, east_pts,
    out_hbm, out, out_sems,
):
    lane = lax.broadcasted_iota(jnp.int32, (8, LANES), 1)
    not_first, not_last = lane > 0, lane < LANES - 1
    first, last = lane == 0, lane == LANES - 1

    def put(i, x, row, val):
        cx, cy, cz = DIRS[i]
        dst = out.at[i, x + 1 + cx, pl.ds(OY + row + cy, val.shape[0]), :]
        if cz == 0:
            dst[...] = val
        elif cz == 1:
            pltpu.store(dst, pltpu.roll(val, 1, 1), mask=not_first[: val.shape[0]])
        else:
            pltpu.store(dst, pltpu.roll(val, LANES - 1, 1), mask=not_last[: val.shape[0]])

    for ids, x, src in ((EAST, -1, from_west), (WEST, CX, from_east)):
        for yb in range(CY // 8):
            at = slice(yb * 8, yb * 8 + 8)
            frc = [force[c, x + 1, yb * 8 + 1 : yb * 8 + 9, :] for c in range(3)]
            rho, mom, solid = src[5, at, :], [src[6 + c, at, :] for c in range(3)], src[9, at, :] != 0.0
            hit = Collision(rho, mom, frc)
            for k, i in enumerate(ids):
                held = src[k, at, :]
                put(i, x, yb * 8, jnp.where(solid, held, KEEP * held + hit.one(i)))
    even = lax.axis_index("gy") % 2 == 0
    for ids, y in ((NORTH, -1), (SOUTH, CY)):
        part = []
        for k in range(10):
            a, b = beside[112 + 8 * k : 120 + 8 * k, :], beyond[112 + 8 * k : 120 + 8 * k, :]
            part.append(jnp.where(even, b, a) if y < 0 else jnp.where(even, a, b))
        frc = [force[c, 1 : CX + 1, y + 1, :] for c in range(3)]
        hit = Collision(part[5], part[6:9], frc)
        solid = part[9] != 0.0
        for k, i in enumerate(ids):
            val = jnp.where(solid, part[k], KEEP * part[k] + hit.one(i))
            cx, cy, cz = DIRS[i]
            if cz != 0:
                val = pltpu.roll(val, 1 if cz == 1 else LANES - 1, 1)
            for x in range(CX):
                dst = out.at[i, x + 1 + cx, OY + y + cy : OY + y + cy + 1, :]
                if cz == 0:
                    dst[...] = val[x : x + 1]
                else:
                    keep = (not_first if cz == 1 else not_last)[0:1]
                    pltpu.store(dst, val[x : x + 1], mask=keep)
    for src, at, i, x, y in (
        (west_pts, 112, 7, -1, -1),
        (west_pts, 118, 9, -1, CY),
        (east_pts, 124, 10, CX, -1),
        (east_pts, 130, 8, CX, CY),
    ):
        held, rho = src[at : at + 1, :], src[at + 1 : at + 2, :]
        mom = [src[at + 2 + c : at + 3 + c, :] for c in range(3)]
        solid = src[at + 5 : at + 6, :] != 0.0
        frc = [force[c, x + 1, y + 1 : y + 2, :] for c in range(3)]
        hit = Collision(rho, mom, frc)
        put(i, x, y, jnp.where(solid, held, KEEP * held + hit.one(i)))

    def send(x):
        return pltpu.make_async_copy(
            out.at[:, x + 1, OY : OY + CY, :], out_hbm.at[:, x], out_sems.at[x]
        )

    def plane(x, carry):
        for yb in range(CY // 8):
            at = slice(yb * 8, yb * 8 + 8)
            g = [pops[i, x, at, :] for i in range(19)]
            solid = flags[x, at, :] != 0
            rho, mom = moments(g)
            frc = [force[c, x + 1, yb * 8 + 1 : yb * 8 + 9, :] for c in range(3)]
            hit = Collision(rho, mom, frc)
            put(0, x, yb * 8, jnp.where(solid, g[0], KEEP * g[0] + hit.base))
            for k in range(1, 19, 2):
                even, odd = hit.terms(k)
                ahead = jnp.where(solid, g[k + 1], KEEP * g[k] + (even + odd))
                back = jnp.where(solid, g[k], KEEP * g[k + 1] + (even - odd))
                put(k, x, yb * 8, ahead)
                put(k + 1, x, yb * 8, back)
                if DIRS[k][2] != 0:
                    up, down = (k, k + 1) if DIRS[k][2] == 1 else (k + 1, k)
                    rising, falling = (ahead, back) if up == k else (back, ahead)
                    rows = pl.ds(OY + yb * 8, 8)
                    pltpu.store(out.at[up, x + 1, rows, :], falling, mask=first)
                    pltpu.store(out.at[down, x + 1, rows, :], rising, mask=last)

        @pl.when(x > 0)
        def _():
            send(x - 1).start()

        return carry

    lax.fori_loop(0, CX, plane, 0)
    send(CX - 1).start()
    for x in range(CX):
        send(x).wait()


def from_behind(block, axis, distance):
    count = lax.axis_size(axis)
    return lax.ppermute(block, axis, [((i - distance) % count, i) for i in range(count)])


def exchanged(block, source):
    count_x, count_y = lax.axis_size("gx"), lax.axis_size("gy")
    pairs = []
    for x in range(count_x):
        for y in range(count_y):
            from_x, from_y = source(x, y)
            pairs.append(((from_x % count_x) * count_y + from_y % count_y, x * count_y + y))
    return lax.ppermute(block, ("gx", "gy"), pairs)


def swapped(block):
    return exchanged(block, lambda x, y: (x, y ^ 1))


def fetched(block, first, second):
    return exchanged(
        block, lambda x, y: (x + (second if y % 2 else first)[0], y + (second if y % 2 else first)[1])
    )


def cost(flops):
    return pl.CostEstimate(flops=flops, bytes_accessed=0, transcendentals=0)


def local(populations, solid_flags, point_cells, point_turbine, blade_speed, chord, turbine_gain):
    points = point_cells.shape[1]
    total_x = CX * lax.axis_size("gx")
    total_y = CY * lax.axis_size("gy")
    sds = jax.ShapeDtypeStruct
    params = pltpu.CompilerParams(vmem_limit_bytes=40 * 1024 * 1024)
    light = pltpu.CompilerParams(vmem_limit_bytes=4 * 1024 * 1024)
    compact = [
        pltpu.VMEM((CHUNK, points), BF16),
        pltpu.VMEM((16, points), F32),
        pltpu.VMEM((LANES, LANES), F32),
        pltpu.VMEM((LANES, LANES), F32),
    ]
    sibling, across, east, west, held_pops = pl.pallas_call(
        sample_kernel,
        out_shape=(
            sds((192, LANES), F32),
            sds((192, LANES), F32),
            sds((10, CY, LANES), F32),
            sds((10, CY, LANES), F32),
            sds(populations.shape, F32),
        ),
        in_specs=[HBM] * 7,
        out_specs=(VMEM,) * 5,
        scratch_shapes=[
            *[pltpu.VMEM((3 * CX * CY, LANES), BF16)] * 3,
            *compact,
            pltpu.VMEM((3, points), F32),
            pltpu.VMEM((16, CHUNK), F32),
            pltpu.SMEM(turbine_gain.shape, F32),
            pltpu.VMEM(solid_flags.shape, jnp.int32),
            pltpu.VMEM((3, points), jnp.int32),
            pltpu.VMEM((1, points), jnp.int32),
            pltpu.VMEM((1, points), F32),
            pltpu.VMEM((3, points), F32),
            pltpu.SemaphoreType.DMA((CX,)),
            pltpu.SemaphoreType.DMA((6,)),
        ],
        compiler_params=params,
        name="sample",
    )(
        *[
            pltpu.with_memory_space_constraint(arg, pltpu.HBM)
            for arg in (
                turbine_gain, populations, solid_flags, point_cells, point_turbine, chord,
                blade_speed,
            )
        ]
    )
    beside = swapped(sibling)
    beyond = exchanged(across, lambda x, y: (x, y + 1 if y % 2 else y - 1))
    from_west = from_behind(east, "gx", 1)
    from_east = from_behind(west, "gx", -1)
    joined = pl.pallas_call(
        join_kernel,
        out_shape=sds((136, LANES), F32),
        in_specs=[VMEM] * 3,
        out_specs=VMEM,
        compiler_params=light,
        name="join",
    )(sibling, beside, beyond)
    west_pts = from_behind(joined, "gx", 1)
    east_pts = from_behind(joined, "gx", -1)
    near = known(joined[:112], known(west_pts[:112], east_pts[:112]))
    force = pl.pallas_call(
        functools.partial(force_kernel, total_x=total_x, total_y=total_y),
        out_shape=sds((3, CX + 2, FY, LANES), F32),
        in_specs=[VMEM, VMEM],
        out_specs=VMEM,
        scratch_shapes=compact,
        compiler_params=params,
        cost_estimate=cost(FORCE_FLOPS),
        name="force",
    )(point_cells, near)
    read = pl.pallas_call(
        step_kernel,
        out_shape=sds(populations.shape, F32),
        in_specs=[VMEM] * 9,
        out_specs=HBM,
        scratch_shapes=[
            pltpu.VMEM((19, CX + 2, CY + 16, LANES), F32),
            pltpu.SemaphoreType.DMA((CX,)),
        ],
        compiler_params=params,
        cost_estimate=cost(STEP_FLOPS),
        name="step",
    )(
        held_pops, solid_flags, force, from_west, from_east, beside, beyond, west_pts, east_pts,
    )
    have = known(near, swapped(near))
    got = fetched(have, (3, 0), (-3, 0))
    have = known(have, got)
    have = known(have, swapped(have))
    got = fetched(have, (7, 0), (4, 4))
    have = known(have, got)
    have = known(have, swapped(have))
    got = fetched(have, (8, 0), (20, 4))
    have = known(have, got)
    point_force = pl.pallas_call(
        finish_kernel,
        out_shape=sds((3, points), F32),
        in_specs=[VMEM] * 2,
        out_specs=VMEM,
        compiler_params=light,
        name="finish",
    )(have, swapped(have))
    return read, point_force


def solution(mesh):
    in_specs = (P(None, "gx", "gy", None), P("gx", "gy", None), P(), P(), P(), P(), P())
    out_specs = (P(None, "gx", "gy", None), P())
    return jax.shard_map(local, mesh=mesh, in_specs=in_specs, out_specs=out_specs, check_vma=False)
```

```python
import functools

import jax
import jax.numpy as jnp
from jax import lax
from jax.experimental import pallas as pl
from jax.experimental.pallas import tpu as pltpu
from jax.sharding import PartitionSpec as P


SMEAR = 3
RELAX = 0.8
SCALE = 1.5
CHUNK = 256
LANES = 128
DIRS = [
    (0, 0, 0),
    (1, 0, 0),
    (-1, 0, 0),
    (0, 1, 0),
    (0, -1, 0),
    (0, 0, 1),
    (0, 0, -1),
    (1, 1, 0),
    (-1, -1, 0),
    (1, -1, 0),
    (-1, 1, 0),
    (1, 0, 1),
    (-1, 0, -1),
    (1, 0, -1),
    (-1, 0, 1),
    (0, 1, 1),
    (0, -1, -1),
    (0, 1, -1),
    (0, -1, 1),
]
OPP = [0, 2, 1, 4, 3, 6, 5, 8, 7, 10, 9, 12, 11, 14, 13, 16, 15, 18, 17]
EAST = [i for i in range(19) if DIRS[i][0] == 1]
WEST = [i for i in range(19) if DIRS[i][0] == -1]
NORTH = [i for i in range(19) if DIRS[i][1] == 1]
SOUTH = [i for i in range(19) if DIRS[i][1] == -1]
CX, CY = 8, 64
F32, BF16 = jnp.float32, jnp.bfloat16
FORCE_FLOPS = 40_000_000
STEP_FLOPS = 60_000_000
HBM = pl.BlockSpec(memory_space=pltpu.HBM)
VMEM = pl.BlockSpec(memory_space=pltpu.VMEM)
NT = (((1,), (1,)), ((), ()))
NN = (((1,), (0,)), ((), ()))


def dot(a, b, dims=NN):
    return lax.dot_general(a, b, dims, preferred_element_type=F32)


def split3(v):
    high = v.astype(BF16)
    rest = v - high.astype(F32)
    mid = rest.astype(BF16)
    low = (rest - mid.astype(F32)).astype(BF16)
    return high, mid, low


def moments(g):
    s = [None] * 19
    d = [None] * 19
    for k in range(1, 19, 2):
        s[k] = g[k] + g[k + 1]
        d[k] = g[k] - g[k + 1]
    w1, w2 = 1.0 / 18.0, 1.0 / 36.0
    rho = (
        g[0] * (1.0 / 3.0)
        + (s[1] + s[3] + s[5]) * w1
        + ((s[7] + s[9]) + (s[11] + s[13]) + (s[15] + s[17])) * w2
    )
    mx = d[1] * w1 + ((d[7] + d[9]) + (d[11] + d[13])) * w2
    my = d[3] * w1 + ((d[7] - d[9]) + (d[15] + d[17])) * w2
    mz = d[5] * w1 + ((d[11] - d[13]) + (d[15] - d[17])) * w2
    return rho, (mx, my, mz)


def along(c, v):
    total = None
    for comp, part in zip(c, v):
        if comp == 0:
            continue
        if total is None:
            total = part if comp > 0 else -part
        else:
            total = total + part if comp > 0 else total - part
    return total


class Collision:
    def __init__(self, rho, mom, force):
        inv = 1.0 / rho
        amp = 1.0 - 0.5 / RELAX
        vel = [(m + 0.5 * f) * inv for m, f in zip(mom, force)]
        usq = vel[0] * vel[0] + vel[1] * vel[1] + vel[2] * vel[2]
        uf = vel[0] * force[0] + vel[1] * force[1] + vel[2] * force[2]
        heavy = rho * (1.0 / RELAX)
        self.base = heavy - 1.5 * heavy * usq - 3.0 * amp * uf
        self.vel = vel
        rho3, rho45 = 3.0 * heavy, 4.5 * heavy
        self.odd_vec = [rho3 * u + (3.0 * amp) * f for u, f in zip(vel, force)]
        self.even_vec = [rho45 * u + (9.0 * amp) * f for u, f in zip(vel, force)]

    def terms(self, k):
        if k == 0:
            return self.base, None
        c = DIRS[k]
        return self.base + along(c, self.vel) * along(c, self.even_vec), along(c, self.odd_vec)

    def one(self, k):
        first = k if k % 2 == 1 else k - 1
        even, odd = self.terms(first)
        return even + odd if first == k else even - odd


KEEP = 1.0 - 1.0 / RELAX


def sample_kernel(
    gain_hbm, pops_hbm, flags_hbm, cells_hbm, turb_hbm, chord_hbm, blade_hbm,
    sibling, across, east, west, pops,
    vh, vm, vl, sel, fld, m128, r128, dense, got_ref,
    gain, flags, cells, turb, chord, blade, sems, in_sems,
):
    small = [
        pltpu.make_async_copy(src, dst, in_sems.at[k])
        for k, (src, dst) in enumerate(
            (
                (cells_hbm, cells),
                (turb_hbm, turb.at[0]),
                (chord_hbm, chord.at[0]),
                (blade_hbm, blade),
                (gain_hbm, gain),
                (flags_hbm, flags),
            )
        )
    ]
    for copy in small:
        copy.start()
    for x in range(CX):
        pltpu.make_async_copy(pops_hbm.at[:, x], pops.at[:, x], sems.at[x]).start()
    points = cells.shape[1]
    tiles = points // LANES
    start_x, start_y = lax.axis_index("gx") * CX, lax.axis_index("gy") * CY
    even = lax.axis_index("gy") % 2 == 0
    for copy in small[:5]:
        copy.wait()
    px = cells[0:1, :] - start_x
    py = cells[1:2, :] - start_y
    own = (px >= 0) & (px < CX) & (py >= 0) & (py < CY)
    own = jnp.where(own, 1.0, 0.0)
    m128[...] = jnp.zeros_like(m128)
    for j in range(tiles):
        m128[j : j + 1, :] = own[:, j * LANES : (j + 1) * LANES]
    mask = m128[...]
    maskb = mask.astype(BF16)
    rows = lax.broadcasted_iota(jnp.int32, (LANES, LANES), 0)
    cols = lax.broadcasted_iota(jnp.int32, (LANES, LANES), 1)
    before = jnp.where(rows < cols, 1.0, 0.0).astype(BF16)
    above = jnp.where(rows > cols, 1.0, 0.0).astype(BF16)
    inside = dot(maskb, before)
    ahead = jnp.sum(dot(above, maskb), axis=1, keepdims=True)
    r128[...] = jnp.where(mask > 0.0, inside + ahead, -1.0)
    count = jnp.sum(mask).astype(jnp.int32)

    fld[0:1, :] = px.astype(F32)
    fld[1:2, :] = py.astype(F32)
    fld[2:3, :] = cells[2:3, :].astype(F32)
    fld[3:4, :] = turb[...].astype(F32)
    ch = split3(chord[...])
    bl = split3(blade[...])
    for k in range(3):
        fld[4 + k : 5 + k, :] = ch[k].astype(F32)
        fld[7 + 3 * k : 10 + 3 * k, :] = bl[k].astype(F32)
    dense[...] = jnp.zeros_like(dense)
    spots = lax.broadcasted_iota(jnp.int32, (CHUNK, LANES), 0).astype(F32)

    def choose(turn):
        base = (turn * CHUNK).astype(F32) if not isinstance(turn, int) else 0.0
        for j in range(tiles):
            hit = r128[j : j + 1, :] - base == spots
            sel[:, j * LANES : (j + 1) * LANES] = jnp.where(hit, 1.0, 0.0).astype(BF16)
        got_ref[...] = dot(fld[...].astype(BF16), sel[...], NT)

    @pl.when(count > 0)
    def _():
        choose(0)

    small[5].wait()

    def plane(x, carry):
        pltpu.make_async_copy(pops_hbm.at[:, x], pops.at[:, x], sems.at[x]).wait()
        for yb in range(CY // 16):
            g = [pops[i, x, yb * 16 : yb * 16 + 16, :] for i in range(19)]
            rho, mom = moments(g)
            for c in range(3):
                at = pl.multiple_of(c * CX * CY + x * CY + yb * 16, 16)
                high, mid, low = split3(mom[c] / rho)
                vh[pl.ds(at, 16), :] = high
                vm[pl.ds(at, 16), :] = mid
                vl[pl.ds(at, 16), :] = low
        return carry

    lax.fori_loop(0, CX, plane, 0)

    def pack(ids, g, flag):
        rho, mom = moments(g)
        solid = flag != 0
        held = [jnp.where(solid, g[OPP[i]], g[i]) for i in ids]
        return held + [rho, *mom, flag.astype(F32)]

    for ids, x, out in ((EAST, CX - 1, east), (WEST, 0, west)):
        for yb in range(CY // 8):
            at = slice(yb * 8, yb * 8 + 8)
            parts = pack(ids, [pops[i, x, at, :] for i in range(19)], flags[x, at, :])
            for k, part in enumerate(parts):
                out[k, at, :] = part
    up = pack(NORTH, [pops[i, :, CY - 1, :] for i in range(19)], flags[:, CY - 1, :])
    down = pack(SOUTH, [pops[i, :, 0, :] for i in range(19)], flags[:, 0, :])
    for k, (a, b) in enumerate(zip(up, down)):
        sibling[112 + 8 * k : 120 + 8 * k, :] = jnp.where(even, a, b)
        across[112 + 8 * k : 120 + 8 * k, :] = jnp.where(even, b, a)

    levels = lax.broadcasted_iota(jnp.int32, (LANES, CHUNK), 0).astype(F32)
    cell_ids = lax.broadcasted_iota(jnp.int32, (CX * CY, CHUNK), 0).astype(F32)

    def chunk(turn, carry):
        @pl.when(turn > 0)
        def _():
            choose(turn)

        got = got_ref[...]
        cell = got[0:1] * CY + got[1:2]
        onez = jnp.where(levels == got[2:3], 1.0, 0.0).astype(BF16)
        factor = jnp.zeros((1, CHUNK), F32)
        for t in range(gain.shape[0]):
            factor = jnp.where(got[3:4] == t, gain[t], factor)
        factor = factor * (got[4:5] + got[5:6] + got[6:7])
        rel = []
        for c in range(3):
            at = slice(c * CX * CY, (c + 1) * CX * CY)
            lines = dot(vh[at, :], onez) + dot(vm[at, :], onez) + dot(vl[at, :], onez)
            sampled = jnp.sum(jnp.where(cell_ids == cell, lines, 0.0), axis=0, keepdims=True)
            speed = got[7 + c : 8 + c] + got[10 + c : 11 + c] + got[13 + c : 14 + c]
            rel.append(sampled - speed)
        size = jnp.sqrt(rel[0] * rel[0] + rel[1] * rel[1] + rel[2] * rel[2] + 0.0001)
        size = -(factor * size)
        pieces = [split3(size * r) for r in rel]
        stack = [pieces[c][k].astype(F32) for k in range(3) for c in range(3)]
        stack = jnp.concatenate(stack + [jnp.zeros((7, CHUNK), F32)], axis=0).astype(BF16)
        spread = dot(stack, sel[...])
        dense[...] += spread[0:3] + spread[3:6] + spread[6:9]
        return carry

    lax.fori_loop(0, (count + CHUNK - 1) // CHUNK, chunk, 0)
    for c in range(3):
        for j in range(tiles):
            sibling[c * tiles + j : c * tiles + j + 1, :] = dense[
                c : c + 1, j * LANES : (j + 1) * LANES
            ]
    sibling[3 * tiles : 112, :] = jnp.zeros((112 - 3 * tiles, LANES), F32)
    across[0:112, :] = sibling[0:112, :]


def known(a, b):
    return jnp.where(a != 0.0, a, b)


def join_kernel(own, beside, beyond, out):
    even = lax.axis_index("gy") % 2 == 0
    out[0:112, :] = known(own[0:112, :], known(beside[0:112, :], beyond[0:112, :]))
    at = 112
    for x, first, second in ((CX - 1, 7, 9), (0, 10, 8)):
        for ids, wanted, south in ((NORTH, first, True), (SOUTH, second, False)):
            for k in [ids.index(wanted), 5, 6, 7, 8, 9]:
                row = slice(112 + 8 * k + x, 113 + 8 * k + x)
                a, b = beside[row, :], beyond[row, :]
                out[at : at + 1, :] = jnp.where(even, b, a) if south else jnp.where(even, a, b)
                at += 1


def finish_kernel(mine, other, out):
    whole = known(mine[...], other[...])
    tiles = out.shape[1] // LANES
    for c in range(3):
        for j in range(tiles):
            row = c * tiles + j
            out[c : c + 1, j * LANES : (j + 1) * LANES] = whole[row : row + 1, :]


FY = 72


def force_kernel(cells, points_in, out, sel, fld, m128, r128, *, total_x, total_y):
    points = cells.shape[1]
    tiles = points // LANES

    def wrapped(v, total):
        v = jnp.where(v < -(total // 2), v + total, v)
        return jnp.where(v >= total // 2, v - total, v)

    px = wrapped(cells[0:1, :] - lax.axis_index("gx") * CX, total_x)
    py = wrapped(cells[1:2, :] - lax.axis_index("gy") * CY, total_y)
    reach = SMEAR + 1
    near = (px >= -reach) & (px < CX + reach) & (py >= -reach) & (py < CY + reach)
    near = jnp.where(near, 1.0, 0.0)
    m128[...] = jnp.zeros_like(m128)
    for j in range(tiles):
        m128[j : j + 1, :] = near[:, j * LANES : (j + 1) * LANES]
    mask = m128[...]
    maskb = mask.astype(BF16)
    rows = lax.broadcasted_iota(jnp.int32, (LANES, LANES), 0)
    cols = lax.broadcasted_iota(jnp.int32, (LANES, LANES), 1)
    before = jnp.where(rows < cols, 1.0, 0.0).astype(BF16)
    above = jnp.where(rows > cols, 1.0, 0.0).astype(BF16)
    inside = dot(maskb, before)
    ahead = jnp.sum(dot(above, maskb), axis=1, keepdims=True)
    r128[...] = jnp.where(mask > 0.0, inside + ahead, -1.0)
    count = jnp.sum(mask).astype(jnp.int32)

    fld[0:1, :] = px.astype(F32)
    fld[1:2, :] = py.astype(F32)
    fld[2:3, :] = cells[2:3, :].astype(F32)
    pieces = split3(points_in[0:112, :])
    for k in range(3):
        piece = pieces[k].astype(F32)
        for c in range(3):
            for j in range(tiles):
                fld[3 + 3 * k + c : 4 + 3 * k + c, j * LANES : (j + 1) * LANES] = piece[
                    c * tiles + j : c * tiles + j + 1, :
                ]
    fld[12:16, :] = jnp.zeros((4, points), F32)
    out[...] = jnp.zeros_like(out)
    spots = lax.broadcasted_iota(jnp.int32, (CHUNK, LANES), 0).astype(F32)

    def kernel_value(cell, point):
        dist = cell - point
        return jnp.where(
            jnp.abs(dist) <= SMEAR, jnp.exp(-((dist / SCALE) * (dist / SCALE))), 0.0
        )

    def iota(size):
        return lax.broadcasted_iota(jnp.int32, (size, CHUNK), 0).astype(F32)

    def chunk(turn, carry):
        base = (turn * CHUNK).astype(F32)
        for j in range(tiles):
            hit = r128[j : j + 1, :] - base == spots
            sel[:, j * LANES : (j + 1) * LANES] = jnp.where(hit, 1.0, 0.0).astype(BF16)
        got = dot(fld[...].astype(BF16), sel[...], NT)
        kx = kernel_value(iota(16) - 1.0, got[0:1])
        ky = kernel_value(iota(FY) - 1.0, got[1:2])
        kz = kernel_value(iota(LANES), got[2:3])
        left = jnp.concatenate(
            [(got[3 + c : 4 + c] + got[6 + c : 7 + c] + got[9 + c : 10 + c]) * ky for c in range(3)],
            axis=0,
        )
        left_high = left.astype(BF16)
        left_low = (left - left_high.astype(F32)).astype(BF16)
        for x in range(CX + 2):
            right = kx[x : x + 1] * kz
            right_high = right.astype(BF16)
            right_low = (right - right_high.astype(F32)).astype(BF16)
            field = dot(left_high, right_high, NT) + (
                dot(left_high, right_low, NT) + dot(left_low, right_high, NT)
            )
            for c in range(3):
                out[c, x, :, :] += field[c * FY : (c + 1) * FY]
        return carry

    lax.fori_loop(0, (count + CHUNK - 1) // CHUNK, chunk, 0)


OY = 8


def step_kernel(
    pops, flags, force, from_west, from_east, beside, beyond, west_pts, east_pts, *rest, low, high
):
    out_hbm, out, out_sems = rest[-3:]
    lane = lax.broadcasted_iota(jnp.int32, (8, LANES), 1)
    not_first, not_last = lane > 0, lane < LANES - 1
    first, last = lane == 0, lane == LANES - 1

    def put(i, x, row, val):
        cx, cy, cz = DIRS[i]
        dst = out.at[i, x - low + 1 + cx, pl.ds(OY + row + cy, val.shape[0]), :]
        if cz == 0:
            dst[...] = val
        elif cz == 1:
            pltpu.store(dst, pltpu.roll(val, 1, 1), mask=not_first[: val.shape[0]])
        else:
            pltpu.store(dst, pltpu.roll(val, LANES - 1, 1), mask=not_last[: val.shape[0]])

    def inside(x):
        return low <= x < high

    def force_at(x, yb):
        return [force[c, x + 1, yb * 8 + 1 : yb * 8 + 9, :] for c in range(3)]

    for ids, x, src in ((EAST, low - 1, from_west), (WEST, high, from_east)):
        for yb in range(CY // 8):
            at = slice(yb * 8, yb * 8 + 8)
            if 0 <= x < CX:
                g = [pops[i, x, at, :] for i in range(19)]
                rho, mom = moments(g)
                solid = flags[x, at, :] != 0
                held = [jnp.where(solid, g[OPP[i]], g[i]) for i in ids]
            else:
                rho, mom = src[5, at, :], [src[6 + c, at, :] for c in range(3)]
                solid = src[9, at, :] != 0.0
                held = [src[k, at, :] for k in range(5)]
            hit = Collision(rho, mom, force_at(x, yb))
            for val, i in zip(held, ids):
                put(i, x, yb * 8, jnp.where(solid, val, KEEP * val + hit.one(i)))
    even = lax.axis_index("gy") % 2 == 0
    for ids, y in ((NORTH, -1), (SOUTH, CY)):
        part = []
        for k in range(10):
            a, b = beside[112 + 8 * k : 120 + 8 * k, :], beyond[112 + 8 * k : 120 + 8 * k, :]
            part.append(jnp.where(even, b, a) if y < 0 else jnp.where(even, a, b))
        frc = [force[c, 1 : CX + 1, y + 1, :] for c in range(3)]
        hit = Collision(part[5], part[6:9], frc)
        solid = part[9] != 0.0
        for k, i in enumerate(ids):
            val = jnp.where(solid, part[k], KEEP * part[k] + hit.one(i))
            cx, cy, cz = DIRS[i]
            if cz != 0:
                val = pltpu.roll(val, 1 if cz == 1 else LANES - 1, 1)
            for x in range(CX):
                if not inside(x + cx):
                    continue
                dst = out.at[i, x - low + 1 + cx, OY + y + cy : OY + y + cy + 1, :]
                if cz == 0:
                    dst[...] = val[x : x + 1]
                else:
                    keep = (not_first if cz == 1 else not_last)[0:1]
                    pltpu.store(dst, val[x : x + 1], mask=keep)
    for src, at, i, x, y in (
        (west_pts, 112, 7, -1, -1),
        (west_pts, 118, 9, -1, CY),
        (east_pts, 124, 10, CX, -1),
        (east_pts, 130, 8, CX, CY),
    ):
        if not inside(x + DIRS[i][0]):
            continue
        held, rho = src[at : at + 1, :], src[at + 1 : at + 2, :]
        mom = [src[at + 2 + c : at + 3 + c, :] for c in range(3)]
        solid = src[at + 5 : at + 6, :] != 0.0
        frc = [force[c, x + 1, y + 1 : y + 2, :] for c in range(3)]
        hit = Collision(rho, mom, frc)
        put(i, x, y, jnp.where(solid, held, KEEP * held + hit.one(i)))

    def send(x):
        return pltpu.make_async_copy(
            out.at[:, x - low + 1, OY : OY + CY, :], out_hbm.at[:, x], out_sems.at[x]
        )

    def plane(x, carry):
        for yb in range(CY // 8):
            at = slice(yb * 8, yb * 8 + 8)
            g = [pops[i, x, at, :] for i in range(19)]
            solid = flags[x, at, :] != 0
            rho, mom = moments(g)
            hit = Collision(rho, mom, force_at(x, yb))
            put(0, x, yb * 8, jnp.where(solid, g[0], KEEP * g[0] + hit.base))
            for k in range(1, 19, 2):
                even, odd = hit.terms(k)
                ahead = jnp.where(solid, g[k + 1], KEEP * g[k] + (even + odd))
                back = jnp.where(solid, g[k], KEEP * g[k + 1] + (even - odd))
                put(k, x, yb * 8, ahead)
                put(k + 1, x, yb * 8, back)
                if DIRS[k][2] != 0:
                    up, down = (k, k + 1) if DIRS[k][2] == 1 else (k + 1, k)
                    rising, falling = (ahead, back) if up == k else (back, ahead)
                    rows = pl.ds(OY + yb * 8, 8)
                    pltpu.store(out.at[up, x - low + 1, rows, :], falling, mask=first)
                    pltpu.store(out.at[down, x - low + 1, rows, :], rising, mask=last)

        @pl.when(x > low)
        def _():
            send(x - 1).start()

        return carry

    lax.fori_loop(low, high, plane, 0)
    send(high - 1).start()
    for x in range(low, high):
        send(x).wait()


def from_behind(block, axis, distance):
    count = lax.axis_size(axis)
    return lax.ppermute(block, axis, [((i - distance) % count, i) for i in range(count)])


def exchanged(block, source):
    count_x, count_y = lax.axis_size("gx"), lax.axis_size("gy")
    pairs = []
    for x in range(count_x):
        for y in range(count_y):
            from_x, from_y = source(x, y)
            pairs.append(((from_x % count_x) * count_y + from_y % count_y, x * count_y + y))
    return lax.ppermute(block, ("gx", "gy"), pairs)


def swapped(block):
    return exchanged(block, lambda x, y: (x, y ^ 1))


def fetched(block, first, second):
    return exchanged(
        block, lambda x, y: (x + (second if y % 2 else first)[0], y + (second if y % 2 else first)[1])
    )


def cost(flops):
    return pl.CostEstimate(flops=flops, bytes_accessed=0, transcendentals=0)


def local(populations, solid_flags, point_cells, point_turbine, blade_speed, chord, turbine_gain):
    points = point_cells.shape[1]
    total_x = CX * lax.axis_size("gx")
    total_y = CY * lax.axis_size("gy")
    sds = jax.ShapeDtypeStruct
    params = pltpu.CompilerParams(vmem_limit_bytes=40 * 1024 * 1024)
    light = pltpu.CompilerParams(vmem_limit_bytes=4 * 1024 * 1024)
    compact = [
        pltpu.VMEM((CHUNK, points), BF16),
        pltpu.VMEM((16, points), F32),
        pltpu.VMEM((LANES, LANES), F32),
        pltpu.VMEM((LANES, LANES), F32),
    ]
    sibling, across, east, west, held_pops = pl.pallas_call(
        sample_kernel,
        out_shape=(
            sds((192, LANES), F32),
            sds((192, LANES), F32),
            sds((10, CY, LANES), F32),
            sds((10, CY, LANES), F32),
            sds(populations.shape, F32),
        ),
        in_specs=[HBM] * 7,
        out_specs=(VMEM,) * 5,
        scratch_shapes=[
            *[pltpu.VMEM((3 * CX * CY, LANES), BF16)] * 3,
            *compact,
            pltpu.VMEM((3, points), F32),
            pltpu.VMEM((16, CHUNK), F32),
            pltpu.SMEM(turbine_gain.shape, F32),
            pltpu.VMEM(solid_flags.shape, jnp.int32),
            pltpu.VMEM((3, points), jnp.int32),
            pltpu.VMEM((1, points), jnp.int32),
            pltpu.VMEM((1, points), F32),
            pltpu.VMEM((3, points), F32),
            pltpu.SemaphoreType.DMA((CX,)),
            pltpu.SemaphoreType.DMA((6,)),
        ],
        compiler_params=params,
        name="sample",
    )(
        *[
            pltpu.with_memory_space_constraint(arg, pltpu.HBM)
            for arg in (
                turbine_gain, populations, solid_flags, point_cells, point_turbine, chord,
                blade_speed,
            )
        ]
    )
    beside = swapped(sibling)
    beyond = exchanged(across, lambda x, y: (x, y + 1 if y % 2 else y - 1))
    from_west = from_behind(east, "gx", 1)
    from_east = from_behind(west, "gx", -1)
    joined = pl.pallas_call(
        join_kernel,
        out_shape=sds((136, LANES), F32),
        in_specs=[VMEM] * 3,
        out_specs=VMEM,
        compiler_params=light,
        name="join",
    )(sibling, beside, beyond)
    west_pts = from_behind(joined, "gx", 1)
    east_pts = from_behind(joined, "gx", -1)
    near = known(joined[:112], known(west_pts[:112], east_pts[:112]))
    force = pl.pallas_call(
        functools.partial(force_kernel, total_x=total_x, total_y=total_y),
        out_shape=sds((3, CX + 2, FY, LANES), F32),
        in_specs=[VMEM, VMEM],
        out_specs=VMEM,
        scratch_shapes=compact,
        compiler_params=params,
        cost_estimate=cost(FORCE_FLOPS),
        name="force",
    )(point_cells, near)
    step_args = (
        held_pops, solid_flags, force, from_west, from_east, beside, beyond, west_pts, east_pts,
    )
    read = None
    for low, high in ((0, CX // 2), (CX // 2, CX)):
        extra = () if read is None else (read,)
        read = pl.pallas_call(
            functools.partial(step_kernel, low=low, high=high),
            out_shape=sds(populations.shape, F32),
            in_specs=[VMEM] * 9 + [HBM] * len(extra),
            out_specs=HBM,
            scratch_shapes=[
                pltpu.VMEM((19, high - low + 2, CY + 16, LANES), F32),
                pltpu.SemaphoreType.DMA((CX,)),
            ],
            input_output_aliases={9: 0} if extra else {},
            compiler_params=params,
            cost_estimate=cost(STEP_FLOPS),
        )(*step_args, *extra)
    have = known(near, swapped(near))
    got = fetched(have, (3, 0), (-3, 0))
    have = known(have, got)
    have = known(have, swapped(have))
    got = fetched(have, (7, 0), (4, 4))
    have = known(have, got)
    have = known(have, swapped(have))
    got = fetched(have, (8, 0), (20, 4))
    have = known(have, got)
    point_force = pl.pallas_call(
        finish_kernel,
        out_shape=sds((3, points), F32),
        in_specs=[VMEM] * 2,
        out_specs=VMEM,
        compiler_params=light,
        name="finish",
    )(have, swapped(have))
    return read, point_force


def solution(mesh):
    in_specs = (P(None, "gx", "gy", None), P("gx", "gy", None), P(), P(), P(), P(), P())
    out_specs = (P(None, "gx", "gy", None), P())
    return jax.shard_map(local, mesh=mesh, in_specs=in_specs, out_specs=out_specs, check_vma=False)
```

```python
import functools

import jax
import jax.numpy as jnp
from jax import lax
from jax.experimental import pallas as pl
from jax.experimental.pallas import tpu as pltpu
from jax.sharding import PartitionSpec as P


SMEAR = 3
RELAX = 0.8
SCALE = 1.5
CHUNK = 256
LANES = 128
DIRS = [
    (0, 0, 0),
    (1, 0, 0),
    (-1, 0, 0),
    (0, 1, 0),
    (0, -1, 0),
    (0, 0, 1),
    (0, 0, -1),
    (1, 1, 0),
    (-1, -1, 0),
    (1, -1, 0),
    (-1, 1, 0),
    (1, 0, 1),
    (-1, 0, -1),
    (1, 0, -1),
    (-1, 0, 1),
    (0, 1, 1),
    (0, -1, -1),
    (0, 1, -1),
    (0, -1, 1),
]
OPP = [0, 2, 1, 4, 3, 6, 5, 8, 7, 10, 9, 12, 11, 14, 13, 16, 15, 18, 17]
EAST = [i for i in range(19) if DIRS[i][0] == 1]
WEST = [i for i in range(19) if DIRS[i][0] == -1]
NORTH = [i for i in range(19) if DIRS[i][1] == 1]
SOUTH = [i for i in range(19) if DIRS[i][1] == -1]
CX, CY = 8, 64
F32, BF16 = jnp.float32, jnp.bfloat16
FORCE_FLOPS = 40_000_000
STEP_FLOPS = 60_000_000
HBM = pl.BlockSpec(memory_space=pltpu.HBM)
VMEM = pl.BlockSpec(memory_space=pltpu.VMEM)
SMEM = pl.BlockSpec(memory_space=pltpu.SMEM)
NT = (((1,), (1,)), ((), ()))
NN = (((1,), (0,)), ((), ()))


def dot(a, b, dims=NN):
    return lax.dot_general(a, b, dims, preferred_element_type=F32)


def split3(v):
    high = v.astype(BF16)
    rest = v - high.astype(F32)
    mid = rest.astype(BF16)
    low = (rest - mid.astype(F32)).astype(BF16)
    return high, mid, low


def moments(g):
    s = [None] * 19
    d = [None] * 19
    for k in range(1, 19, 2):
        s[k] = g[k] + g[k + 1]
        d[k] = g[k] - g[k + 1]
    w1, w2 = 1.0 / 18.0, 1.0 / 36.0
    rho = (
        g[0] * (1.0 / 3.0)
        + (s[1] + s[3] + s[5]) * w1
        + ((s[7] + s[9]) + (s[11] + s[13]) + (s[15] + s[17])) * w2
    )
    mx = d[1] * w1 + ((d[7] + d[9]) + (d[11] + d[13])) * w2
    my = d[3] * w1 + ((d[7] - d[9]) + (d[15] + d[17])) * w2
    mz = d[5] * w1 + ((d[11] - d[13]) + (d[15] - d[17])) * w2
    return rho, (mx, my, mz)


def along(c, v):
    total = None
    for comp, part in zip(c, v):
        if comp == 0:
            continue
        if total is None:
            total = part if comp > 0 else -part
        else:
            total = total + part if comp > 0 else total - part
    return total


class Collision:
    def __init__(self, rho, mom, force):
        inv = 1.0 / rho
        amp = 1.0 - 0.5 / RELAX
        vel = [(m + 0.5 * f) * inv for m, f in zip(mom, force)]
        usq = vel[0] * vel[0] + vel[1] * vel[1] + vel[2] * vel[2]
        uf = vel[0] * force[0] + vel[1] * force[1] + vel[2] * force[2]
        heavy = rho * (1.0 / RELAX)
        self.base = heavy - 1.5 * heavy * usq - 3.0 * amp * uf
        self.vel = vel
        rho3, rho45 = 3.0 * heavy, 4.5 * heavy
        self.odd_vec = [rho3 * u + (3.0 * amp) * f for u, f in zip(vel, force)]
        self.even_vec = [rho45 * u + (9.0 * amp) * f for u, f in zip(vel, force)]

    def terms(self, k):
        if k == 0:
            return self.base, None
        c = DIRS[k]
        return self.base + along(c, self.vel) * along(c, self.even_vec), along(c, self.odd_vec)

    def one(self, k):
        first = k if k % 2 == 1 else k - 1
        even, odd = self.terms(first)
        return even + odd if first == k else even - odd


KEEP = 1.0 - 1.0 / RELAX


def sample_kernel(
    gain_hbm, pops_hbm, flags_hbm, cells_hbm, turb_hbm, chord_hbm, blade_hbm,
    sibling, across, east, west, pops,
    vhm, vl, sel, fld, m128, r128, dense, got_ref,
    gain, flags, cells, turb, chord, blade, sems, in_sems,
):
    small = [
        pltpu.make_async_copy(src, dst, in_sems.at[k])
        for k, (src, dst) in enumerate(
            (
                (cells_hbm, cells),
                (turb_hbm, turb.at[0]),
                (chord_hbm, chord.at[0]),
                (blade_hbm, blade),
                (gain_hbm, gain),
                (flags_hbm, flags),
            )
        )
    ]
    for copy in small:
        copy.start()
    for x in range(CX):
        pltpu.make_async_copy(pops_hbm.at[:, x], pops.at[:, x], sems.at[x]).start()
    points = cells.shape[1]
    tiles = points // LANES
    start_x, start_y = lax.axis_index("gx") * CX, lax.axis_index("gy") * CY
    even = lax.axis_index("gy") % 2 == 0
    for copy in small[:5]:
        copy.wait()
    px = cells[0:1, :] - start_x
    py = cells[1:2, :] - start_y
    own = (px >= 0) & (px < CX) & (py >= 0) & (py < CY)
    own = jnp.where(own, 1.0, 0.0)
    m128[...] = jnp.zeros_like(m128)
    for j in range(tiles):
        m128[j : j + 1, :] = own[:, j * LANES : (j + 1) * LANES]
    mask = m128[...]
    maskb = mask.astype(BF16)
    rows = lax.broadcasted_iota(jnp.int32, (LANES, LANES), 0)
    cols = lax.broadcasted_iota(jnp.int32, (LANES, LANES), 1)
    before = jnp.where(rows < cols, 1.0, 0.0).astype(BF16)
    above = jnp.where(rows > cols, 1.0, 0.0).astype(BF16)
    inside = dot(maskb, before)
    ahead = jnp.sum(dot(above, maskb), axis=1, keepdims=True)
    r128[...] = jnp.where(mask > 0.0, inside + ahead, -1.0)
    count = jnp.sum(mask).astype(jnp.int32)

    fld[0:1, :] = px.astype(F32)
    fld[1:2, :] = py.astype(F32)
    fld[2:3, :] = cells[2:3, :].astype(F32)
    fld[3:4, :] = turb[...].astype(F32)
    ch = split3(chord[...])
    bl = split3(blade[...])
    for k in range(3):
        fld[4 + k : 5 + k, :] = ch[k].astype(F32)
        fld[7 + 3 * k : 10 + 3 * k, :] = bl[k].astype(F32)
    dense[...] = jnp.zeros_like(dense)
    spots = lax.broadcasted_iota(jnp.int32, (CHUNK, LANES), 0).astype(F32)

    def choose(turn):
        base = (turn * CHUNK).astype(F32) if not isinstance(turn, int) else 0.0
        for j in range(tiles):
            hit = r128[j : j + 1, :] - base == spots
            sel[:, j * LANES : (j + 1) * LANES] = jnp.where(hit, 1.0, 0.0).astype(BF16)
        got_ref[...] = dot(fld[...].astype(BF16), sel[...], NT)

    @pl.when(count > 0)
    def _():
        choose(0)

    small[5].wait()

    def plane(x, carry):
        pltpu.make_async_copy(pops_hbm.at[:, x], pops.at[:, x], sems.at[x]).wait()
        for yb in range(CY // 16):
            g = [pops[i, x, yb * 16 : yb * 16 + 16, :] for i in range(19)]
            rho, mom = moments(g)
            for c in range(3):
                at = pl.multiple_of(c * CX * CY + x * CY + yb * 16, 16)
                high, mid, low = split3(mom[c] / rho)
                vhm[pl.ds(at, 16), 0:LANES] = high
                vhm[pl.ds(at, 16), LANES : 2 * LANES] = mid
                vl[pl.ds(at, 16), :] = low
        return carry

    lax.fori_loop(0, CX, plane, 0)

    def pack(ids, g, flag):
        rho, mom = moments(g)
        solid = flag != 0
        held = [jnp.where(solid, g[OPP[i]], g[i]) for i in ids]
        return held + [rho, *mom, flag.astype(F32)]

    for ids, x, out in ((EAST, CX - 1, east), (WEST, 0, west)):
        for yb in range(CY // 8):
            at = slice(yb * 8, yb * 8 + 8)
            parts = pack(ids, [pops[i, x, at, :] for i in range(19)], flags[x, at, :])
            for k, part in enumerate(parts):
                out[k, at, :] = part
    up = pack(NORTH, [pops[i, :, CY - 1, :] for i in range(19)], flags[:, CY - 1, :])
    down = pack(SOUTH, [pops[i, :, 0, :] for i in range(19)], flags[:, 0, :])
    for k, (a, b) in enumerate(zip(up, down)):
        sibling[112 + 8 * k : 120 + 8 * k, :] = jnp.where(even, a, b)
        across[112 + 8 * k : 120 + 8 * k, :] = jnp.where(even, b, a)

    levels = lax.broadcasted_iota(jnp.int32, (LANES, CHUNK), 0).astype(F32)
    cell_ids = lax.broadcasted_iota(jnp.int32, (CX * CY, CHUNK), 0).astype(F32)

    def chunk(turn, carry):
        @pl.when(turn > 0)
        def _():
            choose(turn)

        got = got_ref[...]
        cell = got[0:1] * CY + got[1:2]
        onez = jnp.where(levels == got[2:3], 1.0, 0.0).astype(BF16)
        twice = jnp.concatenate([onez, onez], axis=0)
        factor = jnp.zeros((1, CHUNK), F32)
        for t in range(gain.shape[0]):
            factor = jnp.where(got[3:4] == t, gain[t], factor)
        factor = factor * (got[4:5] + got[5:6] + got[6:7])
        rel = []
        for c in range(3):
            at = slice(c * CX * CY, (c + 1) * CX * CY)
            lines = dot(vhm[at, :], twice) + dot(vl[at, :], onez)
            sampled = jnp.sum(jnp.where(cell_ids == cell, lines, 0.0), axis=0, keepdims=True)
            speed = got[7 + c : 8 + c] + got[10 + c : 11 + c] + got[13 + c : 14 + c]
            rel.append(sampled - speed)
        size = jnp.sqrt(rel[0] * rel[0] + rel[1] * rel[1] + rel[2] * rel[2] + 0.0001)
        size = -(factor * size)
        pieces = [split3(size * r) for r in rel]
        stack = [pieces[c][k].astype(F32) for k in range(3) for c in range(3)]
        stack = jnp.concatenate(stack + [jnp.zeros((7, CHUNK), F32)], axis=0).astype(BF16)
        spread = dot(stack, sel[...])
        dense[...] += spread[0:3] + spread[3:6] + spread[6:9]
        return carry

    lax.fori_loop(0, (count + CHUNK - 1) // CHUNK, chunk, 0)
    for c in range(3):
        for j in range(tiles):
            sibling[c * tiles + j : c * tiles + j + 1, :] = dense[
                c : c + 1, j * LANES : (j + 1) * LANES
            ]
    sibling[3 * tiles : 112, :] = jnp.zeros((112 - 3 * tiles, LANES), F32)
    across[0:112, :] = sibling[0:112, :]


def known(a, b):
    return jnp.where(a != 0.0, a, b)


def join_kernel(own, beside, beyond, out):
    even = lax.axis_index("gy") % 2 == 0
    out[0:112, :] = known(own[0:112, :], known(beside[0:112, :], beyond[0:112, :]))
    at = 112
    for x, first, second in ((CX - 1, 7, 9), (0, 10, 8)):
        for ids, wanted, south in ((NORTH, first, True), (SOUTH, second, False)):
            for k in [ids.index(wanted), 5, 6, 7, 8, 9]:
                row = slice(112 + 8 * k + x, 113 + 8 * k + x)
                a, b = beside[row, :], beyond[row, :]
                out[at : at + 1, :] = jnp.where(even, b, a) if south else jnp.where(even, a, b)
                at += 1


def finish_kernel(mine, other, out):
    whole = known(mine[...], other[...])
    tiles = out.shape[1] // LANES
    for c in range(3):
        for j in range(tiles):
            row = c * tiles + j
            out[c : c + 1, j * LANES : (j + 1) * LANES] = whole[row : row + 1, :]


FY = 72


READY = 2


def choose_points(rank, base, sel):
    spots = lax.broadcasted_iota(jnp.int32, (CHUNK, LANES), 0).astype(F32)
    for j in range(sel.shape[1] // LANES):
        hit = rank[j : j + 1, :] - base == spots
        sel[:, j * LANES : (j + 1) * LANES] = jnp.where(hit, 1.0, 0.0).astype(BF16)


def prep_kernel(cells, sel, spot, rank, places, count_out, m128, *, total_x, total_y):
    points = cells.shape[1]
    tiles = points // LANES

    def wrapped(v, total):
        v = jnp.where(v < -(total // 2), v + total, v)
        return jnp.where(v >= total // 2, v - total, v)

    px = wrapped(cells[0:1, :] - lax.axis_index("gx") * CX, total_x)
    py = wrapped(cells[1:2, :] - lax.axis_index("gy") * CY, total_y)
    reach = SMEAR + 1
    near = (px >= -reach) & (px < CX + reach) & (py >= -reach) & (py < CY + reach)
    near = jnp.where(near, 1.0, 0.0)
    m128[...] = jnp.zeros_like(m128)
    for j in range(tiles):
        m128[j : j + 1, :] = near[:, j * LANES : (j + 1) * LANES]
    mask = m128[...]
    maskb = mask.astype(BF16)
    rows = lax.broadcasted_iota(jnp.int32, (LANES, LANES), 0)
    cols = lax.broadcasted_iota(jnp.int32, (LANES, LANES), 1)
    before = jnp.where(rows < cols, 1.0, 0.0).astype(BF16)
    above = jnp.where(rows > cols, 1.0, 0.0).astype(BF16)
    inside = dot(maskb, before)
    ahead = jnp.sum(dot(above, maskb), axis=1, keepdims=True)
    rank[...] = jnp.where(mask > 0.0, inside + ahead, -1.0)
    count = jnp.sum(mask).astype(jnp.int32)
    count_out[0] = count
    places[0:1, :] = px.astype(F32)
    places[1:2, :] = py.astype(F32)
    places[2:3, :] = cells[2:3, :].astype(F32)
    places[3:8, :] = jnp.zeros((5, points), F32)
    for k in range(READY):

        @pl.when(count > k * CHUNK)
        def _():
            chosen = sel.at[k]
            choose_points(rank, float(k * CHUNK), chosen)
            spot[k] = dot(places[...].astype(BF16), chosen[...], NT)


def force_kernel(sel_in, spot_in, rank, places, count_in, points_in, out, sel, fld):
    points = fld.shape[1]
    tiles = points // LANES
    count = count_in[0]
    out[...] = jnp.zeros_like(out)

    def kernel_value(cell, point):
        dist = cell - point
        return jnp.where(
            jnp.abs(dist) <= SMEAR, jnp.exp(-((dist / SCALE) * (dist / SCALE))), 0.0
        )

    def iota(size):
        return lax.broadcasted_iota(jnp.int32, (size, CHUNK), 0).astype(F32)

    def spread(chosen, spot):
        got = dot(fld[...].astype(BF16), chosen, NT)
        kx = kernel_value(iota(16) - 1.0, spot[0:1])
        ky = kernel_value(iota(FY) - 1.0, spot[1:2])
        kz = kernel_value(iota(LANES), spot[2:3])
        left = jnp.concatenate(
            [(got[c : 1 + c] + got[3 + c : 4 + c] + got[6 + c : 7 + c]) * ky for c in range(3)],
            axis=0,
        )
        left_high = left.astype(BF16)
        left_low = (left - left_high.astype(F32)).astype(BF16)
        for x in range(0, CX + 2, 2):
            right = jnp.concatenate([kx[x : x + 1] * kz, kx[x + 1 : x + 2] * kz], axis=0)
            right_high = right.astype(BF16)
            right_low = (right - right_high.astype(F32)).astype(BF16)
            field = dot(left_high, right_high, NT) + (
                dot(left_high, right_low, NT) + dot(left_low, right_high, NT)
            )
            for c in range(3):
                part = field[c * FY : (c + 1) * FY]
                out[c, x, :, :] += part[:, :LANES]
                out[c, x + 1, :, :] += part[:, LANES:]

    @pl.when(count > 0)
    def _():
        pieces = split3(points_in[0:112, :])
        for k in range(3):
            piece = pieces[k].astype(F32)
            for c in range(3):
                for j in range(tiles):
                    fld[3 * k + c : 1 + 3 * k + c, j * LANES : (j + 1) * LANES] = piece[
                        c * tiles + j : c * tiles + j + 1, :
                    ]
        fld[9:16, :] = jnp.zeros((7, points), F32)

    ready = (jnp.minimum(count, READY * CHUNK) + CHUNK - 1) // CHUNK

    def chunk(turn, carry):
        spread(sel_in[turn], spot_in[turn])
        return carry

    lax.fori_loop(0, ready, chunk, 0)

    def late(turn, carry):
        choose_points(rank, (turn * CHUNK).astype(F32), sel)
        spread(sel[...], dot(places[...].astype(BF16), sel[...], NT))
        return carry

    lax.fori_loop(READY, (count + CHUNK - 1) // CHUNK, late, 0)


OY = 8


def step_kernel(
    pops, flags, force, from_west, from_east, beside, beyond, west_pts, east_pts, *rest, low, high
):
    out_hbm, out, out_sems = rest[-3:]
    lane = lax.broadcasted_iota(jnp.int32, (8, LANES), 1)
    not_first, not_last = lane > 0, lane < LANES - 1
    first, last = lane == 0, lane == LANES - 1

    def put(i, x, row, val):
        cx, cy, cz = DIRS[i]
        dst = out.at[i, x - low + 1 + cx, pl.ds(OY + row + cy, val.shape[0]), :]
        if cz == 0:
            dst[...] = val
        elif cz == 1:
            pltpu.store(dst, pltpu.roll(val, 1, 1), mask=not_first[: val.shape[0]])
        else:
            pltpu.store(dst, pltpu.roll(val, LANES - 1, 1), mask=not_last[: val.shape[0]])

    def inside(x):
        return low <= x < high

    def force_at(x, yb):
        return [force[c, x + 1, yb * 8 + 1 : yb * 8 + 9, :] for c in range(3)]

    for ids, x, src in ((EAST, low - 1, from_west), (WEST, high, from_east)):
        for yb in range(CY // 8):
            at = slice(yb * 8, yb * 8 + 8)
            if 0 <= x < CX:
                g = [pops[i, x, at, :] for i in range(19)]
                rho, mom = moments(g)
                solid = flags[x, at, :] != 0
                held = [jnp.where(solid, g[OPP[i]], g[i]) for i in ids]
            else:
                rho, mom = src[5, at, :], [src[6 + c, at, :] for c in range(3)]
                solid = src[9, at, :] != 0.0
                held = [src[k, at, :] for k in range(5)]
            hit = Collision(rho, mom, force_at(x, yb))
            for val, i in zip(held, ids):
                put(i, x, yb * 8, jnp.where(solid, val, KEEP * val + hit.one(i)))
    even = lax.axis_index("gy") % 2 == 0
    for ids, y in ((NORTH, -1), (SOUTH, CY)):
        part = []
        for k in range(10):
            a, b = beside[112 + 8 * k : 120 + 8 * k, :], beyond[112 + 8 * k : 120 + 8 * k, :]
            part.append(jnp.where(even, b, a) if y < 0 else jnp.where(even, a, b))
        frc = [force[c, 1 : CX + 1, y + 1, :] for c in range(3)]
        hit = Collision(part[5], part[6:9], frc)
        solid = part[9] != 0.0
        for k, i in enumerate(ids):
            val = jnp.where(solid, part[k], KEEP * part[k] + hit.one(i))
            cx, cy, cz = DIRS[i]
            if cz != 0:
                val = pltpu.roll(val, 1 if cz == 1 else LANES - 1, 1)
            for x in range(CX):
                if not inside(x + cx):
                    continue
                dst = out.at[i, x - low + 1 + cx, OY + y + cy : OY + y + cy + 1, :]
                if cz == 0:
                    dst[...] = val[x : x + 1]
                else:
                    keep = (not_first if cz == 1 else not_last)[0:1]
                    pltpu.store(dst, val[x : x + 1], mask=keep)
    for src, at, i, x, y in (
        (west_pts, 112, 7, -1, -1),
        (west_pts, 118, 9, -1, CY),
        (east_pts, 124, 10, CX, -1),
        (east_pts, 130, 8, CX, CY),
    ):
        if not inside(x + DIRS[i][0]):
            continue
        held, rho = src[at : at + 1, :], src[at + 1 : at + 2, :]
        mom = [src[at + 2 + c : at + 3 + c, :] for c in range(3)]
        solid = src[at + 5 : at + 6, :] != 0.0
        frc = [force[c, x + 1, y + 1 : y + 2, :] for c in range(3)]
        hit = Collision(rho, mom, frc)
        put(i, x, y, jnp.where(solid, held, KEEP * held + hit.one(i)))

    def send(x):
        return pltpu.make_async_copy(
            out.at[:, x - low + 1, OY : OY + CY, :], out_hbm.at[:, x], out_sems.at[x]
        )

    def plane(x, carry):
        for yb in range(CY // 8):
            at = slice(yb * 8, yb * 8 + 8)
            g = [pops[i, x, at, :] for i in range(19)]
            solid = flags[x, at, :] != 0
            rho, mom = moments(g)
            hit = Collision(rho, mom, force_at(x, yb))
            put(0, x, yb * 8, jnp.where(solid, g[0], KEEP * g[0] + hit.base))
            for k in range(1, 19, 2):
                even, odd = hit.terms(k)
                ahead = jnp.where(solid, g[k + 1], KEEP * g[k] + (even + odd))
                back = jnp.where(solid, g[k], KEEP * g[k + 1] + (even - odd))
                put(k, x, yb * 8, ahead)
                put(k + 1, x, yb * 8, back)
                if DIRS[k][2] != 0:
                    up, down = (k, k + 1) if DIRS[k][2] == 1 else (k + 1, k)
                    rising, falling = (ahead, back) if up == k else (back, ahead)
                    rows = pl.ds(OY + yb * 8, 8)
                    pltpu.store(out.at[up, x - low + 1, rows, :], falling, mask=first)
                    pltpu.store(out.at[down, x - low + 1, rows, :], rising, mask=last)

        @pl.when(x > low)
        def _():
            send(x - 1).start()

        return carry

    lax.fori_loop(low, high, plane, 0)
    send(high - 1).start()
    for x in range(low, high):
        send(x).wait()


def from_behind(block, axis, distance):
    count = lax.axis_size(axis)
    return lax.ppermute(block, axis, [((i - distance) % count, i) for i in range(count)])


def exchanged(block, source):
    count_x, count_y = lax.axis_size("gx"), lax.axis_size("gy")
    pairs = []
    for x in range(count_x):
        for y in range(count_y):
            from_x, from_y = source(x, y)
            pairs.append(((from_x % count_x) * count_y + from_y % count_y, x * count_y + y))
    return lax.ppermute(block, ("gx", "gy"), pairs)


def swapped(block):
    return exchanged(block, lambda x, y: (x, y ^ 1))


def fetched(block, first, second):
    return exchanged(
        block, lambda x, y: (x + (second if y % 2 else first)[0], y + (second if y % 2 else first)[1])
    )


def cost(flops):
    return pl.CostEstimate(flops=flops, bytes_accessed=0, transcendentals=0)


def local(populations, solid_flags, point_cells, point_turbine, blade_speed, chord, turbine_gain):
    points = point_cells.shape[1]
    total_x = CX * lax.axis_size("gx")
    total_y = CY * lax.axis_size("gy")
    sds = jax.ShapeDtypeStruct
    params = pltpu.CompilerParams(vmem_limit_bytes=24 * 1024 * 1024)
    light = pltpu.CompilerParams(vmem_limit_bytes=4 * 1024 * 1024)
    compact = [
        pltpu.VMEM((CHUNK, points), BF16),
        pltpu.VMEM((16, points), F32),
        pltpu.VMEM((LANES, LANES), F32),
        pltpu.VMEM((LANES, LANES), F32),
    ]
    sibling, across, east, west, held_pops = pl.pallas_call(
        sample_kernel,
        out_shape=(
            sds((192, LANES), F32),
            sds((192, LANES), F32),
            sds((10, CY, LANES), F32),
            sds((10, CY, LANES), F32),
            sds(populations.shape, F32),
        ),
        in_specs=[HBM] * 7,
        out_specs=(VMEM,) * 5,
        scratch_shapes=[
            pltpu.VMEM((3 * CX * CY, 2 * LANES), BF16),
            pltpu.VMEM((3 * CX * CY, LANES), BF16),
            *compact,
            pltpu.VMEM((3, points), F32),
            pltpu.VMEM((16, CHUNK), F32),
            pltpu.SMEM(turbine_gain.shape, F32),
            pltpu.VMEM(solid_flags.shape, jnp.int32),
            pltpu.VMEM((3, points), jnp.int32),
            pltpu.VMEM((1, points), jnp.int32),
            pltpu.VMEM((1, points), F32),
            pltpu.VMEM((3, points), F32),
            pltpu.SemaphoreType.DMA((CX,)),
            pltpu.SemaphoreType.DMA((6,)),
        ],
        compiler_params=params,
        name="sample",
    )(
        *[
            pltpu.with_memory_space_constraint(arg, pltpu.HBM)
            for arg in (
                turbine_gain, populations, solid_flags, point_cells, point_turbine, chord,
                blade_speed,
            )
        ]
    )
    beside = swapped(sibling)
    beyond = exchanged(across, lambda x, y: (x, y + 1 if y % 2 else y - 1))
    from_west = from_behind(east, "gx", 1)
    from_east = from_behind(west, "gx", -1)
    joined = pl.pallas_call(
        join_kernel,
        out_shape=sds((136, LANES), F32),
        in_specs=[VMEM] * 3,
        out_specs=VMEM,
        compiler_params=light,
        name="join",
    )(sibling, beside, beyond)
    west_pts = from_behind(joined, "gx", 1)
    east_pts = from_behind(joined, "gx", -1)
    near = known(joined[:112], known(west_pts[:112], east_pts[:112]))
    prepared = pl.pallas_call(
        functools.partial(prep_kernel, total_x=total_x, total_y=total_y),
        out_shape=(
            sds((READY, CHUNK, points), BF16),
            sds((READY, 8, CHUNK), F32),
            sds((LANES, LANES), F32),
            sds((8, points), F32),
            sds((1,), jnp.int32),
        ),
        in_specs=[VMEM],
        out_specs=(VMEM, VMEM, VMEM, VMEM, SMEM),
        scratch_shapes=[pltpu.VMEM((LANES, LANES), F32)],
        compiler_params=params,
        cost_estimate=cost(FORCE_FLOPS),
        name="prep",
    )(point_cells)
    force = pl.pallas_call(
        force_kernel,
        out_shape=sds((3, CX + 2, FY, LANES), F32),
        in_specs=[VMEM, VMEM, VMEM, VMEM, SMEM, VMEM],
        out_specs=VMEM,
        scratch_shapes=[pltpu.VMEM((CHUNK, points), BF16), pltpu.VMEM((16, points), F32)],
        compiler_params=params,
        cost_estimate=cost(FORCE_FLOPS),
        name="force",
    )(*prepared, near)
    step_args = (
        held_pops, solid_flags, force, from_west, from_east, beside, beyond, west_pts, east_pts,
    )
    read = None
    for low, high in ((0, CX // 2), (CX // 2, CX)):
        extra = () if read is None else (read,)
        read = pl.pallas_call(
            functools.partial(step_kernel, low=low, high=high),
            out_shape=sds(populations.shape, F32),
            in_specs=[VMEM] * 9 + [HBM] * len(extra),
            out_specs=HBM,
            scratch_shapes=[
                pltpu.VMEM((19, high - low + 2, CY + 16, LANES), F32),
                pltpu.SemaphoreType.DMA((CX,)),
            ],
            input_output_aliases={9: 0} if extra else {},
            compiler_params=params,
            cost_estimate=cost(STEP_FLOPS),
        )(*step_args, *extra)
    got = swapped(near)
    have = known(near, got)
    got = fetched(have, (3, 0), (-3, 0))
    have = known(have, got)
    have = known(have, swapped(have))
    got = fetched(have, (7, 0), (4, 4))
    have = known(have, got)
    have = known(have, swapped(have))
    got = fetched(have, (8, 0), (20, 4))
    have = known(have, got)
    point_force = pl.pallas_call(
        finish_kernel,
        out_shape=sds((3, points), F32),
        in_specs=[VMEM] * 2,
        out_specs=VMEM,
        compiler_params=light,
        name="finish",
    )(have, swapped(have))
    return read, point_force


def solution(mesh):
    in_specs = (P(None, "gx", "gy", None), P("gx", "gy", None), P(), P(), P(), P(), P())
    out_specs = (P(None, "gx", "gy", None), P())
    return jax.shard_map(local, mesh=mesh, in_specs=in_specs, out_specs=out_specs, check_vma=False)
```

```python
import functools

import jax
import jax.numpy as jnp
from jax import lax
from jax.experimental import pallas as pl
from jax.experimental.pallas import tpu as pltpu
from jax.sharding import PartitionSpec as P


SMEAR = 3
RELAX = 0.8
SCALE = 1.5
CHUNK = 256
LANES = 128
DIRS = [
    (0, 0, 0),
    (1, 0, 0),
    (-1, 0, 0),
    (0, 1, 0),
    (0, -1, 0),
    (0, 0, 1),
    (0, 0, -1),
    (1, 1, 0),
    (-1, -1, 0),
    (1, -1, 0),
    (-1, 1, 0),
    (1, 0, 1),
    (-1, 0, -1),
    (1, 0, -1),
    (-1, 0, 1),
    (0, 1, 1),
    (0, -1, -1),
    (0, 1, -1),
    (0, -1, 1),
]
OPP = [0, 2, 1, 4, 3, 6, 5, 8, 7, 10, 9, 12, 11, 14, 13, 16, 15, 18, 17]
EAST = [i for i in range(19) if DIRS[i][0] == 1]
WEST = [i for i in range(19) if DIRS[i][0] == -1]
NORTH = [i for i in range(19) if DIRS[i][1] == 1]
SOUTH = [i for i in range(19) if DIRS[i][1] == -1]
CX, CY = 8, 64
F32, BF16 = jnp.float32, jnp.bfloat16
FORCE_FLOPS = 40_000_000
STEP_FLOPS = 60_000_000
HBM = pl.BlockSpec(memory_space=pltpu.HBM)
VMEM = pl.BlockSpec(memory_space=pltpu.VMEM)
NT = (((1,), (1,)), ((), ()))
NN = (((1,), (0,)), ((), ()))


def dot(a, b, dims=NN):
    return lax.dot_general(a, b, dims, preferred_element_type=F32)


def split3(v):
    high = v.astype(BF16)
    rest = v - high.astype(F32)
    mid = rest.astype(BF16)
    low = (rest - mid.astype(F32)).astype(BF16)
    return high, mid, low


def picked(table, lanes):
    return jnp.take_along_axis(table, lanes, axis=1, mode="promise_in_bounds")


def moments(g):
    s = [None] * 19
    d = [None] * 19
    for k in range(1, 19, 2):
        s[k] = g[k] + g[k + 1]
        d[k] = g[k] - g[k + 1]
    w1, w2 = 1.0 / 18.0, 1.0 / 36.0
    rho = (
        g[0] * (1.0 / 3.0)
        + (s[1] + s[3] + s[5]) * w1
        + ((s[7] + s[9]) + (s[11] + s[13]) + (s[15] + s[17])) * w2
    )
    mx = d[1] * w1 + ((d[7] + d[9]) + (d[11] + d[13])) * w2
    my = d[3] * w1 + ((d[7] - d[9]) + (d[15] + d[17])) * w2
    mz = d[5] * w1 + ((d[11] - d[13]) + (d[15] - d[17])) * w2
    return rho, (mx, my, mz)


def along(c, v):
    total = None
    for comp, part in zip(c, v):
        if comp == 0:
            continue
        if total is None:
            total = part if comp > 0 else -part
        else:
            total = total + part if comp > 0 else total - part
    return total


class Collision:
    def __init__(self, rho, mom, force):
        inv = 1.0 / rho
        amp = 1.0 - 0.5 / RELAX
        vel = [(m + 0.5 * f) * inv for m, f in zip(mom, force)]
        usq = vel[0] * vel[0] + vel[1] * vel[1] + vel[2] * vel[2]
        uf = vel[0] * force[0] + vel[1] * force[1] + vel[2] * force[2]
        heavy = rho * (1.0 / RELAX)
        self.base = heavy - 1.5 * heavy * usq - 3.0 * amp * uf
        self.vel = vel
        rho3, rho45 = 3.0 * heavy, 4.5 * heavy
        self.odd_vec = [rho3 * u + (3.0 * amp) * f for u, f in zip(vel, force)]
        self.even_vec = [rho45 * u + (9.0 * amp) * f for u, f in zip(vel, force)]

    def terms(self, k):
        if k == 0:
            return self.base, None
        c = DIRS[k]
        return self.base + along(c, self.vel) * along(c, self.even_vec), along(c, self.odd_vec)

    def one(self, k):
        first = k if k % 2 == 1 else k - 1
        even, odd = self.terms(first)
        return even + odd if first == k else even - odd


KEEP = 1.0 - 1.0 / RELAX


def sample_kernel(
    gain_hbm, pops_hbm, flags_hbm, cells_hbm, turb_hbm, chord_hbm, blade_hbm,
    sibling, across, east, west, pops,
    vhm, vl, sel, fld, m128, r128, got_ref,
    gain, flags, cells, turb, chord, blade, sems, in_sems,
):
    small = [
        pltpu.make_async_copy(src, dst, in_sems.at[k])
        for k, (src, dst) in enumerate(
            (
                (cells_hbm, cells),
                (turb_hbm, turb.at[0]),
                (chord_hbm, chord.at[0]),
                (blade_hbm, blade),
                (gain_hbm, gain),
                (flags_hbm, flags),
            )
        )
    ]
    for copy in small:
        copy.start()
    for x in range(CX):
        pltpu.make_async_copy(pops_hbm.at[:, x], pops.at[:, x], sems.at[x]).start()
    points = cells.shape[1]
    tiles = points // LANES
    start_x, start_y = lax.axis_index("gx") * CX, lax.axis_index("gy") * CY
    even = lax.axis_index("gy") % 2 == 0
    for copy in small[:5]:
        copy.wait()
    px = cells[0:1, :] - start_x
    py = cells[1:2, :] - start_y
    own = (px >= 0) & (px < CX) & (py >= 0) & (py < CY)
    own = jnp.where(own, 1.0, 0.0)
    m128[...] = jnp.zeros_like(m128)
    for j in range(tiles):
        m128[j : j + 1, :] = own[:, j * LANES : (j + 1) * LANES]
    mask = m128[...]
    maskb = mask.astype(BF16)
    rows = lax.broadcasted_iota(jnp.int32, (LANES, LANES), 0)
    cols = lax.broadcasted_iota(jnp.int32, (LANES, LANES), 1)
    before = jnp.where(rows < cols, 1.0, 0.0).astype(BF16)
    above = jnp.where(rows > cols, 1.0, 0.0).astype(BF16)
    inside = dot(maskb, before)
    ahead = jnp.sum(dot(above, maskb), axis=1, keepdims=True)
    r128[...] = jnp.where(mask > 0.0, inside + ahead, -1.0)
    count = jnp.sum(mask).astype(jnp.int32)

    fld[0:1, :] = px.astype(F32)
    fld[1:2, :] = py.astype(F32)
    fld[2:3, :] = cells[2:3, :].astype(F32)
    fld[3:4, :] = turb[...].astype(F32)
    ch = split3(chord[...])
    bl = split3(blade[...])
    for k in range(3):
        fld[4 + k : 5 + k, :] = ch[k].astype(F32)
        fld[7 + 3 * k : 10 + 3 * k, :] = bl[k].astype(F32)
    spots = lax.broadcasted_iota(jnp.int32, (CHUNK, LANES), 0).astype(F32)

    def choose(turn):
        base = (turn * CHUNK).astype(F32) if not isinstance(turn, int) else 0.0
        for j in range(tiles):
            hit = r128[j : j + 1, :] - base == spots
            sel[:, j * LANES : (j + 1) * LANES] = jnp.where(hit, 1.0, 0.0).astype(BF16)
        got_ref[...] = dot(fld[...].astype(BF16), sel[...], NT)

    @pl.when(count > 0)
    def _():
        choose(0)

    small[5].wait()

    def plane(x, carry):
        pltpu.make_async_copy(pops_hbm.at[:, x], pops.at[:, x], sems.at[x]).wait()
        for yb in range(CY // 16):
            g = [pops[i, x, yb * 16 : yb * 16 + 16, :] for i in range(19)]
            rho, mom = moments(g)
            for c in range(3):
                at = pl.multiple_of(c * CX * CY + x * CY + yb * 16, 16)
                high, mid, low = split3(mom[c] / rho)
                vhm[pl.ds(at, 16), 0:LANES] = high
                vhm[pl.ds(at, 16), LANES : 2 * LANES] = mid
                vl[pl.ds(at, 16), :] = low
        return carry

    lax.fori_loop(0, CX, plane, 0)

    def pack(ids, g, flag):
        rho, mom = moments(g)
        solid = flag != 0
        held = [jnp.where(solid, g[OPP[i]], g[i]) for i in ids]
        return held + [rho, *mom, flag.astype(F32)]

    for ids, x, out in ((EAST, CX - 1, east), (WEST, 0, west)):
        for yb in range(CY // 8):
            at = slice(yb * 8, yb * 8 + 8)
            parts = pack(ids, [pops[i, x, at, :] for i in range(19)], flags[x, at, :])
            for k, part in enumerate(parts):
                out[k, at, :] = part
    up = pack(NORTH, [pops[i, :, CY - 1, :] for i in range(19)], flags[:, CY - 1, :])
    down = pack(SOUTH, [pops[i, :, 0, :] for i in range(19)], flags[:, 0, :])
    for k, (a, b) in enumerate(zip(up, down)):
        sibling[112 + 8 * k : 120 + 8 * k, :] = jnp.where(even, a, b)
        across[112 + 8 * k : 120 + 8 * k, :] = jnp.where(even, b, a)

    levels = lax.broadcasted_iota(jnp.int32, (LANES, CHUNK), 0).astype(F32)
    cell_ids = lax.broadcasted_iota(jnp.int32, (CX * CY, CHUNK), 0).astype(F32)

    def chunk(turn, carry):
        @pl.when(turn > 0)
        def _():
            choose(turn)

        got = got_ref[...]
        cell = got[0:1] * CY + got[1:2]
        onez = jnp.where(levels == got[2:3], 1.0, 0.0).astype(BF16)
        twice = jnp.concatenate([onez, onez], axis=0)
        factor = jnp.zeros((1, CHUNK), F32)
        for t in range(gain.shape[0]):
            factor = jnp.where(got[3:4] == t, gain[t], factor)
        factor = factor * (got[4:5] + got[5:6] + got[6:7])
        rel = []
        for c in range(3):
            at = slice(c * CX * CY, (c + 1) * CX * CY)
            lines = dot(vhm[at, :], twice) + dot(vl[at, :], onez)
            sampled = jnp.sum(jnp.where(cell_ids == cell, lines, 0.0), axis=0, keepdims=True)
            speed = got[7 + c : 8 + c] + got[10 + c : 11 + c] + got[13 + c : 14 + c]
            rel.append(sampled - speed)
        size = jnp.sqrt(rel[0] * rel[0] + rel[1] * rel[1] + rel[2] * rel[2] + 0.0001)
        size = -(factor * size)
        for c in range(3):
            value = size * rel[c]
            low = jnp.broadcast_to(value[:, :LANES], (8, LANES))
            high = jnp.broadcast_to(value[:, LANES:], (8, LANES))
            for t in range(0, tiles, 8):
                count_rows = min(8, tiles - t)
                order = r128[t : t + 8, :].astype(jnp.int32) - turn * CHUNK
                inside_chunk = (order >= 0) & (order < CHUNK)
                spot = order & (LANES - 1)
                got_value = jnp.where(order >= LANES, picked(high, spot), picked(low, spot))
                at = slice(c * tiles + t, c * tiles + t + count_rows)
                sibling[at, :] = jnp.where(inside_chunk, got_value, 0.0)[:count_rows] + sibling[at, :]
        return carry

    sibling[0:112, :] = jnp.zeros((112, LANES), F32)
    lax.fori_loop(0, (count + CHUNK - 1) // CHUNK, chunk, 0)
    across[0:112, :] = sibling[0:112, :]


def known(a, b):
    return jnp.where(a != 0.0, a, b)


def join_kernel(own, beside, beyond, out):
    even = lax.axis_index("gy") % 2 == 0
    out[0:112, :] = known(own[0:112, :], known(beside[0:112, :], beyond[0:112, :]))
    at = 112
    for x, first, second in ((CX - 1, 7, 9), (0, 10, 8)):
        for ids, wanted, south in ((NORTH, first, True), (SOUTH, second, False)):
            for k in [ids.index(wanted), 5, 6, 7, 8, 9]:
                row = slice(112 + 8 * k + x, 113 + 8 * k + x)
                a, b = beside[row, :], beyond[row, :]
                out[at : at + 1, :] = jnp.where(even, b, a) if south else jnp.where(even, a, b)
                at += 1


def finish_kernel(mine, other, out):
    whole = known(mine[...], other[...])
    tiles = out.shape[1] // LANES
    for c in range(3):
        for j in range(tiles):
            row = c * tiles + j
            out[c : c + 1, j * LANES : (j + 1) * LANES] = whole[row : row + 1, :]


FY = 72


READY = 4


def choose_points(rank, base, sel):
    spots = lax.broadcasted_iota(jnp.int32, (CHUNK, LANES), 0).astype(F32)
    for j in range(sel.shape[1] // LANES):
        hit = rank[j : j + 1, :] - base == spots
        sel[:, j * LANES : (j + 1) * LANES] = jnp.where(hit, 1.0, 0.0).astype(BF16)


def prep_kernel(cells, spot, rank, places, sel, m128, *, total_x, total_y):
    points = cells.shape[1]
    tiles = points // LANES

    def wrapped(v, total):
        v = jnp.where(v < -(total // 2), v + total, v)
        return jnp.where(v >= total // 2, v - total, v)

    px = wrapped(cells[0:1, :] - lax.axis_index("gx") * CX, total_x)
    py = wrapped(cells[1:2, :] - lax.axis_index("gy") * CY, total_y)
    reach = SMEAR + 1
    near = (px >= -reach) & (px < CX + reach) & (py >= -reach) & (py < CY + reach)
    near = jnp.where(near, 1.0, 0.0)
    m128[...] = jnp.zeros_like(m128)
    for j in range(tiles):
        m128[j : j + 1, :] = near[:, j * LANES : (j + 1) * LANES]
    mask = m128[...]
    maskb = mask.astype(BF16)
    rows = lax.broadcasted_iota(jnp.int32, (LANES, LANES), 0)
    cols = lax.broadcasted_iota(jnp.int32, (LANES, LANES), 1)
    before = jnp.where(rows < cols, 1.0, 0.0).astype(BF16)
    above = jnp.where(rows > cols, 1.0, 0.0).astype(BF16)
    inside = dot(maskb, before)
    ahead = jnp.sum(dot(above, maskb), axis=1, keepdims=True)
    rank[...] = jnp.where(mask > 0.0, inside + ahead, -1.0)
    count = jnp.sum(mask).astype(jnp.int32)
    places[0:1, :] = px.astype(F32)
    places[1:2, :] = py.astype(F32)
    places[2:3, :] = cells[2:3, :].astype(F32)
    number = lax.broadcasted_iota(jnp.int32, (1, points), 1)
    places[3:4, :] = (number // LANES).astype(F32)
    places[4:5, :] = (number % LANES).astype(F32)
    places[5:6, :] = jnp.ones((1, points), F32)
    places[6:8, :] = jnp.zeros((2, points), F32)

    def chunk(turn, carry):
        choose_points(rank, (turn * CHUNK).astype(F32), sel)
        spot[turn] = dot(places[...].astype(BF16), sel[...], NT)
        return carry

    lax.fori_loop(0, jnp.minimum((count + CHUNK - 1) // CHUNK, READY), chunk, 0)
    spot[READY] = jnp.broadcast_to(count.astype(F32), (8, CHUNK))


def force_kernel(spot_in, rank, places, points_in, out, sel, late):
    tiles = places.shape[1] // LANES
    count = jnp.max(spot_in[READY, 0:1, 0:LANES]).astype(jnp.int32)
    out[...] = jnp.zeros_like(out)

    def kernel_value(cell, point):
        dist = cell - point
        return jnp.where(
            jnp.abs(dist) <= SMEAR, jnp.exp(-((dist / SCALE) * (dist / SCALE))), 0.0
        )

    def iota(size):
        return lax.broadcasted_iota(jnp.int32, (size, CHUNK), 0).astype(F32)

    row_ids = lax.broadcasted_iota(jnp.int32, (8, LANES), 0)

    def spread(spot):
        forces = []
        for c in range(3):
            halves = []
            for h in range(0, CHUNK, LANES):
                row = jnp.broadcast_to(spot[3:4, h : h + LANES].astype(jnp.int32), (8, LANES))
                lane = jnp.broadcast_to(spot[4:5, h : h + LANES].astype(jnp.int32), (8, LANES))
                total = jnp.zeros((8, LANES), F32)
                for t in range(c * tiles // 8, ((c + 1) * tiles - 1) // 8 + 1):
                    value = picked(points_in[8 * t : 8 * t + 8, :], lane)
                    total = jnp.where(row_ids + (8 * t - c * tiles) == row, value, total)
                halves.append(jnp.sum(total, axis=0, keepdims=True))
            force = jnp.concatenate(halves, axis=1)
            forces.append(jnp.where(spot[5:6] > 0.5, force, 0.0))
        kx = kernel_value(iota(16) - 1.0, spot[0:1])
        ky = kernel_value(iota(FY) - 1.0, spot[1:2])
        kz = kernel_value(iota(LANES), spot[2:3])
        left = jnp.concatenate([f * ky for f in forces], axis=0)
        left_high = left.astype(BF16)
        left_low = (left - left_high.astype(F32)).astype(BF16)
        left_both = jnp.concatenate([left_high, left_low], axis=0)
        lines = 3 * FY
        for x in range(0, CX + 2, 2):
            right = jnp.concatenate([kx[x : x + 1] * kz, kx[x + 1 : x + 2] * kz], axis=0)
            right_high = right.astype(BF16)
            right_low = (right - right_high.astype(F32)).astype(BF16)
            both = dot(left_both, right_high, NT)
            field = both[:lines] + (dot(left_high, right_low, NT) + both[lines:])
            for c in range(3):
                part = field[c * FY : (c + 1) * FY]
                out[c, x, :, :] += part[:, :LANES]
                out[c, x + 1, :, :] += part[:, LANES:]

    chunks = (count + CHUNK - 1) // CHUNK

    def chunk(turn, carry):
        @pl.when(turn >= READY)
        def _():
            choose_points(rank, (turn * CHUNK).astype(F32), sel)
            late[...] = dot(places[...].astype(BF16), sel[...], NT)

        @pl.when(turn < READY)
        def _():
            late[...] = spot_in[turn]

        spread(late[...])
        return carry

    lax.fori_loop(0, chunks, chunk, 0)


OY = 8


def step_kernel(
    pops, flags, force, from_west, from_east, beside, beyond, west_pts, east_pts, *rest, low, high
):
    out_hbm, out, out_sems = rest[-3:]
    lane = lax.broadcasted_iota(jnp.int32, (8, LANES), 1)
    not_first, not_last = lane > 0, lane < LANES - 1
    first, last = lane == 0, lane == LANES - 1

    def put(i, x, row, val):
        cx, cy, cz = DIRS[i]
        dst = out.at[i, x - low + 1 + cx, pl.ds(OY + row + cy, val.shape[0]), :]
        if cz == 0:
            dst[...] = val
        elif cz == 1:
            pltpu.store(dst, pltpu.roll(val, 1, 1), mask=not_first[: val.shape[0]])
        else:
            pltpu.store(dst, pltpu.roll(val, LANES - 1, 1), mask=not_last[: val.shape[0]])

    def inside(x):
        return low <= x < high

    def force_at(x, yb):
        return [force[c, x + 1, yb * 8 + 1 : yb * 8 + 9, :] for c in range(3)]

    for ids, x, src in ((EAST, low - 1, from_west), (WEST, high, from_east)):
        for yb in range(CY // 8):
            at = slice(yb * 8, yb * 8 + 8)
            if 0 <= x < CX:
                g = [pops[i, x, at, :] for i in range(19)]
                rho, mom = moments(g)
                solid = flags[x, at, :] != 0
                held = [jnp.where(solid, g[OPP[i]], g[i]) for i in ids]
            else:
                rho, mom = src[5, at, :], [src[6 + c, at, :] for c in range(3)]
                solid = src[9, at, :] != 0.0
                held = [src[k, at, :] for k in range(5)]
            hit = Collision(rho, mom, force_at(x, yb))
            for val, i in zip(held, ids):
                put(i, x, yb * 8, jnp.where(solid, val, KEEP * val + hit.one(i)))
    even = lax.axis_index("gy") % 2 == 0
    for ids, y in ((NORTH, -1), (SOUTH, CY)):
        part = []
        for k in range(10):
            a, b = beside[112 + 8 * k : 120 + 8 * k, :], beyond[112 + 8 * k : 120 + 8 * k, :]
            part.append(jnp.where(even, b, a) if y < 0 else jnp.where(even, a, b))
        frc = [force[c, 1 : CX + 1, y + 1, :] for c in range(3)]
        hit = Collision(part[5], part[6:9], frc)
        solid = part[9] != 0.0
        for k, i in enumerate(ids):
            val = jnp.where(solid, part[k], KEEP * part[k] + hit.one(i))
            cx, cy, cz = DIRS[i]
            if cz != 0:
                val = pltpu.roll(val, 1 if cz == 1 else LANES - 1, 1)
            for x in range(CX):
                if not inside(x + cx):
                    continue
                dst = out.at[i, x - low + 1 + cx, OY + y + cy : OY + y + cy + 1, :]
                if cz == 0:
                    dst[...] = val[x : x + 1]
                else:
                    keep = (not_first if cz == 1 else not_last)[0:1]
                    pltpu.store(dst, val[x : x + 1], mask=keep)
    for src, at, i, x, y in (
        (west_pts, 112, 7, -1, -1),
        (west_pts, 118, 9, -1, CY),
        (east_pts, 124, 10, CX, -1),
        (east_pts, 130, 8, CX, CY),
    ):
        if not inside(x + DIRS[i][0]):
            continue
        held, rho = src[at : at + 1, :], src[at + 1 : at + 2, :]
        mom = [src[at + 2 + c : at + 3 + c, :] for c in range(3)]
        solid = src[at + 5 : at + 6, :] != 0.0
        frc = [force[c, x + 1, y + 1 : y + 2, :] for c in range(3)]
        hit = Collision(rho, mom, frc)
        put(i, x, y, jnp.where(solid, held, KEEP * held + hit.one(i)))

    def send(x):
        return pltpu.make_async_copy(
            out.at[:, x - low + 1, OY : OY + CY, :], out_hbm.at[:, x], out_sems.at[x]
        )

    def plane(x, carry):
        for yb in range(CY // 8):
            at = slice(yb * 8, yb * 8 + 8)
            g = [pops[i, x, at, :] for i in range(19)]
            solid = flags[x, at, :] != 0
            rho, mom = moments(g)
            hit = Collision(rho, mom, force_at(x, yb))
            put(0, x, yb * 8, jnp.where(solid, g[0], KEEP * g[0] + hit.base))
            for k in range(1, 19, 2):
                even, odd = hit.terms(k)
                ahead = jnp.where(solid, g[k + 1], KEEP * g[k] + (even + odd))
                back = jnp.where(solid, g[k], KEEP * g[k + 1] + (even - odd))
                put(k, x, yb * 8, ahead)
                put(k + 1, x, yb * 8, back)
                if DIRS[k][2] != 0:
                    up, down = (k, k + 1) if DIRS[k][2] == 1 else (k + 1, k)
                    rising, falling = (ahead, back) if up == k else (back, ahead)
                    rows = pl.ds(OY + yb * 8, 8)
                    pltpu.store(out.at[up, x - low + 1, rows, :], falling, mask=first)
                    pltpu.store(out.at[down, x - low + 1, rows, :], rising, mask=last)

        @pl.when(x > low)
        def _():
            send(x - 1).start()

        return carry

    lax.fori_loop(low, high, plane, 0)
    send(high - 1).start()
    for x in range(low, high):
        send(x).wait()


def from_behind(block, axis, distance):
    count = lax.axis_size(axis)
    return lax.ppermute(block, axis, [((i - distance) % count, i) for i in range(count)])


def exchanged(block, source):
    count_x, count_y = lax.axis_size("gx"), lax.axis_size("gy")
    pairs = []
    for x in range(count_x):
        for y in range(count_y):
            from_x, from_y = source(x, y)
            pairs.append(((from_x % count_x) * count_y + from_y % count_y, x * count_y + y))
    return lax.ppermute(block, ("gx", "gy"), pairs)


def swapped(block):
    return exchanged(block, lambda x, y: (x, y ^ 1))


def fetched(block, first, second):
    return exchanged(
        block, lambda x, y: (x + (second if y % 2 else first)[0], y + (second if y % 2 else first)[1])
    )


def cost(flops):
    return pl.CostEstimate(flops=flops, bytes_accessed=0, transcendentals=0)


def local(populations, solid_flags, point_cells, point_turbine, blade_speed, chord, turbine_gain):
    points = point_cells.shape[1]
    total_x = CX * lax.axis_size("gx")
    total_y = CY * lax.axis_size("gy")
    sds = jax.ShapeDtypeStruct
    params = pltpu.CompilerParams(vmem_limit_bytes=24 * 1024 * 1024)
    light = pltpu.CompilerParams(vmem_limit_bytes=4 * 1024 * 1024)
    compact = [
        pltpu.VMEM((CHUNK, points), BF16),
        pltpu.VMEM((16, points), F32),
        pltpu.VMEM((LANES, LANES), F32),
        pltpu.VMEM((LANES, LANES), F32),
    ]
    sibling, across, east, west, held_pops = pl.pallas_call(
        sample_kernel,
        out_shape=(
            sds((192, LANES), F32),
            sds((192, LANES), F32),
            sds((10, CY, LANES), F32),
            sds((10, CY, LANES), F32),
            sds(populations.shape, F32),
        ),
        in_specs=[HBM] * 7,
        out_specs=(VMEM,) * 5,
        scratch_shapes=[
            pltpu.VMEM((3 * CX * CY, 2 * LANES), BF16),
            pltpu.VMEM((3 * CX * CY, LANES), BF16),
            *compact,
            pltpu.VMEM((16, CHUNK), F32),
            pltpu.SMEM(turbine_gain.shape, F32),
            pltpu.VMEM(solid_flags.shape, jnp.int32),
            pltpu.VMEM((3, points), jnp.int32),
            pltpu.VMEM((1, points), jnp.int32),
            pltpu.VMEM((1, points), F32),
            pltpu.VMEM((3, points), F32),
            pltpu.SemaphoreType.DMA((CX,)),
            pltpu.SemaphoreType.DMA((6,)),
        ],
        compiler_params=params,
        name="sample",
    )(
        *[
            pltpu.with_memory_space_constraint(arg, pltpu.HBM)
            for arg in (
                turbine_gain, populations, solid_flags, point_cells, point_turbine, chord,
                blade_speed,
            )
        ]
    )
    beside = swapped(sibling)
    beyond = exchanged(across, lambda x, y: (x, y + 1 if y % 2 else y - 1))
    from_west = from_behind(east, "gx", 1)
    from_east = from_behind(west, "gx", -1)
    joined = pl.pallas_call(
        join_kernel,
        out_shape=sds((136, LANES), F32),
        in_specs=[VMEM] * 3,
        out_specs=VMEM,
        compiler_params=light,
        name="join",
    )(sibling, beside, beyond)
    west_pts = from_behind(joined, "gx", 1)
    east_pts = from_behind(joined, "gx", -1)
    near = known(joined[:112], known(west_pts[:112], east_pts[:112]))
    prepared = pl.pallas_call(
        functools.partial(prep_kernel, total_x=total_x, total_y=total_y),
        out_shape=(
            sds((READY + 1, 8, CHUNK), F32),
            sds((LANES, LANES), F32),
            sds((8, points), F32),
        ),
        in_specs=[VMEM],
        out_specs=(VMEM, VMEM, VMEM),
        scratch_shapes=[pltpu.VMEM((CHUNK, points), BF16), pltpu.VMEM((LANES, LANES), F32)],
        compiler_params=params,
        cost_estimate=cost(FORCE_FLOPS),
        name="prep",
    )(point_cells)
    force = pl.pallas_call(
        force_kernel,
        out_shape=sds((3, CX + 2, FY, LANES), F32),
        in_specs=[VMEM] * 4,
        out_specs=VMEM,
        scratch_shapes=[pltpu.VMEM((CHUNK, points), BF16), pltpu.VMEM((8, CHUNK), F32)],
        compiler_params=params,
        cost_estimate=cost(FORCE_FLOPS),
        name="force",
    )(*prepared, near)
    step_args = (
        held_pops, solid_flags, force, from_west, from_east, beside, beyond, west_pts, east_pts,
    )
    read = None
    for low, high in ((0, CX // 2), (CX // 2, CX)):
        extra = () if read is None else (read,)
        read = pl.pallas_call(
            functools.partial(step_kernel, low=low, high=high),
            out_shape=sds(populations.shape, F32),
            in_specs=[VMEM] * 9 + [HBM] * len(extra),
            out_specs=HBM,
            scratch_shapes=[
                pltpu.VMEM((19, high - low + 2, CY + 16, LANES), F32),
                pltpu.SemaphoreType.DMA((CX,)),
            ],
            input_output_aliases={9: 0} if extra else {},
            compiler_params=params,
            cost_estimate=cost(STEP_FLOPS),
        )(*step_args, *extra)
    got = swapped(near)
    have = known(near, got)
    got = fetched(have, (3, 0), (-3, 0))
    have = known(have, got)
    have = known(have, swapped(have))
    got = fetched(have, (7, 0), (4, 4))
    have = known(have, got)
    have = known(have, swapped(have))
    got = fetched(have, (8, 0), (20, 4))
    have = known(have, got)
    point_force = pl.pallas_call(
        finish_kernel,
        out_shape=sds((3, points), F32),
        in_specs=[VMEM] * 2,
        out_specs=VMEM,
        compiler_params=light,
        name="finish",
    )(have, swapped(have))
    return read, point_force


def solution(mesh):
    in_specs = (P(None, "gx", "gy", None), P("gx", "gy", None), P(), P(), P(), P(), P())
    out_specs = (P(None, "gx", "gy", None), P())
    return jax.shard_map(local, mesh=mesh, in_specs=in_specs, out_specs=out_specs, check_vma=False)
```

```python
import functools

import jax
import jax.numpy as jnp
from jax import lax
from jax.experimental import pallas as pl
from jax.experimental.pallas import tpu as pltpu
from jax.sharding import PartitionSpec as P


SMEAR = 3
RELAX = 0.8
SCALE = 1.5
CHUNK = 256
LANES = 128
DIRS = [
    (0, 0, 0),
    (1, 0, 0),
    (-1, 0, 0),
    (0, 1, 0),
    (0, -1, 0),
    (0, 0, 1),
    (0, 0, -1),
    (1, 1, 0),
    (-1, -1, 0),
    (1, -1, 0),
    (-1, 1, 0),
    (1, 0, 1),
    (-1, 0, -1),
    (1, 0, -1),
    (-1, 0, 1),
    (0, 1, 1),
    (0, -1, -1),
    (0, 1, -1),
    (0, -1, 1),
]
OPP = [0, 2, 1, 4, 3, 6, 5, 8, 7, 10, 9, 12, 11, 14, 13, 16, 15, 18, 17]
EAST = [i for i in range(19) if DIRS[i][0] == 1]
WEST = [i for i in range(19) if DIRS[i][0] == -1]
NORTH = [i for i in range(19) if DIRS[i][1] == 1]
SOUTH = [i for i in range(19) if DIRS[i][1] == -1]
CX, CY = 8, 64
F32, BF16 = jnp.float32, jnp.bfloat16
FORCE_FLOPS = 40_000_000
STEP_FLOPS = 60_000_000
HBM = pl.BlockSpec(memory_space=pltpu.HBM)
VMEM = pl.BlockSpec(memory_space=pltpu.VMEM)
NT = (((1,), (1,)), ((), ()))
NN = (((1,), (0,)), ((), ()))


def dot(a, b, dims=NN):
    return lax.dot_general(a, b, dims, preferred_element_type=F32)


def split3(v):
    high = v.astype(BF16)
    rest = v - high.astype(F32)
    mid = rest.astype(BF16)
    low = (rest - mid.astype(F32)).astype(BF16)
    return high, mid, low


def picked(table, lanes):
    return jnp.take_along_axis(table, lanes, axis=1, mode="promise_in_bounds")


def moments(g):
    s = [None] * 19
    d = [None] * 19
    for k in range(1, 19, 2):
        s[k] = g[k] + g[k + 1]
        d[k] = g[k] - g[k + 1]
    w1, w2 = 1.0 / 18.0, 1.0 / 36.0
    rho = (
        g[0] * (1.0 / 3.0)
        + (s[1] + s[3] + s[5]) * w1
        + ((s[7] + s[9]) + (s[11] + s[13]) + (s[15] + s[17])) * w2
    )
    mx = d[1] * w1 + ((d[7] + d[9]) + (d[11] + d[13])) * w2
    my = d[3] * w1 + ((d[7] - d[9]) + (d[15] + d[17])) * w2
    mz = d[5] * w1 + ((d[11] - d[13]) + (d[15] - d[17])) * w2
    return rho, (mx, my, mz)


def along(c, v):
    total = None
    for comp, part in zip(c, v):
        if comp == 0:
            continue
        if total is None:
            total = part if comp > 0 else -part
        else:
            total = total + part if comp > 0 else total - part
    return total


class Collision:
    def __init__(self, rho, mom, force):
        inv = 1.0 / rho
        amp = 1.0 - 0.5 / RELAX
        vel = [(m + 0.5 * f) * inv for m, f in zip(mom, force)]
        usq = vel[0] * vel[0] + vel[1] * vel[1] + vel[2] * vel[2]
        uf = vel[0] * force[0] + vel[1] * force[1] + vel[2] * force[2]
        heavy = rho * (1.0 / RELAX)
        self.base = heavy - 1.5 * heavy * usq - 3.0 * amp * uf
        self.vel = vel
        rho3, rho45 = 3.0 * heavy, 4.5 * heavy
        self.odd_vec = [rho3 * u + (3.0 * amp) * f for u, f in zip(vel, force)]
        self.even_vec = [rho45 * u + (9.0 * amp) * f for u, f in zip(vel, force)]

    def terms(self, k):
        if k == 0:
            return self.base, None
        c = DIRS[k]
        return self.base + along(c, self.vel) * along(c, self.even_vec), along(c, self.odd_vec)

    def one(self, k):
        first = k if k % 2 == 1 else k - 1
        even, odd = self.terms(first)
        return even + odd if first == k else even - odd


KEEP = 1.0 - 1.0 / RELAX


def choose_points(rank, base, sel):
    spots = lax.broadcasted_iota(jnp.int32, (CHUNK, LANES), 0).astype(F32)
    for j in range(sel.shape[1] // LANES):
        hit = rank[j : j + 1, :] - base == spots
        sel[:, j * LANES : (j + 1) * LANES] = jnp.where(hit, 1.0, 0.0).astype(BF16)


def number_points(wanted, m128, rank):
    m128[...] = jnp.zeros_like(m128)
    for j in range(wanted.shape[1] // LANES):
        m128[j : j + 1, :] = wanted[:, j * LANES : (j + 1) * LANES]
    mask = m128[...]
    maskb = mask.astype(BF16)
    rows = lax.broadcasted_iota(jnp.int32, (LANES, LANES), 0)
    cols = lax.broadcasted_iota(jnp.int32, (LANES, LANES), 1)
    before = jnp.where(rows < cols, 1.0, 0.0).astype(BF16)
    above = jnp.where(rows > cols, 1.0, 0.0).astype(BF16)
    inside = dot(maskb, before)
    ahead = jnp.sum(dot(above, maskb), axis=1, keepdims=True)
    rank[...] = jnp.where(mask > 0.0, inside + ahead, -1.0)
    return jnp.sum(mask).astype(jnp.int32)


def dense_kernel(
    gain_hbm, pops_hbm, flags_hbm, cells_hbm, turb_hbm, chord_hbm, blade_hbm,
    sibling, across, east, west, pops, vhm, vl, fld, r128, got_ref,
    sel, m128, gain, flags, cells, turb, chord, blade, sems, in_sems,
):
    small = [
        pltpu.make_async_copy(src, dst, in_sems.at[k])
        for k, (src, dst) in enumerate(
            (
                (cells_hbm, cells),
                (turb_hbm, turb.at[0]),
                (chord_hbm, chord.at[0]),
                (blade_hbm, blade),
                (gain_hbm, gain),
                (flags_hbm, flags),
            )
        )
    ]
    for copy in small:
        copy.start()
    for x in range(CX):
        pltpu.make_async_copy(pops_hbm.at[:, x], pops.at[:, x], sems.at[x]).start()
    points = cells.shape[1]
    start_x, start_y = lax.axis_index("gx") * CX, lax.axis_index("gy") * CY
    even = lax.axis_index("gy") % 2 == 0
    for copy in small[:5]:
        copy.wait()
    px = cells[0:1, :] - start_x
    py = cells[1:2, :] - start_y
    own = (px >= 0) & (px < CX) & (py >= 0) & (py < CY)
    count = number_points(jnp.where(own, 1.0, 0.0), m128, r128)

    @pl.when(count > 0)
    def _():
        fld[0:1, :] = px.astype(F32)
        fld[1:2, :] = py.astype(F32)
        fld[2:3, :] = cells[2:3, :].astype(F32)
        owner = turb[...]
        gains = jnp.zeros((1, points), F32)
        for t in range(gain.shape[0]):
            gains = jnp.where(owner == t, gain[t], gains)
        factor = split3(chord[...] * gains)
        bl = split3(blade[...])
        for k in range(3):
            fld[3 + k : 4 + k, :] = factor[k].astype(F32)
            fld[6 + 3 * k : 9 + 3 * k, :] = bl[k].astype(F32)
        fld[15:16, :] = jnp.zeros((1, points), F32)
        choose_points(r128, 0.0, sel)
        got_ref[...] = dot(fld[...].astype(BF16), sel[...], NT)

    small[5].wait()

    def plane(x, carry):
        pltpu.make_async_copy(pops_hbm.at[:, x], pops.at[:, x], sems.at[x]).wait()
        for yb in range(CY // 16):
            g = [pops[i, x, yb * 16 : yb * 16 + 16, :] for i in range(19)]
            rho, mom = moments(g)
            for c in range(3):
                at = pl.multiple_of(c * CX * CY + x * CY + yb * 16, 16)
                high, mid, low = split3(mom[c] / rho)
                vhm[pl.ds(at, 16), 0:LANES] = high
                vhm[pl.ds(at, 16), LANES : 2 * LANES] = mid
                vl[pl.ds(at, 16), :] = low
        return carry

    lax.fori_loop(0, CX, plane, 0)

    def pack(ids, g, flag):
        rho, mom = moments(g)
        solid = flag != 0
        held = [jnp.where(solid, g[OPP[i]], g[i]) for i in ids]
        return held + [rho, *mom, flag.astype(F32)]

    for ids, x, out in ((EAST, CX - 1, east), (WEST, 0, west)):
        for yb in range(CY // 8):
            at = slice(yb * 8, yb * 8 + 8)
            parts = pack(ids, [pops[i, x, at, :] for i in range(19)], flags[x, at, :])
            for k, part in enumerate(parts):
                out[k, at, :] = part
    up = pack(NORTH, [pops[i, :, CY - 1, :] for i in range(19)], flags[:, CY - 1, :])
    down = pack(SOUTH, [pops[i, :, 0, :] for i in range(19)], flags[:, 0, :])
    for k, (a, b) in enumerate(zip(up, down)):
        sibling[8 * k : 8 * k + 8, :] = jnp.where(even, a, b)
        across[8 * k : 8 * k + 8, :] = jnp.where(even, b, a)


def sample_kernel(rows_sibling, rows_across, vhm, vl, fld, r128, got_in, sibling, across, sel, got_ref):
    tiles = fld.shape[1] // LANES
    count = jnp.max(r128[...]).astype(jnp.int32) + 1
    levels = lax.broadcasted_iota(jnp.int32, (LANES, CHUNK), 0).astype(F32)
    cell_ids = lax.broadcasted_iota(jnp.int32, (CX * CY, CHUNK), 0).astype(F32)

    def chunk(turn, carry):
        @pl.when(turn == 0)
        def _():
            got_ref[...] = got_in[...]

        @pl.when(turn > 0)
        def _():
            choose_points(r128, (turn * CHUNK).astype(F32), sel)
            got_ref[...] = dot(fld[...].astype(BF16), sel[...], NT)

        got = got_ref[...]
        cell = got[0:1] * CY + got[1:2]
        onez = jnp.where(levels == got[2:3], 1.0, 0.0).astype(BF16)
        twice = jnp.concatenate([onez, onez], axis=0)
        factor = got[3:4] + got[4:5] + got[5:6]
        rel = []
        for c in range(3):
            at = slice(c * CX * CY, (c + 1) * CX * CY)
            lines = dot(vhm[at, :], twice) + dot(vl[at, :], onez)
            sampled = jnp.sum(jnp.where(cell_ids == cell, lines, 0.0), axis=0, keepdims=True)
            speed = got[6 + c : 7 + c] + got[9 + c : 10 + c] + got[12 + c : 13 + c]
            rel.append(sampled - speed)
        size = jnp.sqrt(rel[0] * rel[0] + rel[1] * rel[1] + rel[2] * rel[2] + 0.0001)
        size = -(factor * size)
        for c in range(3):
            value = size * rel[c]
            low = jnp.broadcast_to(value[:, :LANES], (8, LANES))
            high = jnp.broadcast_to(value[:, LANES:], (8, LANES))
            for t in range(0, tiles, 8):
                count_rows = min(8, tiles - t)
                order = r128[t : t + 8, :].astype(jnp.int32) - turn * CHUNK
                inside_chunk = (order >= 0) & (order < CHUNK)
                spot = order & (LANES - 1)
                got_value = jnp.where(order >= LANES, picked(high, spot), picked(low, spot))
                at = slice(c * tiles + t, c * tiles + t + count_rows)
                sibling[at, :] = jnp.where(inside_chunk, got_value, 0.0)[:count_rows] + sibling[at, :]
        return carry

    sibling[0:112, :] = jnp.zeros((112, LANES), F32)
    lax.fori_loop(0, (count + CHUNK - 1) // CHUNK, chunk, 0)
    across[0:112, :] = sibling[0:112, :]
    sibling[112:192, :] = rows_sibling[...]
    across[112:192, :] = rows_across[...]


def known(a, b):
    return jnp.where(a != 0.0, a, b)


def join_kernel(own, beside, beyond, out):
    even = lax.axis_index("gy") % 2 == 0
    out[0:112, :] = known(own[0:112, :], known(beside[0:112, :], beyond[0:112, :]))
    at = 112
    for x, first, second in ((CX - 1, 7, 9), (0, 10, 8)):
        for ids, wanted, south in ((NORTH, first, True), (SOUTH, second, False)):
            for k in [ids.index(wanted), 5, 6, 7, 8, 9]:
                row = slice(112 + 8 * k + x, 113 + 8 * k + x)
                a, b = beside[row, :], beyond[row, :]
                out[at : at + 1, :] = jnp.where(even, b, a) if south else jnp.where(even, a, b)
                at += 1


def finish_kernel(mine, other, out):
    whole = known(mine[...], other[...])
    tiles = out.shape[1] // LANES
    for c in range(3):
        for j in range(tiles):
            row = c * tiles + j
            out[c : c + 1, j * LANES : (j + 1) * LANES] = whole[row : row + 1, :]


FY = 72


READY = 4


def prep_kernel(cells, spot, rank, places, sel, m128, *, total_x, total_y):
    points = cells.shape[1]

    def wrapped(v, total):
        v = jnp.where(v < -(total // 2), v + total, v)
        return jnp.where(v >= total // 2, v - total, v)

    px = wrapped(cells[0:1, :] - lax.axis_index("gx") * CX, total_x)
    py = wrapped(cells[1:2, :] - lax.axis_index("gy") * CY, total_y)
    reach = SMEAR + 1
    near = (px >= -reach) & (px < CX + reach) & (py >= -reach) & (py < CY + reach)
    count = number_points(jnp.where(near, 1.0, 0.0), m128, rank)
    places[0:1, :] = px.astype(F32)
    places[1:2, :] = py.astype(F32)
    places[2:3, :] = cells[2:3, :].astype(F32)
    number = lax.broadcasted_iota(jnp.int32, (1, points), 1)
    places[3:4, :] = (number // LANES).astype(F32)
    places[4:5, :] = (number % LANES).astype(F32)
    places[5:6, :] = jnp.ones((1, points), F32)
    places[6:8, :] = jnp.zeros((2, points), F32)

    def chunk(turn, carry):
        choose_points(rank, (turn * CHUNK).astype(F32), sel)
        spot[turn] = dot(places[...].astype(BF16), sel[...], NT)
        return carry

    lax.fori_loop(0, jnp.minimum((count + CHUNK - 1) // CHUNK, READY), chunk, 0)
    spot[READY] = jnp.broadcast_to(count.astype(F32), (8, CHUNK))


def force_kernel(spot_in, rank, places, points_in, out, sel, late):
    tiles = places.shape[1] // LANES
    count = jnp.max(spot_in[READY, 0:1, 0:LANES]).astype(jnp.int32)
    out[...] = jnp.zeros_like(out)

    def kernel_value(cell, point):
        dist = cell - point
        return jnp.where(
            jnp.abs(dist) <= SMEAR, jnp.exp(-((dist / SCALE) * (dist / SCALE))), 0.0
        )

    def iota(size):
        return lax.broadcasted_iota(jnp.int32, (size, CHUNK), 0).astype(F32)

    row_ids = lax.broadcasted_iota(jnp.int32, (8, LANES), 0)

    def spread(spot):
        forces = []
        for c in range(3):
            halves = []
            for h in range(0, CHUNK, LANES):
                row = jnp.broadcast_to(spot[3:4, h : h + LANES].astype(jnp.int32), (8, LANES))
                lane = jnp.broadcast_to(spot[4:5, h : h + LANES].astype(jnp.int32), (8, LANES))
                total = jnp.zeros((8, LANES), F32)
                for t in range(c * tiles // 8, ((c + 1) * tiles - 1) // 8 + 1):
                    value = picked(points_in[8 * t : 8 * t + 8, :], lane)
                    total = jnp.where(row_ids + (8 * t - c * tiles) == row, value, total)
                halves.append(jnp.sum(total, axis=0, keepdims=True))
            force = jnp.concatenate(halves, axis=1)
            forces.append(jnp.where(spot[5:6] > 0.5, force, 0.0))
        kx = kernel_value(iota(16) - 1.0, spot[0:1])
        ky = kernel_value(iota(FY) - 1.0, spot[1:2])
        kz = kernel_value(iota(LANES), spot[2:3])
        left = jnp.concatenate([f * ky for f in forces], axis=0)
        left_high = left.astype(BF16)
        left_low = (left - left_high.astype(F32)).astype(BF16)
        left_both = jnp.concatenate([left_high, left_low], axis=0)
        lines = 3 * FY
        for x in range(0, CX + 2, 2):
            right = jnp.concatenate([kx[x : x + 1] * kz, kx[x + 1 : x + 2] * kz], axis=0)
            right_high = right.astype(BF16)
            right_low = (right - right_high.astype(F32)).astype(BF16)
            both = dot(left_both, right_high, NT)
            field = both[:lines] + (dot(left_high, right_low, NT) + both[lines:])
            for c in range(3):
                part = field[c * FY : (c + 1) * FY]
                out[c, x, :, :] += part[:, :LANES]
                out[c, x + 1, :, :] += part[:, LANES:]

    chunks = (count + CHUNK - 1) // CHUNK

    def chunk(turn, carry):
        @pl.when(turn >= READY)
        def _():
            choose_points(rank, (turn * CHUNK).astype(F32), sel)
            late[...] = dot(places[...].astype(BF16), sel[...], NT)

        @pl.when(turn < READY)
        def _():
            late[...] = spot_in[turn]

        spread(late[...])
        return carry

    lax.fori_loop(0, chunks, chunk, 0)


OY = 8


def step_kernel(
    pops, flags, force, from_west, from_east, beside, beyond, west_pts, east_pts, *rest, low, high
):
    out_hbm, out, out_sems = rest[-3:]
    lane = lax.broadcasted_iota(jnp.int32, (8, LANES), 1)
    not_first, not_last = lane > 0, lane < LANES - 1
    first, last = lane == 0, lane == LANES - 1

    def put(i, x, row, val):
        cx, cy, cz = DIRS[i]
        dst = out.at[i, x - low + 1 + cx, pl.ds(OY + row + cy, val.shape[0]), :]
        if cz == 0:
            dst[...] = val
        elif cz == 1:
            pltpu.store(dst, pltpu.roll(val, 1, 1), mask=not_first[: val.shape[0]])
        else:
            pltpu.store(dst, pltpu.roll(val, LANES - 1, 1), mask=not_last[: val.shape[0]])

    def inside(x):
        return low <= x < high

    def force_at(x, yb):
        return [force[c, x + 1, yb * 8 + 1 : yb * 8 + 9, :] for c in range(3)]

    for ids, x, src in ((EAST, low - 1, from_west), (WEST, high, from_east)):
        for yb in range(CY // 8):
            at = slice(yb * 8, yb * 8 + 8)
            if 0 <= x < CX:
                g = [pops[i, x, at, :] for i in range(19)]
                rho, mom = moments(g)
                solid = flags[x, at, :] != 0
                held = [jnp.where(solid, g[OPP[i]], g[i]) for i in ids]
            else:
                rho, mom = src[5, at, :], [src[6 + c, at, :] for c in range(3)]
                solid = src[9, at, :] != 0.0
                held = [src[k, at, :] for k in range(5)]
            hit = Collision(rho, mom, force_at(x, yb))
            for val, i in zip(held, ids):
                put(i, x, yb * 8, jnp.where(solid, val, KEEP * val + hit.one(i)))
    even = lax.axis_index("gy") % 2 == 0
    for ids, y in ((NORTH, -1), (SOUTH, CY)):
        part = []
        for k in range(10):
            a, b = beside[112 + 8 * k : 120 + 8 * k, :], beyond[112 + 8 * k : 120 + 8 * k, :]
            part.append(jnp.where(even, b, a) if y < 0 else jnp.where(even, a, b))
        frc = [force[c, 1 : CX + 1, y + 1, :] for c in range(3)]
        hit = Collision(part[5], part[6:9], frc)
        solid = part[9] != 0.0
        for k, i in enumerate(ids):
            val = jnp.where(solid, part[k], KEEP * part[k] + hit.one(i))
            cx, cy, cz = DIRS[i]
            if cz != 0:
                val = pltpu.roll(val, 1 if cz == 1 else LANES - 1, 1)
            for x in range(CX):
                if not inside(x + cx):
                    continue
                dst = out.at[i, x - low + 1 + cx, OY + y + cy : OY + y + cy + 1, :]
                if cz == 0:
                    dst[...] = val[x : x + 1]
                else:
                    keep = (not_first if cz == 1 else not_last)[0:1]
                    pltpu.store(dst, val[x : x + 1], mask=keep)
    for src, at, i, x, y in (
        (west_pts, 112, 7, -1, -1),
        (west_pts, 118, 9, -1, CY),
        (east_pts, 124, 10, CX, -1),
        (east_pts, 130, 8, CX, CY),
    ):
        if not inside(x + DIRS[i][0]):
            continue
        held, rho = src[at : at + 1, :], src[at + 1 : at + 2, :]
        mom = [src[at + 2 + c : at + 3 + c, :] for c in range(3)]
        solid = src[at + 5 : at + 6, :] != 0.0
        frc = [force[c, x + 1, y + 1 : y + 2, :] for c in range(3)]
        hit = Collision(rho, mom, frc)
        put(i, x, y, jnp.where(solid, held, KEEP * held + hit.one(i)))

    def send(x):
        return pltpu.make_async_copy(
            out.at[:, x - low + 1, OY : OY + CY, :], out_hbm.at[:, x], out_sems.at[x]
        )

    def plane(x, carry):
        for yb in range(CY // 8):
            at = slice(yb * 8, yb * 8 + 8)
            g = [pops[i, x, at, :] for i in range(19)]
            solid = flags[x, at, :] != 0
            rho, mom = moments(g)
            hit = Collision(rho, mom, force_at(x, yb))
            put(0, x, yb * 8, jnp.where(solid, g[0], KEEP * g[0] + hit.base))
            for k in range(1, 19, 2):
                even, odd = hit.terms(k)
                ahead = jnp.where(solid, g[k + 1], KEEP * g[k] + (even + odd))
                back = jnp.where(solid, g[k], KEEP * g[k + 1] + (even - odd))
                put(k, x, yb * 8, ahead)
                put(k + 1, x, yb * 8, back)
                if DIRS[k][2] != 0:
                    up, down = (k, k + 1) if DIRS[k][2] == 1 else (k + 1, k)
                    rising, falling = (ahead, back) if up == k else (back, ahead)
                    rows = pl.ds(OY + yb * 8, 8)
                    pltpu.store(out.at[up, x - low + 1, rows, :], falling, mask=first)
                    pltpu.store(out.at[down, x - low + 1, rows, :], rising, mask=last)

        @pl.when(x > low)
        def _():
            send(x - 1).start()

        return carry

    lax.fori_loop(low, high, plane, 0)
    send(high - 1).start()
    for x in range(low, high):
        send(x).wait()


def from_behind(block, axis, distance):
    count = lax.axis_size(axis)
    return lax.ppermute(block, axis, [((i - distance) % count, i) for i in range(count)])


def exchanged(block, source):
    count_x, count_y = lax.axis_size("gx"), lax.axis_size("gy")
    pairs = []
    for x in range(count_x):
        for y in range(count_y):
            from_x, from_y = source(x, y)
            pairs.append(((from_x % count_x) * count_y + from_y % count_y, x * count_y + y))
    return lax.ppermute(block, ("gx", "gy"), pairs)


def swapped(block):
    return exchanged(block, lambda x, y: (x, y ^ 1))


def fetched(block, first, second):
    return exchanged(
        block, lambda x, y: (x + (second if y % 2 else first)[0], y + (second if y % 2 else first)[1])
    )


def cost(flops):
    return pl.CostEstimate(flops=flops, bytes_accessed=0, transcendentals=0)


def local(populations, solid_flags, point_cells, point_turbine, blade_speed, chord, turbine_gain):
    points = point_cells.shape[1]
    total_x = CX * lax.axis_size("gx")
    total_y = CY * lax.axis_size("gy")
    sds = jax.ShapeDtypeStruct
    params = pltpu.CompilerParams(vmem_limit_bytes=24 * 1024 * 1024)
    light = pltpu.CompilerParams(vmem_limit_bytes=4 * 1024 * 1024)
    rows_sibling, rows_across, east, west, held_pops, vhm, vl, fld, rank, got = pl.pallas_call(
        dense_kernel,
        out_shape=(
            sds((80, LANES), F32),
            sds((80, LANES), F32),
            sds((10, CY, LANES), F32),
            sds((10, CY, LANES), F32),
            sds(populations.shape, F32),
            sds((3 * CX * CY, 2 * LANES), BF16),
            sds((3 * CX * CY, LANES), BF16),
            sds((16, points), F32),
            sds((LANES, LANES), F32),
            sds((16, CHUNK), F32),
        ),
        in_specs=[HBM] * 7,
        out_specs=(VMEM,) * 10,
        scratch_shapes=[
            pltpu.VMEM((CHUNK, points), BF16),
            pltpu.VMEM((LANES, LANES), F32),
            pltpu.SMEM(turbine_gain.shape, F32),
            pltpu.VMEM(solid_flags.shape, jnp.int32),
            pltpu.VMEM((3, points), jnp.int32),
            pltpu.VMEM((1, points), jnp.int32),
            pltpu.VMEM((1, points), F32),
            pltpu.VMEM((3, points), F32),
            pltpu.SemaphoreType.DMA((CX,)),
            pltpu.SemaphoreType.DMA((6,)),
        ],
        compiler_params=params,
        name="dense",
    )(
        *[
            pltpu.with_memory_space_constraint(arg, pltpu.HBM)
            for arg in (
                turbine_gain, populations, solid_flags, point_cells, point_turbine, chord,
                blade_speed,
            )
        ]
    )
    from_west = from_behind(east, "gx", 1)
    from_east = from_behind(west, "gx", -1)
    sibling, across = pl.pallas_call(
        sample_kernel,
        out_shape=(sds((192, LANES), F32), sds((192, LANES), F32)),
        in_specs=[VMEM] * 7,
        out_specs=(VMEM, VMEM),
        scratch_shapes=[pltpu.VMEM((CHUNK, points), BF16), pltpu.VMEM((16, CHUNK), F32)],
        compiler_params=params,
        cost_estimate=cost(FORCE_FLOPS),
        name="sample",
    )(rows_sibling, rows_across, vhm, vl, fld, rank, got)
    beside = swapped(sibling)
    beyond = exchanged(across, lambda x, y: (x, y + 1 if y % 2 else y - 1))
    joined = pl.pallas_call(
        join_kernel,
        out_shape=sds((136, LANES), F32),
        in_specs=[VMEM] * 3,
        out_specs=VMEM,
        compiler_params=light,
        name="join",
    )(sibling, beside, beyond)
    west_pts = from_behind(joined, "gx", 1)
    east_pts = from_behind(joined, "gx", -1)
    near = known(joined[:112], known(west_pts[:112], east_pts[:112]))
    prepared = pl.pallas_call(
        functools.partial(prep_kernel, total_x=total_x, total_y=total_y),
        out_shape=(
            sds((READY + 1, 8, CHUNK), F32),
            sds((LANES, LANES), F32),
            sds((8, points), F32),
        ),
        in_specs=[VMEM],
        out_specs=(VMEM, VMEM, VMEM),
        scratch_shapes=[pltpu.VMEM((CHUNK, points), BF16), pltpu.VMEM((LANES, LANES), F32)],
        compiler_params=params,
        cost_estimate=cost(FORCE_FLOPS),
        name="prep",
    )(point_cells)
    force = pl.pallas_call(
        force_kernel,
        out_shape=sds((3, CX + 2, FY, LANES), F32),
        in_specs=[VMEM] * 4,
        out_specs=VMEM,
        scratch_shapes=[pltpu.VMEM((CHUNK, points), BF16), pltpu.VMEM((8, CHUNK), F32)],
        compiler_params=params,
        cost_estimate=cost(FORCE_FLOPS),
        name="force",
    )(*prepared, near)
    step_args = (
        held_pops, solid_flags, force, from_west, from_east, beside, beyond, west_pts, east_pts,
    )
    read = None
    for low, high in ((0, CX // 2), (CX // 2, CX)):
        extra = () if read is None else (read,)
        read = pl.pallas_call(
            functools.partial(step_kernel, low=low, high=high),
            out_shape=sds(populations.shape, F32),
            in_specs=[VMEM] * 9 + [HBM] * len(extra),
            out_specs=HBM,
            scratch_shapes=[
                pltpu.VMEM((19, high - low + 2, CY + 16, LANES), F32),
                pltpu.SemaphoreType.DMA((CX,)),
            ],
            input_output_aliases={9: 0} if extra else {},
            compiler_params=params,
            cost_estimate=cost(STEP_FLOPS),
        )(*step_args, *extra)
    got = swapped(near)
    have = known(near, got)
    got = fetched(have, (3, 0), (-3, 0))
    have = known(have, got)
    have = known(have, swapped(have))
    got = fetched(have, (7, 0), (4, 4))
    have = known(have, got)
    have = known(have, swapped(have))
    got = fetched(have, (8, 0), (20, 4))
    have = known(have, got)
    point_force = pl.pallas_call(
        finish_kernel,
        out_shape=sds((3, points), F32),
        in_specs=[VMEM] * 2,
        out_specs=VMEM,
        compiler_params=light,
        name="finish",
    )(have, swapped(have))
    return read, point_force


def solution(mesh):
    in_specs = (P(None, "gx", "gy", None), P("gx", "gy", None), P(), P(), P(), P(), P())
    out_specs = (P(None, "gx", "gy", None), P())
    return jax.shard_map(local, mesh=mesh, in_specs=in_specs, out_specs=out_specs, check_vma=False)
```

```python
import functools

import jax
import jax.numpy as jnp
from jax import lax
from jax.experimental import pallas as pl
from jax.experimental.pallas import tpu as pltpu
from jax.sharding import PartitionSpec as P


SMEAR = 3
RELAX = 0.8
SCALE = 1.5
CHUNK = 256
LANES = 128
DIRS = [
    (0, 0, 0),
    (1, 0, 0),
    (-1, 0, 0),
    (0, 1, 0),
    (0, -1, 0),
    (0, 0, 1),
    (0, 0, -1),
    (1, 1, 0),
    (-1, -1, 0),
    (1, -1, 0),
    (-1, 1, 0),
    (1, 0, 1),
    (-1, 0, -1),
    (1, 0, -1),
    (-1, 0, 1),
    (0, 1, 1),
    (0, -1, -1),
    (0, 1, -1),
    (0, -1, 1),
]
OPP = [0, 2, 1, 4, 3, 6, 5, 8, 7, 10, 9, 12, 11, 14, 13, 16, 15, 18, 17]
EAST = [i for i in range(19) if DIRS[i][0] == 1]
WEST = [i for i in range(19) if DIRS[i][0] == -1]
NORTH = [i for i in range(19) if DIRS[i][1] == 1]
SOUTH = [i for i in range(19) if DIRS[i][1] == -1]
CX, CY = 8, 64
F32, BF16 = jnp.float32, jnp.bfloat16
FORCE_FLOPS = 40_000_000
STEP_FLOPS = 60_000_000
HBM = pl.BlockSpec(memory_space=pltpu.HBM)
VMEM = pl.BlockSpec(memory_space=pltpu.VMEM)
NT = (((1,), (1,)), ((), ()))
NN = (((1,), (0,)), ((), ()))


def dot(a, b, dims=NN):
    return lax.dot_general(a, b, dims, preferred_element_type=F32)


def split3(v):
    high = v.astype(BF16)
    rest = v - high.astype(F32)
    mid = rest.astype(BF16)
    low = (rest - mid.astype(F32)).astype(BF16)
    return high, mid, low


def picked(table, lanes):
    return jnp.take_along_axis(table, lanes, axis=1, mode="promise_in_bounds")


def moments(g):
    s = [None] * 19
    d = [None] * 19
    for k in range(1, 19, 2):
        s[k] = g[k] + g[k + 1]
        d[k] = g[k] - g[k + 1]
    w1, w2 = 1.0 / 18.0, 1.0 / 36.0
    rho = (
        g[0] * (1.0 / 3.0)
        + (s[1] + s[3] + s[5]) * w1
        + ((s[7] + s[9]) + (s[11] + s[13]) + (s[15] + s[17])) * w2
    )
    mx = d[1] * w1 + ((d[7] + d[9]) + (d[11] + d[13])) * w2
    my = d[3] * w1 + ((d[7] - d[9]) + (d[15] + d[17])) * w2
    mz = d[5] * w1 + ((d[11] - d[13]) + (d[15] - d[17])) * w2
    return rho, (mx, my, mz)


def along(c, v):
    total = None
    for comp, part in zip(c, v):
        if comp == 0:
            continue
        if total is None:
            total = part if comp > 0 else -part
        else:
            total = total + part if comp > 0 else total - part
    return total


class Collision:
    def __init__(self, rho, mom, force):
        inv = 1.0 / rho
        amp = 1.0 - 0.5 / RELAX
        vel = [(m + 0.5 * f) * inv for m, f in zip(mom, force)]
        usq = vel[0] * vel[0] + vel[1] * vel[1] + vel[2] * vel[2]
        uf = vel[0] * force[0] + vel[1] * force[1] + vel[2] * force[2]
        heavy = rho * (1.0 / RELAX)
        self.base = heavy - 1.5 * heavy * usq - 3.0 * amp * uf
        self.vel = vel
        rho3, rho45 = 3.0 * heavy, 4.5 * heavy
        self.odd_vec = [rho3 * u + (3.0 * amp) * f for u, f in zip(vel, force)]
        self.even_vec = [rho45 * u + (9.0 * amp) * f for u, f in zip(vel, force)]

    def terms(self, k):
        if k == 0:
            return self.base, None
        c = DIRS[k]
        return self.base + along(c, self.vel) * along(c, self.even_vec), along(c, self.odd_vec)

    def one(self, k):
        first = k if k % 2 == 1 else k - 1
        even, odd = self.terms(first)
        return even + odd if first == k else even - odd


KEEP = 1.0 - 1.0 / RELAX


def sample_kernel(
    gain_hbm, pops_hbm, flags_hbm, cells_hbm, turb_hbm, chord_hbm, blade_hbm,
    sibling, across, east, west, pops,
    vhm, vl, sel, fld, m128, r128, got_ref,
    gain, flags, cells, turb, chord, blade, sems, in_sems,
):
    small = [
        pltpu.make_async_copy(src, dst, in_sems.at[k])
        for k, (src, dst) in enumerate(
            (
                (cells_hbm, cells),
                (turb_hbm, turb.at[0]),
                (chord_hbm, chord.at[0]),
                (blade_hbm, blade),
                (gain_hbm, gain),
                (flags_hbm, flags),
            )
        )
    ]
    for copy in small:
        copy.start()
    for x in range(CX):
        pltpu.make_async_copy(pops_hbm.at[:, x], pops.at[:, x], sems.at[x]).start()
    points = cells.shape[1]
    tiles = points // LANES
    start_x, start_y = lax.axis_index("gx") * CX, lax.axis_index("gy") * CY
    even = lax.axis_index("gy") % 2 == 0
    for copy in small[:5]:
        copy.wait()
    px = cells[0:1, :] - start_x
    py = cells[1:2, :] - start_y
    own = (px >= 0) & (px < CX) & (py >= 0) & (py < CY)
    own = jnp.where(own, 1.0, 0.0)
    m128[...] = jnp.zeros_like(m128)
    for j in range(tiles):
        m128[j : j + 1, :] = own[:, j * LANES : (j + 1) * LANES]
    mask = m128[...]
    maskb = mask.astype(BF16)
    rows = lax.broadcasted_iota(jnp.int32, (LANES, LANES), 0)
    cols = lax.broadcasted_iota(jnp.int32, (LANES, LANES), 1)
    before = jnp.where(rows < cols, 1.0, 0.0).astype(BF16)
    above = jnp.where(rows > cols, 1.0, 0.0).astype(BF16)
    inside = dot(maskb, before)
    ahead = jnp.sum(dot(above, maskb), axis=1, keepdims=True)
    r128[...] = jnp.where(mask > 0.0, inside + ahead, -1.0)
    count = jnp.sum(mask).astype(jnp.int32)

    fld[0:1, :] = px.astype(F32)
    fld[1:2, :] = py.astype(F32)
    fld[2:3, :] = cells[2:3, :].astype(F32)
    fld[3:4, :] = turb[...].astype(F32)
    ch = split3(chord[...])
    bl = split3(blade[...])
    for k in range(3):
        fld[4 + k : 5 + k, :] = ch[k].astype(F32)
        fld[7 + 3 * k : 10 + 3 * k, :] = bl[k].astype(F32)
    spots = lax.broadcasted_iota(jnp.int32, (CHUNK, LANES), 0).astype(F32)

    def choose(turn):
        base = (turn * CHUNK).astype(F32) if not isinstance(turn, int) else 0.0
        for j in range(tiles):
            hit = r128[j : j + 1, :] - base == spots
            sel[:, j * LANES : (j + 1) * LANES] = jnp.where(hit, 1.0, 0.0).astype(BF16)
        got_ref[...] = dot(fld[...].astype(BF16), sel[...], NT)

    @pl.when(count > 0)
    def _():
        choose(0)

    small[5].wait()

    def plane(x, carry):
        pltpu.make_async_copy(pops_hbm.at[:, x], pops.at[:, x], sems.at[x]).wait()
        for yb in range(CY // 16):
            g = [pops[i, x, yb * 16 : yb * 16 + 16, :] for i in range(19)]
            rho, mom = moments(g)
            for c in range(3):
                at = pl.multiple_of(c * CX * CY + x * CY + yb * 16, 16)
                high, mid, low = split3(mom[c] / rho)
                vhm[pl.ds(at, 16), 0:LANES] = high
                vhm[pl.ds(at, 16), LANES : 2 * LANES] = mid
                vl[pl.ds(at, 16), :] = low
        return carry

    lax.fori_loop(0, CX, plane, 0)

    def pack(ids, g, flag):
        rho, mom = moments(g)
        solid = flag != 0
        held = [jnp.where(solid, g[OPP[i]], g[i]) for i in ids]
        return held + [rho, *mom, flag.astype(F32)]

    for ids, x, out in ((EAST, CX - 1, east), (WEST, 0, west)):
        for yb in range(CY // 8):
            at = slice(yb * 8, yb * 8 + 8)
            parts = pack(ids, [pops[i, x, at, :] for i in range(19)], flags[x, at, :])
            for k, part in enumerate(parts):
                out[k, at, :] = part
    up = pack(NORTH, [pops[i, :, CY - 1, :] for i in range(19)], flags[:, CY - 1, :])
    down = pack(SOUTH, [pops[i, :, 0, :] for i in range(19)], flags[:, 0, :])
    for k, (a, b) in enumerate(zip(up, down)):
        sibling[112 + 8 * k : 120 + 8 * k, :] = jnp.where(even, a, b)
        across[112 + 8 * k : 120 + 8 * k, :] = jnp.where(even, b, a)

    levels = lax.broadcasted_iota(jnp.int32, (LANES, CHUNK), 0).astype(F32)
    cell_ids = lax.broadcasted_iota(jnp.int32, (CX * CY, CHUNK), 0).astype(F32)

    def chunk(turn, carry):
        @pl.when(turn > 0)
        def _():
            choose(turn)

        got = got_ref[...]
        cell = got[0:1] * CY + got[1:2]
        onez = jnp.where(levels == got[2:3], 1.0, 0.0).astype(BF16)
        twice = jnp.concatenate([onez, onez], axis=0)
        factor = jnp.zeros((1, CHUNK), F32)
        for t in range(gain.shape[0]):
            factor = jnp.where(got[3:4] == t, gain[t], factor)
        factor = factor * (got[4:5] + got[5:6] + got[6:7])
        rel = []
        for c in range(3):
            at = slice(c * CX * CY, (c + 1) * CX * CY)
            lines = dot(vhm[at, :], twice) + dot(vl[at, :], onez)
            sampled = jnp.sum(jnp.where(cell_ids == cell, lines, 0.0), axis=0, keepdims=True)
            speed = got[7 + c : 8 + c] + got[10 + c : 11 + c] + got[13 + c : 14 + c]
            rel.append(sampled - speed)
        size = jnp.sqrt(rel[0] * rel[0] + rel[1] * rel[1] + rel[2] * rel[2] + 0.0001)
        size = -(factor * size)
        for c in range(3):
            value = size * rel[c]
            low = jnp.broadcast_to(value[:, :LANES], (8, LANES))
            high = jnp.broadcast_to(value[:, LANES:], (8, LANES))
            for t in range(0, tiles, 8):
                count_rows = min(8, tiles - t)
                order = r128[t : t + 8, :].astype(jnp.int32) - turn * CHUNK
                inside_chunk = (order >= 0) & (order < CHUNK)
                spot = order & (LANES - 1)
                got_value = jnp.where(order >= LANES, picked(high, spot), picked(low, spot))
                at = slice(c * tiles + t, c * tiles + t + count_rows)
                sibling[at, :] = jnp.where(inside_chunk, got_value, 0.0)[:count_rows] + sibling[at, :]
        return carry

    sibling[0:112, :] = jnp.zeros((112, LANES), F32)
    lax.fori_loop(0, (count + CHUNK - 1) // CHUNK, chunk, 0)
    across[0:112, :] = sibling[0:112, :]


def known(a, b):
    return jnp.where(a != 0.0, a, b)


def join_kernel(own, beside, beyond, out):
    even = lax.axis_index("gy") % 2 == 0
    out[0:112, :] = known(own[0:112, :], known(beside[0:112, :], beyond[0:112, :]))
    at = 112
    for x, first, second in ((CX - 1, 7, 9), (0, 10, 8)):
        for ids, wanted, south in ((NORTH, first, True), (SOUTH, second, False)):
            for k in [ids.index(wanted), 5, 6, 7, 8, 9]:
                row = slice(112 + 8 * k + x, 113 + 8 * k + x)
                a, b = beside[row, :], beyond[row, :]
                out[at : at + 1, :] = jnp.where(even, b, a) if south else jnp.where(even, a, b)
                at += 1


def finish_kernel(mine, other, out):
    whole = known(mine[...], other[...])
    tiles = out.shape[1] // LANES
    for c in range(3):
        for j in range(tiles):
            row = c * tiles + j
            out[c : c + 1, j * LANES : (j + 1) * LANES] = whole[row : row + 1, :]


FY = 72


READY = 4


def choose_points(rank, base, sel):
    spots = lax.broadcasted_iota(jnp.int32, (CHUNK, LANES), 0).astype(F32)
    for j in range(sel.shape[1] // LANES):
        hit = rank[j : j + 1, :] - base == spots
        sel[:, j * LANES : (j + 1) * LANES] = jnp.where(hit, 1.0, 0.0).astype(BF16)


def prep_kernel(cells, spot, rank, places, sel, m128, *, total_x, total_y):
    points = cells.shape[1]
    tiles = points // LANES

    def wrapped(v, total):
        v = jnp.where(v < -(total // 2), v + total, v)
        return jnp.where(v >= total // 2, v - total, v)

    px = wrapped(cells[0:1, :] - lax.axis_index("gx") * CX, total_x)
    py = wrapped(cells[1:2, :] - lax.axis_index("gy") * CY, total_y)
    reach = SMEAR + 1
    near = (px >= -reach) & (px < CX + reach) & (py >= -reach) & (py < CY + reach)
    near = jnp.where(near, 1.0, 0.0)
    m128[...] = jnp.zeros_like(m128)
    for j in range(tiles):
        m128[j : j + 1, :] = near[:, j * LANES : (j + 1) * LANES]
    mask = m128[...]
    maskb = mask.astype(BF16)
    rows = lax.broadcasted_iota(jnp.int32, (LANES, LANES), 0)
    cols = lax.broadcasted_iota(jnp.int32, (LANES, LANES), 1)
    before = jnp.where(rows < cols, 1.0, 0.0).astype(BF16)
    above = jnp.where(rows > cols, 1.0, 0.0).astype(BF16)
    inside = dot(maskb, before)
    ahead = jnp.sum(dot(above, maskb), axis=1, keepdims=True)
    rank[...] = jnp.where(mask > 0.0, inside + ahead, -1.0)
    count = jnp.sum(mask).astype(jnp.int32)
    places[0:1, :] = px.astype(F32)
    places[1:2, :] = py.astype(F32)
    places[2:3, :] = cells[2:3, :].astype(F32)
    number = lax.broadcasted_iota(jnp.int32, (1, points), 1)
    places[3:4, :] = (number // LANES).astype(F32)
    places[4:5, :] = (number % LANES).astype(F32)
    places[5:6, :] = jnp.ones((1, points), F32)
    places[6:8, :] = jnp.zeros((2, points), F32)

    def chunk(turn, carry):
        choose_points(rank, (turn * CHUNK).astype(F32), sel)
        spot[turn] = dot(places[...].astype(BF16), sel[...], NT)
        return carry

    lax.fori_loop(0, jnp.minimum((count + CHUNK - 1) // CHUNK, READY), chunk, 0)
    spot[READY] = jnp.broadcast_to(count.astype(F32), (8, CHUNK))


def force_kernel(spot_in, rank, places, points_in, out, sel, late):
    tiles = places.shape[1] // LANES
    count = jnp.max(spot_in[READY, 0:1, 0:LANES]).astype(jnp.int32)
    out[...] = jnp.zeros_like(out)

    def kernel_value(cell, point):
        dist = cell - point
        return jnp.where(
            jnp.abs(dist) <= SMEAR, jnp.exp(-((dist / SCALE) * (dist / SCALE))), 0.0
        )

    def iota(size):
        return lax.broadcasted_iota(jnp.int32, (size, CHUNK), 0).astype(F32)

    row_ids = lax.broadcasted_iota(jnp.int32, (8, LANES), 0)

    def spread(spot):
        forces = []
        for c in range(3):
            halves = []
            for h in range(0, CHUNK, LANES):
                row = jnp.broadcast_to(spot[3:4, h : h + LANES].astype(jnp.int32), (8, LANES))
                lane = jnp.broadcast_to(spot[4:5, h : h + LANES].astype(jnp.int32), (8, LANES))
                total = jnp.zeros((8, LANES), F32)
                for t in range(c * tiles // 8, ((c + 1) * tiles - 1) // 8 + 1):
                    value = picked(points_in[8 * t : 8 * t + 8, :], lane)
                    total = jnp.where(row_ids + (8 * t - c * tiles) == row, value, total)
                halves.append(jnp.sum(total, axis=0, keepdims=True))
            force = jnp.concatenate(halves, axis=1)
            forces.append(jnp.where(spot[5:6] > 0.5, force, 0.0))
        kx = kernel_value(iota(16) - 1.0, spot[0:1])
        ky = kernel_value(iota(FY) - 1.0, spot[1:2])
        kz = kernel_value(iota(LANES), spot[2:3])
        left = jnp.concatenate([f * ky for f in forces], axis=0)
        left_high = left.astype(BF16)
        left_low = (left - left_high.astype(F32)).astype(BF16)
        left_both = jnp.concatenate([left_high, left_low], axis=0)
        lines = 3 * FY
        for x in range(0, CX + 2, 2):
            right = jnp.concatenate([kx[x : x + 1] * kz, kx[x + 1 : x + 2] * kz], axis=0)
            right_high = right.astype(BF16)
            right_low = (right - right_high.astype(F32)).astype(BF16)
            both = dot(left_both, right_high, NT)
            field = both[:lines] + (dot(left_high, right_low, NT) + both[lines:])
            for c in range(3):
                part = field[c * FY : (c + 1) * FY]
                out[c, x, :, :] += part[:, :LANES]
                out[c, x + 1, :, :] += part[:, LANES:]

    chunks = (count + CHUNK - 1) // CHUNK

    def chunk(turn, carry):
        @pl.when(turn >= READY)
        def _():
            choose_points(rank, (turn * CHUNK).astype(F32), sel)
            late[...] = dot(places[...].astype(BF16), sel[...], NT)

        @pl.when(turn < READY)
        def _():
            late[...] = spot_in[turn]

        spread(late[...])
        return carry

    lax.fori_loop(0, chunks, chunk, 0)


OY = 8


def step_kernel(
    pops, flags, force, from_west, from_east, beside, beyond, west_pts, east_pts, *rest, low, high
):
    out_hbm, out, out_sems = rest[-3:]
    lane = lax.broadcasted_iota(jnp.int32, (8, LANES), 1)
    not_first, not_last = lane > 0, lane < LANES - 1
    first, last = lane == 0, lane == LANES - 1

    def put(i, x, row, val):
        cx, cy, cz = DIRS[i]
        dst = out.at[i, x - low + 1 + cx, pl.ds(OY + row + cy, val.shape[0]), :]
        if cz == 0:
            dst[...] = val
        elif cz == 1:
            pltpu.store(dst, pltpu.roll(val, 1, 1), mask=not_first[: val.shape[0]])
        else:
            pltpu.store(dst, pltpu.roll(val, LANES - 1, 1), mask=not_last[: val.shape[0]])

    def inside(x):
        return low <= x < high

    def force_at(x, yb):
        return [force[c, x + 1, yb * 8 + 1 : yb * 8 + 9, :] for c in range(3)]

    for ids, x, src in ((EAST, low - 1, from_west), (WEST, high, from_east)):
        for yb in range(CY // 8):
            at = slice(yb * 8, yb * 8 + 8)
            if 0 <= x < CX:
                g = [pops[i, x, at, :] for i in range(19)]
                rho, mom = moments(g)
                solid = flags[x, at, :] != 0
                held = [jnp.where(solid, g[OPP[i]], g[i]) for i in ids]
            else:
                rho, mom = src[5, at, :], [src[6 + c, at, :] for c in range(3)]
                solid = src[9, at, :] != 0.0
                held = [src[k, at, :] for k in range(5)]
            hit = Collision(rho, mom, force_at(x, yb))
            for val, i in zip(held, ids):
                put(i, x, yb * 8, jnp.where(solid, val, KEEP * val + hit.one(i)))
    even = lax.axis_index("gy") % 2 == 0
    for ids, y in ((NORTH, -1), (SOUTH, CY)):
        part = []
        for k in range(10):
            a, b = beside[112 + 8 * k : 120 + 8 * k, :], beyond[112 + 8 * k : 120 + 8 * k, :]
            part.append(jnp.where(even, b, a) if y < 0 else jnp.where(even, a, b))
        frc = [force[c, 1 : CX + 1, y + 1, :] for c in range(3)]
        hit = Collision(part[5], part[6:9], frc)
        solid = part[9] != 0.0
        for k, i in enumerate(ids):
            val = jnp.where(solid, part[k], KEEP * part[k] + hit.one(i))
            cx, cy, cz = DIRS[i]
            if cz != 0:
                val = pltpu.roll(val, 1 if cz == 1 else LANES - 1, 1)
            for x in range(CX):
                if not inside(x + cx):
                    continue
                dst = out.at[i, x - low + 1 + cx, OY + y + cy : OY + y + cy + 1, :]
                if cz == 0:
                    dst[...] = val[x : x + 1]
                else:
                    keep = (not_first if cz == 1 else not_last)[0:1]
                    pltpu.store(dst, val[x : x + 1], mask=keep)
    for src, at, i, x, y in (
        (west_pts, 112, 7, -1, -1),
        (west_pts, 118, 9, -1, CY),
        (east_pts, 124, 10, CX, -1),
        (east_pts, 130, 8, CX, CY),
    ):
        if not inside(x + DIRS[i][0]):
            continue
        held, rho = src[at : at + 1, :], src[at + 1 : at + 2, :]
        mom = [src[at + 2 + c : at + 3 + c, :] for c in range(3)]
        solid = src[at + 5 : at + 6, :] != 0.0
        frc = [force[c, x + 1, y + 1 : y + 2, :] for c in range(3)]
        hit = Collision(rho, mom, frc)
        put(i, x, y, jnp.where(solid, held, KEEP * held + hit.one(i)))

    def send(x):
        return pltpu.make_async_copy(
            out.at[:, x - low + 1, OY : OY + CY, :], out_hbm.at[:, x], out_sems.at[x]
        )

    def plane(x, carry):
        for yb in range(CY // 8):
            at = slice(yb * 8, yb * 8 + 8)
            g = [pops[i, x, at, :] for i in range(19)]
            solid = flags[x, at, :] != 0
            rho, mom = moments(g)
            hit = Collision(rho, mom, force_at(x, yb))
            put(0, x, yb * 8, jnp.where(solid, g[0], KEEP * g[0] + hit.base))
            for k in range(1, 19, 2):
                even, odd = hit.terms(k)
                ahead = jnp.where(solid, g[k + 1], KEEP * g[k] + (even + odd))
                back = jnp.where(solid, g[k], KEEP * g[k + 1] + (even - odd))
                put(k, x, yb * 8, ahead)
                put(k + 1, x, yb * 8, back)
                if DIRS[k][2] != 0:
                    up, down = (k, k + 1) if DIRS[k][2] == 1 else (k + 1, k)
                    rising, falling = (ahead, back) if up == k else (back, ahead)
                    rows = pl.ds(OY + yb * 8, 8)
                    pltpu.store(out.at[up, x - low + 1, rows, :], falling, mask=first)
                    pltpu.store(out.at[down, x - low + 1, rows, :], rising, mask=last)

        @pl.when(x > low)
        def _():
            send(x - 1).start()

        return carry

    lax.fori_loop(low, high, plane, 0)
    send(high - 1).start()
    for x in range(low, high):
        send(x).wait()


def from_behind(block, axis, distance):
    count = lax.axis_size(axis)
    return lax.ppermute(block, axis, [((i - distance) % count, i) for i in range(count)])


def exchanged(block, source):
    count_x, count_y = lax.axis_size("gx"), lax.axis_size("gy")
    pairs = []
    for x in range(count_x):
        for y in range(count_y):
            from_x, from_y = source(x, y)
            pairs.append(((from_x % count_x) * count_y + from_y % count_y, x * count_y + y))
    return lax.ppermute(block, ("gx", "gy"), pairs)


def swapped(block):
    return exchanged(block, lambda x, y: (x, y ^ 1))


def fetched(block, first, second):
    return exchanged(
        block, lambda x, y: (x + (second if y % 2 else first)[0], y + (second if y % 2 else first)[1])
    )


def cost(flops):
    return pl.CostEstimate(flops=flops, bytes_accessed=0, transcendentals=0)


def local(populations, solid_flags, point_cells, point_turbine, blade_speed, chord, turbine_gain):
    points = point_cells.shape[1]
    total_x = CX * lax.axis_size("gx")
    total_y = CY * lax.axis_size("gy")
    sds = jax.ShapeDtypeStruct
    params = pltpu.CompilerParams(vmem_limit_bytes=24 * 1024 * 1024)
    light = pltpu.CompilerParams(vmem_limit_bytes=4 * 1024 * 1024)
    compact = [
        pltpu.VMEM((CHUNK, points), BF16),
        pltpu.VMEM((16, points), F32),
        pltpu.VMEM((LANES, LANES), F32),
        pltpu.VMEM((LANES, LANES), F32),
    ]
    sibling, across, east, west, held_pops = pl.pallas_call(
        sample_kernel,
        out_shape=(
            sds((192, LANES), F32),
            sds((192, LANES), F32),
            sds((10, CY, LANES), F32),
            sds((10, CY, LANES), F32),
            sds(populations.shape, F32),
        ),
        in_specs=[HBM] * 7,
        out_specs=(VMEM,) * 5,
        scratch_shapes=[
            pltpu.VMEM((3 * CX * CY, 2 * LANES), BF16),
            pltpu.VMEM((3 * CX * CY, LANES), BF16),
            *compact,
            pltpu.VMEM((16, CHUNK), F32),
            pltpu.SMEM(turbine_gain.shape, F32),
            pltpu.VMEM(solid_flags.shape, jnp.int32),
            pltpu.VMEM((3, points), jnp.int32),
            pltpu.VMEM((1, points), jnp.int32),
            pltpu.VMEM((1, points), F32),
            pltpu.VMEM((3, points), F32),
            pltpu.SemaphoreType.DMA((CX,)),
            pltpu.SemaphoreType.DMA((6,)),
        ],
        compiler_params=params,
        name="sample",
    )(
        *[
            pltpu.with_memory_space_constraint(arg, pltpu.HBM)
            for arg in (
                turbine_gain, populations, solid_flags, point_cells, point_turbine, chord,
                blade_speed,
            )
        ]
    )
    beside = swapped(sibling)
    beyond = exchanged(across, lambda x, y: (x, y + 1 if y % 2 else y - 1))
    from_west = from_behind(east, "gx", 1)
    from_east = from_behind(west, "gx", -1)
    joined = pl.pallas_call(
        join_kernel,
        out_shape=sds((136, LANES), F32),
        in_specs=[VMEM] * 3,
        out_specs=VMEM,
        compiler_params=light,
        name="join",
    )(sibling, beside, beyond)
    west_pts = from_behind(joined, "gx", 1)
    east_pts = from_behind(joined, "gx", -1)
    other_half = exchanged(joined, lambda x, y: (x, y + 4))
    near = known(joined[:112], known(west_pts[:112], east_pts[:112]))
    prepared = pl.pallas_call(
        functools.partial(prep_kernel, total_x=total_x, total_y=total_y),
        out_shape=(
            sds((READY + 1, 8, CHUNK), F32),
            sds((LANES, LANES), F32),
            sds((8, points), F32),
        ),
        in_specs=[VMEM],
        out_specs=(VMEM, VMEM, VMEM),
        scratch_shapes=[pltpu.VMEM((CHUNK, points), BF16), pltpu.VMEM((LANES, LANES), F32)],
        compiler_params=params,
        cost_estimate=cost(FORCE_FLOPS),
        name="prep",
    )(point_cells)
    force = pl.pallas_call(
        force_kernel,
        out_shape=sds((3, CX + 2, FY, LANES), F32),
        in_specs=[VMEM] * 4,
        out_specs=VMEM,
        scratch_shapes=[pltpu.VMEM((CHUNK, points), BF16), pltpu.VMEM((8, CHUNK), F32)],
        compiler_params=params,
        cost_estimate=cost(FORCE_FLOPS),
        name="force",
    )(*prepared, near)
    step_args = (
        held_pops, solid_flags, force, from_west, from_east, beside, beyond, west_pts, east_pts,
    )
    read = None
    for low, high in ((0, CX // 2), (CX // 2, CX)):
        extra = () if read is None else (read,)
        read = pl.pallas_call(
            functools.partial(step_kernel, low=low, high=high),
            out_shape=sds(populations.shape, F32),
            in_specs=[VMEM] * 9 + [HBM] * len(extra),
            out_specs=HBM,
            scratch_shapes=[
                pltpu.VMEM((19, high - low + 2, CY + 16, LANES), F32),
                pltpu.SemaphoreType.DMA((CX,)),
            ],
            input_output_aliases={9: 0} if extra else {},
            compiler_params=params,
            cost_estimate=cost(STEP_FLOPS),
        )(*step_args, *extra)
    have = known(near, other_half[:112])
    got = swapped(have)
    have = known(have, got)
    got = fetched(have, (4, 0), (-4, 0))
    have = known(have, got)
    have = known(have, swapped(have))
    got = fetched(have, (12, 0), (-12, 0))
    have = known(have, got)
    have = known(have, swapped(have))
    got = exchanged(
        have, lambda x, y: (x // 4 * 4 + (x + 2) % 4, y) if y % 2 else (x, y + 4)
    )
    have = known(have, got)
    point_force = pl.pallas_call(
        finish_kernel,
        out_shape=sds((3, points), F32),
        in_specs=[VMEM] * 2,
        out_specs=VMEM,
        compiler_params=light,
        name="finish",
    )(have, swapped(have))
    return read, point_force


def solution(mesh):
    in_specs = (P(None, "gx", "gy", None), P("gx", "gy", None), P(), P(), P(), P(), P())
    out_specs = (P(None, "gx", "gy", None), P())
    return jax.shard_map(local, mesh=mesh, in_specs=in_specs, out_specs=out_specs, check_vma=False)
```

```python
import functools

import jax
import jax.numpy as jnp
from jax import lax
from jax.experimental import pallas as pl
from jax.experimental.pallas import tpu as pltpu
from jax.sharding import PartitionSpec as P


SMEAR = 3
RELAX = 0.8
SCALE = 1.5
CHUNK = 256
LANES = 128
DIRS = [
    (0, 0, 0),
    (1, 0, 0),
    (-1, 0, 0),
    (0, 1, 0),
    (0, -1, 0),
    (0, 0, 1),
    (0, 0, -1),
    (1, 1, 0),
    (-1, -1, 0),
    (1, -1, 0),
    (-1, 1, 0),
    (1, 0, 1),
    (-1, 0, -1),
    (1, 0, -1),
    (-1, 0, 1),
    (0, 1, 1),
    (0, -1, -1),
    (0, 1, -1),
    (0, -1, 1),
]
OPP = [0, 2, 1, 4, 3, 6, 5, 8, 7, 10, 9, 12, 11, 14, 13, 16, 15, 18, 17]
EAST = [i for i in range(19) if DIRS[i][0] == 1]
WEST = [i for i in range(19) if DIRS[i][0] == -1]
NORTH = [i for i in range(19) if DIRS[i][1] == 1]
SOUTH = [i for i in range(19) if DIRS[i][1] == -1]
CX, CY = 8, 64
F32, BF16 = jnp.float32, jnp.bfloat16
FORCE_FLOPS = 40_000_000
STEP_FLOPS = 60_000_000
HBM = pl.BlockSpec(memory_space=pltpu.HBM)
VMEM = pl.BlockSpec(memory_space=pltpu.VMEM)
NT = (((1,), (1,)), ((), ()))
NN = (((1,), (0,)), ((), ()))


def dot(a, b, dims=NN):
    return lax.dot_general(a, b, dims, preferred_element_type=F32)


def split3(v):
    high = v.astype(BF16)
    rest = v - high.astype(F32)
    mid = rest.astype(BF16)
    low = (rest - mid.astype(F32)).astype(BF16)
    return high, mid, low


def picked(table, lanes):
    return jnp.take_along_axis(table, lanes, axis=1, mode="promise_in_bounds")


def moments(g):
    s = [None] * 19
    d = [None] * 19
    for k in range(1, 19, 2):
        s[k] = g[k] + g[k + 1]
        d[k] = g[k] - g[k + 1]
    w1, w2 = 1.0 / 18.0, 1.0 / 36.0
    rho = (
        g[0] * (1.0 / 3.0)
        + (s[1] + s[3] + s[5]) * w1
        + ((s[7] + s[9]) + (s[11] + s[13]) + (s[15] + s[17])) * w2
    )
    mx = d[1] * w1 + ((d[7] + d[9]) + (d[11] + d[13])) * w2
    my = d[3] * w1 + ((d[7] - d[9]) + (d[15] + d[17])) * w2
    mz = d[5] * w1 + ((d[11] - d[13]) + (d[15] - d[17])) * w2
    return rho, (mx, my, mz)


def along(c, v):
    total = None
    for comp, part in zip(c, v):
        if comp == 0:
            continue
        if total is None:
            total = part if comp > 0 else -part
        else:
            total = total + part if comp > 0 else total - part
    return total


class Collision:
    def __init__(self, rho, mom, force):
        inv = 1.0 / rho
        amp = 1.0 - 0.5 / RELAX
        vel = [(m + 0.5 * f) * inv for m, f in zip(mom, force)]
        usq = vel[0] * vel[0] + vel[1] * vel[1] + vel[2] * vel[2]
        uf = vel[0] * force[0] + vel[1] * force[1] + vel[2] * force[2]
        heavy = rho * (1.0 / RELAX)
        self.base = heavy - 1.5 * heavy * usq - 3.0 * amp * uf
        self.vel = vel
        rho3, rho45 = 3.0 * heavy, 4.5 * heavy
        self.odd_vec = [rho3 * u + (3.0 * amp) * f for u, f in zip(vel, force)]
        self.even_vec = [rho45 * u + (9.0 * amp) * f for u, f in zip(vel, force)]

    def terms(self, k):
        if k == 0:
            return self.base, None
        c = DIRS[k]
        return self.base + along(c, self.vel) * along(c, self.even_vec), along(c, self.odd_vec)

    def one(self, k):
        first = k if k % 2 == 1 else k - 1
        even, odd = self.terms(first)
        return even + odd if first == k else even - odd


KEEP = 1.0 - 1.0 / RELAX


def sample_kernel(
    gain_hbm, pops_hbm, flags_hbm, cells_hbm, turb_hbm, chord_hbm, blade_hbm,
    sibling, across, paired, unpaired, pops,
    vhm, vl, sel, fld, m128, r128, got_ref,
    gain, flags, cells, turb, chord, blade, sems, in_sems,
):
    small = [
        pltpu.make_async_copy(src, dst, in_sems.at[k])
        for k, (src, dst) in enumerate(
            (
                (cells_hbm, cells),
                (turb_hbm, turb.at[0]),
                (chord_hbm, chord.at[0]),
                (blade_hbm, blade),
                (gain_hbm, gain),
                (flags_hbm, flags),
            )
        )
    ]
    for copy in small:
        copy.start()
    for x in range(CX):
        pltpu.make_async_copy(pops_hbm.at[:, x], pops.at[:, x], sems.at[x]).start()
    points = cells.shape[1]
    tiles = points // LANES
    start_x, start_y = lax.axis_index("gx") * CX, lax.axis_index("gy") * CY
    even = lax.axis_index("gy") % 2 == 0
    for copy in small[:5]:
        copy.wait()
    px = cells[0:1, :] - start_x
    py = cells[1:2, :] - start_y
    own = (px >= 0) & (px < CX) & (py >= 0) & (py < CY)
    own = jnp.where(own, 1.0, 0.0)
    m128[...] = jnp.zeros_like(m128)
    for j in range(tiles):
        m128[j : j + 1, :] = own[:, j * LANES : (j + 1) * LANES]
    mask = m128[...]
    maskb = mask.astype(BF16)
    rows = lax.broadcasted_iota(jnp.int32, (LANES, LANES), 0)
    cols = lax.broadcasted_iota(jnp.int32, (LANES, LANES), 1)
    before = jnp.where(rows < cols, 1.0, 0.0).astype(BF16)
    above = jnp.where(rows > cols, 1.0, 0.0).astype(BF16)
    inside = dot(maskb, before)
    ahead = jnp.sum(dot(above, maskb), axis=1, keepdims=True)
    r128[...] = jnp.where(mask > 0.0, inside + ahead, -1.0)
    count = jnp.sum(mask).astype(jnp.int32)

    fld[0:1, :] = px.astype(F32)
    fld[1:2, :] = py.astype(F32)
    fld[2:3, :] = cells[2:3, :].astype(F32)
    fld[3:4, :] = turb[...].astype(F32)
    ch = split3(chord[...])
    bl = split3(blade[...])
    for k in range(3):
        fld[4 + k : 5 + k, :] = ch[k].astype(F32)
        fld[7 + 3 * k : 10 + 3 * k, :] = bl[k].astype(F32)
    spots = lax.broadcasted_iota(jnp.int32, (CHUNK, LANES), 0).astype(F32)

    def choose(turn):
        base = (turn * CHUNK).astype(F32) if not isinstance(turn, int) else 0.0
        for j in range(tiles):
            hit = r128[j : j + 1, :] - base == spots
            sel[:, j * LANES : (j + 1) * LANES] = jnp.where(hit, 1.0, 0.0).astype(BF16)
        got_ref[...] = dot(fld[...].astype(BF16), sel[...], NT)

    @pl.when(count > 0)
    def _():
        choose(0)

    small[5].wait()

    def plane(x, carry):
        pltpu.make_async_copy(pops_hbm.at[:, x], pops.at[:, x], sems.at[x]).wait()
        for yb in range(CY // 16):
            g = [pops[i, x, yb * 16 : yb * 16 + 16, :] for i in range(19)]
            rho, mom = moments(g)
            for c in range(3):
                at = pl.multiple_of(c * CX * CY + x * CY + yb * 16, 16)
                high, mid, low = split3(mom[c] / rho)
                vhm[pl.ds(at, 16), 0:LANES] = high
                vhm[pl.ds(at, 16), LANES : 2 * LANES] = mid
                vl[pl.ds(at, 16), :] = low
        return carry

    lax.fori_loop(0, CX, plane, 0)

    def pack(ids, g, flag):
        rho, mom = moments(g)
        solid = flag != 0
        held = [jnp.where(solid, g[OPP[i]], g[i]) for i in ids]
        return held + [rho, *mom, flag.astype(F32)]

    even_x = lax.axis_index("gx") % 2 == 0
    for yb in range(CY // 8):
        at = slice(yb * 8, yb * 8 + 8)
        ahead = pack(EAST, [pops[i, CX - 1, at, :] for i in range(19)], flags[CX - 1, at, :])
        back = pack(WEST, [pops[i, 0, at, :] for i in range(19)], flags[0, at, :])
        for k, (a, b) in enumerate(zip(ahead, back)):
            paired[k, at, :] = jnp.where(even_x, a, b)
            unpaired[k, at, :] = jnp.where(even_x, b, a)
    up = pack(NORTH, [pops[i, :, CY - 1, :] for i in range(19)], flags[:, CY - 1, :])
    down = pack(SOUTH, [pops[i, :, 0, :] for i in range(19)], flags[:, 0, :])
    for k, (a, b) in enumerate(zip(up, down)):
        sibling[112 + 8 * k : 120 + 8 * k, :] = jnp.where(even, a, b)
        across[112 + 8 * k : 120 + 8 * k, :] = jnp.where(even, b, a)

    levels = lax.broadcasted_iota(jnp.int32, (LANES, CHUNK), 0).astype(F32)
    cell_ids = lax.broadcasted_iota(jnp.int32, (CX * CY, CHUNK), 0).astype(F32)

    def chunk(turn, carry):
        @pl.when(turn > 0)
        def _():
            choose(turn)

        got = got_ref[...]
        cell = got[0:1] * CY + got[1:2]
        onez = jnp.where(levels == got[2:3], 1.0, 0.0).astype(BF16)
        twice = jnp.concatenate([onez, onez], axis=0)
        factor = jnp.zeros((1, CHUNK), F32)
        for t in range(gain.shape[0]):
            factor = jnp.where(got[3:4] == t, gain[t], factor)
        factor = factor * (got[4:5] + got[5:6] + got[6:7])
        rel = []
        for c in range(3):
            at = slice(c * CX * CY, (c + 1) * CX * CY)
            lines = dot(vhm[at, :], twice) + dot(vl[at, :], onez)
            sampled = jnp.sum(jnp.where(cell_ids == cell, lines, 0.0), axis=0, keepdims=True)
            speed = got[7 + c : 8 + c] + got[10 + c : 11 + c] + got[13 + c : 14 + c]
            rel.append(sampled - speed)
        size = jnp.sqrt(rel[0] * rel[0] + rel[1] * rel[1] + rel[2] * rel[2] + 0.0001)
        size = -(factor * size)
        for c in range(3):
            value = size * rel[c]
            low = jnp.broadcast_to(value[:, :LANES], (8, LANES))
            high = jnp.broadcast_to(value[:, LANES:], (8, LANES))
            for t in range(0, tiles, 8):
                count_rows = min(8, tiles - t)
                order = r128[t : t + 8, :].astype(jnp.int32) - turn * CHUNK
                inside_chunk = (order >= 0) & (order < CHUNK)
                spot = order & (LANES - 1)
                got_value = jnp.where(order >= LANES, picked(high, spot), picked(low, spot))
                at = slice(c * tiles + t, c * tiles + t + count_rows)
                sibling[at, :] = jnp.where(inside_chunk, got_value, 0.0)[:count_rows] + sibling[at, :]
        return carry

    sibling[0:112, :] = jnp.zeros((112, LANES), F32)
    lax.fori_loop(0, (count + CHUNK - 1) // CHUNK, chunk, 0)
    across[0:112, :] = sibling[0:112, :]


def known(a, b):
    return jnp.where(a != 0.0, a, b)


def join_kernel(own, beside, beyond, out):
    even = lax.axis_index("gy") % 2 == 0
    out[0:112, :] = known(own[0:112, :], known(beside[0:112, :], beyond[0:112, :]))
    at = 112
    for x, first, second in ((CX - 1, 7, 9), (0, 10, 8)):
        for ids, wanted, south in ((NORTH, first, True), (SOUTH, second, False)):
            for k in [ids.index(wanted), 5, 6, 7, 8, 9]:
                row = slice(112 + 8 * k + x, 113 + 8 * k + x)
                a, b = beside[row, :], beyond[row, :]
                out[at : at + 1, :] = jnp.where(even, b, a) if south else jnp.where(even, a, b)
                at += 1


def finish_kernel(mine, other, out):
    whole = known(mine[...], other[...])
    tiles = out.shape[1] // LANES
    for c in range(3):
        for j in range(tiles):
            row = c * tiles + j
            out[c : c + 1, j * LANES : (j + 1) * LANES] = whole[row : row + 1, :]


FY = 72


READY = 4


def choose_points(rank, base, sel):
    spots = lax.broadcasted_iota(jnp.int32, (CHUNK, LANES), 0).astype(F32)
    for j in range(sel.shape[1] // LANES):
        hit = rank[j : j + 1, :] - base == spots
        sel[:, j * LANES : (j + 1) * LANES] = jnp.where(hit, 1.0, 0.0).astype(BF16)


def prep_kernel(cells, spot, rank, places, sel, m128, *, total_x, total_y):
    points = cells.shape[1]
    tiles = points // LANES

    def wrapped(v, total):
        v = jnp.where(v < -(total // 2), v + total, v)
        return jnp.where(v >= total // 2, v - total, v)

    px = wrapped(cells[0:1, :] - lax.axis_index("gx") * CX, total_x)
    py = wrapped(cells[1:2, :] - lax.axis_index("gy") * CY, total_y)
    reach = SMEAR + 1
    near = (px >= -reach) & (px < CX + reach) & (py >= -reach) & (py < CY + reach)
    near = jnp.where(near, 1.0, 0.0)
    m128[...] = jnp.zeros_like(m128)
    for j in range(tiles):
        m128[j : j + 1, :] = near[:, j * LANES : (j + 1) * LANES]
    mask = m128[...]
    maskb = mask.astype(BF16)
    rows = lax.broadcasted_iota(jnp.int32, (LANES, LANES), 0)
    cols = lax.broadcasted_iota(jnp.int32, (LANES, LANES), 1)
    before = jnp.where(rows < cols, 1.0, 0.0).astype(BF16)
    above = jnp.where(rows > cols, 1.0, 0.0).astype(BF16)
    inside = dot(maskb, before)
    ahead = jnp.sum(dot(above, maskb), axis=1, keepdims=True)
    rank[...] = jnp.where(mask > 0.0, inside + ahead, -1.0)
    count = jnp.sum(mask).astype(jnp.int32)
    places[0:1, :] = px.astype(F32)
    places[1:2, :] = py.astype(F32)
    places[2:3, :] = cells[2:3, :].astype(F32)
    number = lax.broadcasted_iota(jnp.int32, (1, points), 1)
    places[3:4, :] = (number // LANES).astype(F32)
    places[4:5, :] = (number % LANES).astype(F32)
    places[5:6, :] = jnp.ones((1, points), F32)
    places[6:8, :] = jnp.zeros((2, points), F32)

    def chunk(turn, carry):
        choose_points(rank, (turn * CHUNK).astype(F32), sel)
        spot[turn] = dot(places[...].astype(BF16), sel[...], NT)
        return carry

    lax.fori_loop(0, jnp.minimum((count + CHUNK - 1) // CHUNK, READY), chunk, 0)
    spot[READY] = jnp.broadcast_to(count.astype(F32), (8, CHUNK))


def force_kernel(spot_in, rank, places, points_in, out, sel, late):
    tiles = places.shape[1] // LANES
    count = jnp.max(spot_in[READY, 0:1, 0:LANES]).astype(jnp.int32)
    out[...] = jnp.zeros_like(out)

    def kernel_value(cell, point):
        dist = cell - point
        return jnp.where(
            jnp.abs(dist) <= SMEAR, jnp.exp(-((dist / SCALE) * (dist / SCALE))), 0.0
        )

    def iota(size):
        return lax.broadcasted_iota(jnp.int32, (size, CHUNK), 0).astype(F32)

    row_ids = lax.broadcasted_iota(jnp.int32, (8, LANES), 0)

    def spread(spot):
        forces = []
        for c in range(3):
            halves = []
            for h in range(0, CHUNK, LANES):
                row = jnp.broadcast_to(spot[3:4, h : h + LANES].astype(jnp.int32), (8, LANES))
                lane = jnp.broadcast_to(spot[4:5, h : h + LANES].astype(jnp.int32), (8, LANES))
                total = jnp.zeros((8, LANES), F32)
                for t in range(c * tiles // 8, ((c + 1) * tiles - 1) // 8 + 1):
                    value = picked(points_in[8 * t : 8 * t + 8, :], lane)
                    total = jnp.where(row_ids + (8 * t - c * tiles) == row, value, total)
                halves.append(jnp.sum(total, axis=0, keepdims=True))
            force = jnp.concatenate(halves, axis=1)
            forces.append(jnp.where(spot[5:6] > 0.5, force, 0.0))
        kx = kernel_value(iota(16) - 1.0, spot[0:1])
        ky = kernel_value(iota(FY) - 1.0, spot[1:2])
        kz = kernel_value(iota(LANES), spot[2:3])
        left = jnp.concatenate([f * ky for f in forces], axis=0)
        left_high = left.astype(BF16)
        left_low = (left - left_high.astype(F32)).astype(BF16)
        left_both = jnp.concatenate([left_high, left_low], axis=0)
        lines = 3 * FY
        for x in range(0, CX + 2, 2):
            right = jnp.concatenate([kx[x : x + 1] * kz, kx[x + 1 : x + 2] * kz], axis=0)
            right_high = right.astype(BF16)
            right_low = (right - right_high.astype(F32)).astype(BF16)
            both = dot(left_both, right_high, NT)
            field = both[:lines] + (dot(left_high, right_low, NT) + both[lines:])
            for c in range(3):
                part = field[c * FY : (c + 1) * FY]
                out[c, x, :, :] += part[:, :LANES]
                out[c, x + 1, :, :] += part[:, LANES:]

    chunks = (count + CHUNK - 1) // CHUNK

    def chunk(turn, carry):
        @pl.when(turn >= READY)
        def _():
            choose_points(rank, (turn * CHUNK).astype(F32), sel)
            late[...] = dot(places[...].astype(BF16), sel[...], NT)

        @pl.when(turn < READY)
        def _():
            late[...] = spot_in[turn]

        spread(late[...])
        return carry

    lax.fori_loop(0, chunks, chunk, 0)


OY = 8


def step_kernel(
    pops, flags, force, paired, unpaired, beside, beyond, pair_pts, other_pts, *rest, low, high
):
    out_hbm, out, out_sems = rest[-3:]
    lane = lax.broadcasted_iota(jnp.int32, (8, LANES), 1)
    not_first, not_last = lane > 0, lane < LANES - 1
    first, last = lane == 0, lane == LANES - 1

    def put(i, x, row, val):
        cx, cy, cz = DIRS[i]
        dst = out.at[i, x - low + 1 + cx, pl.ds(OY + row + cy, val.shape[0]), :]
        if cz == 0:
            dst[...] = val
        elif cz == 1:
            pltpu.store(dst, pltpu.roll(val, 1, 1), mask=not_first[: val.shape[0]])
        else:
            pltpu.store(dst, pltpu.roll(val, LANES - 1, 1), mask=not_last[: val.shape[0]])

    def inside(x):
        return low <= x < high

    def force_at(x, yb):
        return [force[c, x + 1, yb * 8 + 1 : yb * 8 + 9, :] for c in range(3)]

    even_x = lax.axis_index("gx") % 2 == 0

    def from_side(west, pair, other):
        return jnp.where(even_x, other, pair) if west else jnp.where(even_x, pair, other)

    for ids, x in ((EAST, low - 1), (WEST, high)):
        for yb in range(CY // 8):
            at = slice(yb * 8, yb * 8 + 8)
            if 0 <= x < CX:
                g = [pops[i, x, at, :] for i in range(19)]
                rho, mom = moments(g)
                solid = flags[x, at, :] != 0
                held = [jnp.where(solid, g[OPP[i]], g[i]) for i in ids]
            else:
                part = [from_side(x < 0, paired[k, at, :], unpaired[k, at, :]) for k in range(10)]
                rho, mom = part[5], part[6:9]
                solid = part[9] != 0.0
                held = part[:5]
            hit = Collision(rho, mom, force_at(x, yb))
            for val, i in zip(held, ids):
                put(i, x, yb * 8, jnp.where(solid, val, KEEP * val + hit.one(i)))
    even = lax.axis_index("gy") % 2 == 0
    for ids, y in ((NORTH, -1), (SOUTH, CY)):
        part = []
        for k in range(10):
            a, b = beside[112 + 8 * k : 120 + 8 * k, :], beyond[112 + 8 * k : 120 + 8 * k, :]
            part.append(jnp.where(even, b, a) if y < 0 else jnp.where(even, a, b))
        frc = [force[c, 1 : CX + 1, y + 1, :] for c in range(3)]
        hit = Collision(part[5], part[6:9], frc)
        solid = part[9] != 0.0
        for k, i in enumerate(ids):
            val = jnp.where(solid, part[k], KEEP * part[k] + hit.one(i))
            cx, cy, cz = DIRS[i]
            if cz != 0:
                val = pltpu.roll(val, 1 if cz == 1 else LANES - 1, 1)
            for x in range(CX):
                if not inside(x + cx):
                    continue
                dst = out.at[i, x - low + 1 + cx, OY + y + cy : OY + y + cy + 1, :]
                if cz == 0:
                    dst[...] = val[x : x + 1]
                else:
                    keep = (not_first if cz == 1 else not_last)[0:1]
                    pltpu.store(dst, val[x : x + 1], mask=keep)
    for at, i, x, y in ((112, 7, -1, -1), (118, 9, -1, CY), (124, 10, CX, -1), (130, 8, CX, CY)):
        if not inside(x + DIRS[i][0]):
            continue
        part = [
            from_side(x < 0, pair_pts[at + k : at + k + 1, :], other_pts[at + k : at + k + 1, :])
            for k in range(6)
        ]
        held, rho, mom = part[0], part[1], part[2:5]
        solid = part[5] != 0.0
        frc = [force[c, x + 1, y + 1 : y + 2, :] for c in range(3)]
        hit = Collision(rho, mom, frc)
        put(i, x, y, jnp.where(solid, held, KEEP * held + hit.one(i)))

    def send(x):
        return pltpu.make_async_copy(
            out.at[:, x - low + 1, OY : OY + CY, :], out_hbm.at[:, x], out_sems.at[x]
        )

    def plane(x, carry):
        for yb in range(CY // 8):
            at = slice(yb * 8, yb * 8 + 8)
            g = [pops[i, x, at, :] for i in range(19)]
            solid = flags[x, at, :] != 0
            rho, mom = moments(g)
            hit = Collision(rho, mom, force_at(x, yb))
            put(0, x, yb * 8, jnp.where(solid, g[0], KEEP * g[0] + hit.base))
            for k in range(1, 19, 2):
                even, odd = hit.terms(k)
                ahead = jnp.where(solid, g[k + 1], KEEP * g[k] + (even + odd))
                back = jnp.where(solid, g[k], KEEP * g[k + 1] + (even - odd))
                put(k, x, yb * 8, ahead)
                put(k + 1, x, yb * 8, back)
                if DIRS[k][2] != 0:
                    up, down = (k, k + 1) if DIRS[k][2] == 1 else (k + 1, k)
                    rising, falling = (ahead, back) if up == k else (back, ahead)
                    rows = pl.ds(OY + yb * 8, 8)
                    pltpu.store(out.at[up, x - low + 1, rows, :], falling, mask=first)
                    pltpu.store(out.at[down, x - low + 1, rows, :], rising, mask=last)

        @pl.when(x > low)
        def _():
            send(x - 1).start()

        return carry

    lax.fori_loop(low, high, plane, 0)
    send(high - 1).start()
    for x in range(low, high):
        send(x).wait()


def exchanged(block, source):
    count_x, count_y = lax.axis_size("gx"), lax.axis_size("gy")
    pairs = []
    for x in range(count_x):
        for y in range(count_y):
            from_x, from_y = source(x, y)
            pairs.append(((from_x % count_x) * count_y + from_y % count_y, x * count_y + y))
    return lax.ppermute(block, ("gx", "gy"), pairs)


def swapped(block):
    return exchanged(block, lambda x, y: (x, y ^ 1))


def along_z(block, distance):
    def source(x, y):
        return x + 4 * distance * (1 if (x // 4 + y) % 2 == 0 else -1), y

    return exchanged(block, source)


def cost(flops):
    return pl.CostEstimate(flops=flops, bytes_accessed=0, transcendentals=0)


def local(populations, solid_flags, point_cells, point_turbine, blade_speed, chord, turbine_gain):
    points = point_cells.shape[1]
    total_x = CX * lax.axis_size("gx")
    total_y = CY * lax.axis_size("gy")
    sds = jax.ShapeDtypeStruct
    params = pltpu.CompilerParams(vmem_limit_bytes=24 * 1024 * 1024)
    light = pltpu.CompilerParams(vmem_limit_bytes=4 * 1024 * 1024)
    compact = [
        pltpu.VMEM((CHUNK, points), BF16),
        pltpu.VMEM((16, points), F32),
        pltpu.VMEM((LANES, LANES), F32),
        pltpu.VMEM((LANES, LANES), F32),
    ]
    sibling, across, paired, unpaired, held_pops = pl.pallas_call(
        sample_kernel,
        out_shape=(
            sds((192, LANES), F32),
            sds((192, LANES), F32),
            sds((10, CY, LANES), F32),
            sds((10, CY, LANES), F32),
            sds(populations.shape, F32),
        ),
        in_specs=[HBM] * 7,
        out_specs=(VMEM,) * 5,
        scratch_shapes=[
            pltpu.VMEM((3 * CX * CY, 2 * LANES), BF16),
            pltpu.VMEM((3 * CX * CY, LANES), BF16),
            *compact,
            pltpu.VMEM((16, CHUNK), F32),
            pltpu.SMEM(turbine_gain.shape, F32),
            pltpu.VMEM(solid_flags.shape, jnp.int32),
            pltpu.VMEM((3, points), jnp.int32),
            pltpu.VMEM((1, points), jnp.int32),
            pltpu.VMEM((1, points), F32),
            pltpu.VMEM((3, points), F32),
            pltpu.SemaphoreType.DMA((CX,)),
            pltpu.SemaphoreType.DMA((6,)),
        ],
        compiler_params=params,
        name="sample",
    )(
        *[
            pltpu.with_memory_space_constraint(arg, pltpu.HBM)
            for arg in (
                turbine_gain, populations, solid_flags, point_cells, point_turbine, chord,
                blade_speed,
            )
        ]
    )
    beside = swapped(sibling)
    beyond = exchanged(across, lambda x, y: (x, y + 1 if y % 2 else y - 1))
    paired = exchanged(paired, lambda x, y: (x ^ 1, y))
    unpaired = exchanged(unpaired, lambda x, y: (x + 1 if x % 2 else x - 1, y))
    joined = pl.pallas_call(
        join_kernel,
        out_shape=sds((136, LANES), F32),
        in_specs=[VMEM] * 3,
        out_specs=VMEM,
        compiler_params=light,
        name="join",
    )(sibling, beside, beyond)
    pair_pts = exchanged(joined, lambda x, y: (x ^ 1, y))
    other_pts = exchanged(joined, lambda x, y: (x + 1 if x % 2 else x - 1, y))
    other_half = exchanged(joined, lambda x, y: (x, y + 4))
    near = known(joined[:112], known(pair_pts[:112], other_pts[:112]))
    prepared = pl.pallas_call(
        functools.partial(prep_kernel, total_x=total_x, total_y=total_y),
        out_shape=(
            sds((READY + 1, 8, CHUNK), F32),
            sds((LANES, LANES), F32),
            sds((8, points), F32),
        ),
        in_specs=[VMEM],
        out_specs=(VMEM, VMEM, VMEM),
        scratch_shapes=[pltpu.VMEM((CHUNK, points), BF16), pltpu.VMEM((LANES, LANES), F32)],
        compiler_params=params,
        cost_estimate=cost(FORCE_FLOPS),
        name="prep",
    )(point_cells)
    force = pl.pallas_call(
        force_kernel,
        out_shape=sds((3, CX + 2, FY, LANES), F32),
        in_specs=[VMEM] * 4,
        out_specs=VMEM,
        scratch_shapes=[pltpu.VMEM((CHUNK, points), BF16), pltpu.VMEM((8, CHUNK), F32)],
        compiler_params=params,
        cost_estimate=cost(FORCE_FLOPS),
        name="force",
    )(*prepared, near)
    step_args = (
        held_pops, solid_flags, force, paired, unpaired, beside, beyond, pair_pts, other_pts,
    )
    read = None
    for low, high in ((0, CX // 2), (CX // 2, CX)):
        extra = () if read is None else (read,)
        read = pl.pallas_call(
            functools.partial(step_kernel, low=low, high=high),
            out_shape=sds(populations.shape, F32),
            in_specs=[VMEM] * 9 + [HBM] * len(extra),
            out_specs=HBM,
            scratch_shapes=[
                pltpu.VMEM((19, high - low + 2, CY + 16, LANES), F32),
                pltpu.SemaphoreType.DMA((CX,)),
            ],
            input_output_aliases={9: 0} if extra else {},
            compiler_params=params,
            cost_estimate=cost(STEP_FLOPS),
        )(*step_args, *extra)
    have = known(near, other_half[:112])
    got = swapped(have)
    have = known(have, got)
    got = along_z(have, 1)
    have = known(have, got)
    have = known(have, swapped(have))
    got = along_z(have, 3)
    have = known(have, got)
    have = known(have, swapped(have))
    got = exchanged(
        have, lambda x, y: (x // 4 * 4 + (x + 2) % 4, y) if y % 2 else (x, y + 4)
    )
    have = known(have, got)
    point_force = pl.pallas_call(
        finish_kernel,
        out_shape=sds((3, points), F32),
        in_specs=[VMEM] * 2,
        out_specs=VMEM,
        compiler_params=light,
        name="finish",
    )(have, swapped(have))
    return read, point_force


def solution(mesh):
    in_specs = (P(None, "gx", "gy", None), P("gx", "gy", None), P(), P(), P(), P(), P())
    out_specs = (P(None, "gx", "gy", None), P())
    return jax.shard_map(local, mesh=mesh, in_specs=in_specs, out_specs=out_specs, check_vma=False)
```

```python
import functools

import jax
import jax.numpy as jnp
from jax import lax
from jax.experimental import pallas as pl
from jax.experimental.pallas import tpu as pltpu
from jax.sharding import PartitionSpec as P


SMEAR = 3
RELAX = 0.8
SCALE = 1.5
CHUNK = 256
LANES = 128
DIRS = [
    (0, 0, 0),
    (1, 0, 0),
    (-1, 0, 0),
    (0, 1, 0),
    (0, -1, 0),
    (0, 0, 1),
    (0, 0, -1),
    (1, 1, 0),
    (-1, -1, 0),
    (1, -1, 0),
    (-1, 1, 0),
    (1, 0, 1),
    (-1, 0, -1),
    (1, 0, -1),
    (-1, 0, 1),
    (0, 1, 1),
    (0, -1, -1),
    (0, 1, -1),
    (0, -1, 1),
]
OPP = [0, 2, 1, 4, 3, 6, 5, 8, 7, 10, 9, 12, 11, 14, 13, 16, 15, 18, 17]
EAST = [i for i in range(19) if DIRS[i][0] == 1]
WEST = [i for i in range(19) if DIRS[i][0] == -1]
NORTH = [i for i in range(19) if DIRS[i][1] == 1]
SOUTH = [i for i in range(19) if DIRS[i][1] == -1]
CX, CY = 8, 64
F32, BF16 = jnp.float32, jnp.bfloat16
FORCE_FLOPS = 40_000_000
STEP_FLOPS = 60_000_000
HBM = pl.BlockSpec(memory_space=pltpu.HBM)
VMEM = pl.BlockSpec(memory_space=pltpu.VMEM)
NT = (((1,), (1,)), ((), ()))
NN = (((1,), (0,)), ((), ()))


def dot(a, b, dims=NN):
    return lax.dot_general(a, b, dims, preferred_element_type=F32)


def split3(v):
    high = v.astype(BF16)
    rest = v - high.astype(F32)
    mid = rest.astype(BF16)
    low = (rest - mid.astype(F32)).astype(BF16)
    return high, mid, low


def picked(table, lanes):
    return jnp.take_along_axis(table, lanes, axis=1, mode="promise_in_bounds")


def moments(g):
    s = [None] * 19
    d = [None] * 19
    for k in range(1, 19, 2):
        s[k] = g[k] + g[k + 1]
        d[k] = g[k] - g[k + 1]
    w1, w2 = 1.0 / 18.0, 1.0 / 36.0
    rho = (
        g[0] * (1.0 / 3.0)
        + (s[1] + s[3] + s[5]) * w1
        + ((s[7] + s[9]) + (s[11] + s[13]) + (s[15] + s[17])) * w2
    )
    mx = d[1] * w1 + ((d[7] + d[9]) + (d[11] + d[13])) * w2
    my = d[3] * w1 + ((d[7] - d[9]) + (d[15] + d[17])) * w2
    mz = d[5] * w1 + ((d[11] - d[13]) + (d[15] - d[17])) * w2
    return rho, (mx, my, mz)


def along(c, v):
    total = None
    for comp, part in zip(c, v):
        if comp == 0:
            continue
        if total is None:
            total = part if comp > 0 else -part
        else:
            total = total + part if comp > 0 else total - part
    return total


class Collision:
    def __init__(self, rho, mom, force):
        inv = 1.0 / rho
        amp = 1.0 - 0.5 / RELAX
        vel = [(m + 0.5 * f) * inv for m, f in zip(mom, force)]
        usq = vel[0] * vel[0] + vel[1] * vel[1] + vel[2] * vel[2]
        uf = vel[0] * force[0] + vel[1] * force[1] + vel[2] * force[2]
        heavy = rho * (1.0 / RELAX)
        self.base = heavy - 1.5 * heavy * usq - 3.0 * amp * uf
        self.vel = vel
        rho3, rho45 = 3.0 * heavy, 4.5 * heavy
        self.odd_vec = [rho3 * u + (3.0 * amp) * f for u, f in zip(vel, force)]
        self.even_vec = [rho45 * u + (9.0 * amp) * f for u, f in zip(vel, force)]

    def terms(self, k):
        if k == 0:
            return self.base, None
        c = DIRS[k]
        return self.base + along(c, self.vel) * along(c, self.even_vec), along(c, self.odd_vec)

    def one(self, k):
        first = k if k % 2 == 1 else k - 1
        even, odd = self.terms(first)
        return even + odd if first == k else even - odd


KEEP = 1.0 - 1.0 / RELAX


def sample_kernel(
    gain_hbm, pops_hbm, flags_hbm, cells_hbm, turb_hbm, chord_hbm, blade_hbm,
    sibling, across, paired, unpaired, pops,
    vhm, vl, sel, fld, m128, r128, got_ref,
    gain, flags, cells, turb, chord, blade, sems, in_sems,
):
    small = [
        pltpu.make_async_copy(src, dst, in_sems.at[k])
        for k, (src, dst) in enumerate(
            (
                (cells_hbm, cells),
                (turb_hbm, turb.at[0]),
                (chord_hbm, chord.at[0]),
                (blade_hbm, blade),
                (gain_hbm, gain),
                (flags_hbm, flags),
            )
        )
    ]
    for copy in small:
        copy.start()
    for x in range(CX):
        pltpu.make_async_copy(pops_hbm.at[:, x], pops.at[:, x], sems.at[x]).start()
    points = cells.shape[1]
    tiles = points // LANES
    start_x, start_y = lax.axis_index("gx") * CX, lax.axis_index("gy") * CY
    even = lax.axis_index("gy") % 2 == 0
    for copy in small[:5]:
        copy.wait()
    px = cells[0:1, :] - start_x
    py = cells[1:2, :] - start_y
    own = (px >= 0) & (px < CX) & (py >= 0) & (py < CY)
    own = jnp.where(own, 1.0, 0.0)
    m128[...] = jnp.zeros_like(m128)
    for j in range(tiles):
        m128[j : j + 1, :] = own[:, j * LANES : (j + 1) * LANES]
    mask = m128[...]
    maskb = mask.astype(BF16)
    rows = lax.broadcasted_iota(jnp.int32, (LANES, LANES), 0)
    cols = lax.broadcasted_iota(jnp.int32, (LANES, LANES), 1)
    before = jnp.where(rows < cols, 1.0, 0.0).astype(BF16)
    above = jnp.where(rows > cols, 1.0, 0.0).astype(BF16)
    inside = dot(maskb, before)
    ahead = jnp.sum(dot(above, maskb), axis=1, keepdims=True)
    r128[...] = jnp.where(mask > 0.0, inside + ahead, -1.0)
    count = jnp.sum(mask).astype(jnp.int32)

    fld[0:1, :] = px.astype(F32)
    fld[1:2, :] = py.astype(F32)
    fld[2:3, :] = cells[2:3, :].astype(F32)
    fld[3:4, :] = turb[...].astype(F32)
    ch = split3(chord[...])
    bl = split3(blade[...])
    for k in range(3):
        fld[4 + k : 5 + k, :] = ch[k].astype(F32)
        fld[7 + 3 * k : 10 + 3 * k, :] = bl[k].astype(F32)
    spots = lax.broadcasted_iota(jnp.int32, (CHUNK, LANES), 0).astype(F32)

    def choose(turn):
        base = (turn * CHUNK).astype(F32) if not isinstance(turn, int) else 0.0
        for j in range(tiles):
            hit = r128[j : j + 1, :] - base == spots
            sel[:, j * LANES : (j + 1) * LANES] = jnp.where(hit, 1.0, 0.0).astype(BF16)
        got_ref[...] = dot(fld[...].astype(BF16), sel[...], NT)

    @pl.when(count > 0)
    def _():
        choose(0)

    small[5].wait()

    def plane(x, carry):
        pltpu.make_async_copy(pops_hbm.at[:, x], pops.at[:, x], sems.at[x]).wait()
        for yb in range(CY // 16):
            g = [pops[i, x, yb * 16 : yb * 16 + 16, :] for i in range(19)]
            rho, mom = moments(g)
            for c in range(3):
                at = pl.multiple_of(c * CX * CY + x * CY + yb * 16, 16)
                high, mid, low = split3(mom[c] / rho)
                vhm[pl.ds(at, 16), 0:LANES] = high
                vhm[pl.ds(at, 16), LANES : 2 * LANES] = mid
                vl[pl.ds(at, 16), :] = low
        return carry

    lax.fori_loop(0, CX, plane, 0)

    def pack(ids, g, flag):
        rho, mom = moments(g)
        solid = flag != 0
        held = [jnp.where(solid, g[OPP[i]], g[i]) for i in ids]
        return held + [rho, *mom, flag.astype(F32)]

    even_x = lax.axis_index("gx") % 2 == 0
    for yb in range(CY // 8):
        at = slice(yb * 8, yb * 8 + 8)
        ahead = pack(EAST, [pops[i, CX - 1, at, :] for i in range(19)], flags[CX - 1, at, :])
        back = pack(WEST, [pops[i, 0, at, :] for i in range(19)], flags[0, at, :])
        for k, (a, b) in enumerate(zip(ahead, back)):
            paired[k, at, :] = jnp.where(even_x, a, b)
            unpaired[k, at, :] = jnp.where(even_x, b, a)
    up = pack(NORTH, [pops[i, :, CY - 1, :] for i in range(19)], flags[:, CY - 1, :])
    down = pack(SOUTH, [pops[i, :, 0, :] for i in range(19)], flags[:, 0, :])
    for k, (a, b) in enumerate(zip(up, down)):
        sibling[112 + 8 * k : 120 + 8 * k, :] = jnp.where(even, a, b)
        across[112 + 8 * k : 120 + 8 * k, :] = jnp.where(even, b, a)

    levels = lax.broadcasted_iota(jnp.int32, (LANES, CHUNK), 0).astype(F32)
    cell_ids = lax.broadcasted_iota(jnp.int32, (CX * CY, CHUNK), 0).astype(F32)

    def chunk(turn, carry):
        @pl.when(turn > 0)
        def _():
            choose(turn)

        got = got_ref[...]
        cell = got[0:1] * CY + got[1:2]
        onez = jnp.where(levels == got[2:3], 1.0, 0.0).astype(BF16)
        twice = jnp.concatenate([onez, onez], axis=0)
        factor = jnp.zeros((1, CHUNK), F32)
        for t in range(gain.shape[0]):
            factor = jnp.where(got[3:4] == t, gain[t], factor)
        factor = factor * (got[4:5] + got[5:6] + got[6:7])
        rel = []
        for c in range(3):
            at = slice(c * CX * CY, (c + 1) * CX * CY)
            lines = dot(vhm[at, :], twice) + dot(vl[at, :], onez)
            sampled = jnp.sum(jnp.where(cell_ids == cell, lines, 0.0), axis=0, keepdims=True)
            speed = got[7 + c : 8 + c] + got[10 + c : 11 + c] + got[13 + c : 14 + c]
            rel.append(sampled - speed)
        size = jnp.sqrt(rel[0] * rel[0] + rel[1] * rel[1] + rel[2] * rel[2] + 0.0001)
        size = -(factor * size)
        for c in range(3):
            value = size * rel[c]
            low = jnp.broadcast_to(value[:, :LANES], (8, LANES))
            high = jnp.broadcast_to(value[:, LANES:], (8, LANES))
            for t in range(0, tiles, 8):
                count_rows = min(8, tiles - t)
                order = r128[t : t + 8, :].astype(jnp.int32) - turn * CHUNK
                inside_chunk = (order >= 0) & (order < CHUNK)
                spot = order & (LANES - 1)
                got_value = jnp.where(order >= LANES, picked(high, spot), picked(low, spot))
                at = slice(c * tiles + t, c * tiles + t + count_rows)
                sibling[at, :] = jnp.where(inside_chunk, got_value, 0.0)[:count_rows] + sibling[at, :]
        return carry

    sibling[0:112, :] = jnp.zeros((112, LANES), F32)
    lax.fori_loop(0, (count + CHUNK - 1) // CHUNK, chunk, 0)
    across[0:112, :] = sibling[0:112, :]


def known(a, b):
    return jnp.where(a != 0.0, a, b)


def join_kernel(own, beside, beyond, out):
    even = lax.axis_index("gy") % 2 == 0
    out[0:112, :] = known(own[0:112, :], known(beside[0:112, :], beyond[0:112, :]))
    at = 112
    for x, first, second in ((CX - 1, 7, 9), (0, 10, 8)):
        for ids, wanted, south in ((NORTH, first, True), (SOUTH, second, False)):
            for k in [ids.index(wanted), 5, 6, 7, 8, 9]:
                row = slice(112 + 8 * k + x, 113 + 8 * k + x)
                a, b = beside[row, :], beyond[row, :]
                out[at : at + 1, :] = jnp.where(even, b, a) if south else jnp.where(even, a, b)
                at += 1


def finish_kernel(mine, other, out):
    whole = known(mine[...], other[...])
    tiles = out.shape[1] // LANES
    for c in range(3):
        for j in range(tiles):
            row = c * tiles + j
            out[c : c + 1, j * LANES : (j + 1) * LANES] = whole[row : row + 1, :]


FY = 72


READY = 4


def choose_points(rank, base, sel):
    spots = lax.broadcasted_iota(jnp.int32, (CHUNK, LANES), 0).astype(F32)
    for j in range(sel.shape[1] // LANES):
        hit = rank[j : j + 1, :] - base == spots
        sel[:, j * LANES : (j + 1) * LANES] = jnp.where(hit, 1.0, 0.0).astype(BF16)


def prep_kernel(cells, spot, rank, places, sel, m128, *, total_x, total_y):
    points = cells.shape[1]
    tiles = points // LANES

    def wrapped(v, total):
        v = jnp.where(v < -(total // 2), v + total, v)
        return jnp.where(v >= total // 2, v - total, v)

    px = wrapped(cells[0:1, :] - lax.axis_index("gx") * CX, total_x)
    py = wrapped(cells[1:2, :] - lax.axis_index("gy") * CY, total_y)
    reach = SMEAR + 1
    near = (px >= -reach) & (px < CX + reach) & (py >= -reach) & (py < CY + reach)
    near = jnp.where(near, 1.0, 0.0)
    m128[...] = jnp.zeros_like(m128)
    for j in range(tiles):
        m128[j : j + 1, :] = near[:, j * LANES : (j + 1) * LANES]
    mask = m128[...]
    maskb = mask.astype(BF16)
    rows = lax.broadcasted_iota(jnp.int32, (LANES, LANES), 0)
    cols = lax.broadcasted_iota(jnp.int32, (LANES, LANES), 1)
    before = jnp.where(rows < cols, 1.0, 0.0).astype(BF16)
    above = jnp.where(rows > cols, 1.0, 0.0).astype(BF16)
    inside = dot(maskb, before)
    ahead = jnp.sum(dot(above, maskb), axis=1, keepdims=True)
    rank[...] = jnp.where(mask > 0.0, inside + ahead, -1.0)
    count = jnp.sum(mask).astype(jnp.int32)
    places[0:1, :] = px.astype(F32)
    places[1:2, :] = py.astype(F32)
    places[2:3, :] = cells[2:3, :].astype(F32)
    number = lax.broadcasted_iota(jnp.int32, (1, points), 1)
    places[3:4, :] = (number // LANES).astype(F32)
    places[4:5, :] = (number % LANES).astype(F32)
    places[5:6, :] = jnp.ones((1, points), F32)
    places[6:8, :] = jnp.zeros((2, points), F32)

    def chunk(turn, carry):
        choose_points(rank, (turn * CHUNK).astype(F32), sel)
        spot[turn] = dot(places[...].astype(BF16), sel[...], NT)
        return carry

    lax.fori_loop(0, jnp.minimum((count + CHUNK - 1) // CHUNK, READY), chunk, 0)
    spot[READY] = jnp.broadcast_to(count.astype(F32), (8, CHUNK))


def force_kernel(spot_in, rank, places, points_in, out, sel, late):
    tiles = places.shape[1] // LANES
    count = jnp.max(spot_in[READY, 0:1, 0:LANES]).astype(jnp.int32)
    out[...] = jnp.zeros_like(out)

    def kernel_value(cell, point):
        dist = cell - point
        return jnp.where(
            jnp.abs(dist) <= SMEAR, jnp.exp(-((dist / SCALE) * (dist / SCALE))), 0.0
        )

    def iota(size):
        return lax.broadcasted_iota(jnp.int32, (size, CHUNK), 0).astype(F32)

    row_ids = lax.broadcasted_iota(jnp.int32, (8, LANES), 0)

    def spread(spot):
        forces = []
        for c in range(3):
            halves = []
            for h in range(0, CHUNK, LANES):
                row = jnp.broadcast_to(spot[3:4, h : h + LANES].astype(jnp.int32), (8, LANES))
                lane = jnp.broadcast_to(spot[4:5, h : h + LANES].astype(jnp.int32), (8, LANES))
                total = jnp.zeros((8, LANES), F32)
                for t in range(c * tiles // 8, ((c + 1) * tiles - 1) // 8 + 1):
                    value = picked(points_in[8 * t : 8 * t + 8, :], lane)
                    total = jnp.where(row_ids + (8 * t - c * tiles) == row, value, total)
                halves.append(jnp.sum(total, axis=0, keepdims=True))
            force = jnp.concatenate(halves, axis=1)
            forces.append(jnp.where(spot[5:6] > 0.5, force, 0.0))
        kx = kernel_value(iota(16) - 1.0, spot[0:1])
        ky = kernel_value(iota(FY) - 1.0, spot[1:2])
        kz = kernel_value(iota(LANES), spot[2:3])
        left = jnp.concatenate([f * ky for f in forces], axis=0)
        left_high = left.astype(BF16)
        left_low = (left - left_high.astype(F32)).astype(BF16)
        left_both = jnp.concatenate([left_high, left_low], axis=0)
        lines = 3 * FY
        for x in range(0, CX + 2, 2):
            right = jnp.concatenate([kx[x : x + 1] * kz, kx[x + 1 : x + 2] * kz], axis=0)
            right_high = right.astype(BF16)
            right_low = (right - right_high.astype(F32)).astype(BF16)
            both = dot(left_both, right_high, NT)
            field = both[:lines] + (dot(left_high, right_low, NT) + both[lines:])
            for c in range(3):
                part = field[c * FY : (c + 1) * FY]
                out[c, x, :, :] += part[:, :LANES]
                out[c, x + 1, :, :] += part[:, LANES:]

    chunks = (count + CHUNK - 1) // CHUNK

    def chunk(turn, carry):
        @pl.when(turn >= READY)
        def _():
            choose_points(rank, (turn * CHUNK).astype(F32), sel)
            late[...] = dot(places[...].astype(BF16), sel[...], NT)

        @pl.when(turn < READY)
        def _():
            late[...] = spot_in[turn]

        spread(late[...])
        return carry

    lax.fori_loop(0, chunks, chunk, 0)


OY = 8


def step_kernel(
    pops, flags, force, paired, unpaired, beside, beyond, pair_pts, other_pts, *rest, low, high
):
    out_hbm, out, out_sems = rest[-3:]
    lane = lax.broadcasted_iota(jnp.int32, (8, LANES), 1)
    not_first, not_last = lane > 0, lane < LANES - 1
    first, last = lane == 0, lane == LANES - 1

    def put(i, x, row, val):
        cx, cy, cz = DIRS[i]
        dst = out.at[i, x - low + 1 + cx, pl.ds(OY + row + cy, val.shape[0]), :]
        if cz == 0:
            dst[...] = val
        elif cz == 1:
            pltpu.store(dst, pltpu.roll(val, 1, 1), mask=not_first[: val.shape[0]])
        else:
            pltpu.store(dst, pltpu.roll(val, LANES - 1, 1), mask=not_last[: val.shape[0]])

    def inside(x):
        return low <= x < high

    def force_at(x, yb):
        return [force[c, x + 1, yb * 8 + 1 : yb * 8 + 9, :] for c in range(3)]

    even_x = lax.axis_index("gx") % 2 == 0

    def from_side(west, pair, other):
        return jnp.where(even_x, other, pair) if west else jnp.where(even_x, pair, other)

    for ids, x in ((EAST, low - 1), (WEST, high)):
        for yb in range(CY // 8):
            at = slice(yb * 8, yb * 8 + 8)
            if 0 <= x < CX:
                g = [pops[i, x, at, :] for i in range(19)]
                rho, mom = moments(g)
                solid = flags[x, at, :] != 0
                held = [jnp.where(solid, g[OPP[i]], g[i]) for i in ids]
            else:
                part = [from_side(x < 0, paired[k, at, :], unpaired[k, at, :]) for k in range(10)]
                rho, mom = part[5], part[6:9]
                solid = part[9] != 0.0
                held = part[:5]
            hit = Collision(rho, mom, force_at(x, yb))
            for val, i in zip(held, ids):
                put(i, x, yb * 8, jnp.where(solid, val, KEEP * val + hit.one(i)))
    even = lax.axis_index("gy") % 2 == 0
    for ids, y in ((NORTH, -1), (SOUTH, CY)):
        part = []
        for k in range(10):
            a, b = beside[112 + 8 * k : 120 + 8 * k, :], beyond[112 + 8 * k : 120 + 8 * k, :]
            part.append(jnp.where(even, b, a) if y < 0 else jnp.where(even, a, b))
        frc = [force[c, 1 : CX + 1, y + 1, :] for c in range(3)]
        hit = Collision(part[5], part[6:9], frc)
        solid = part[9] != 0.0
        for k, i in enumerate(ids):
            val = jnp.where(solid, part[k], KEEP * part[k] + hit.one(i))
            cx, cy, cz = DIRS[i]
            if cz != 0:
                val = pltpu.roll(val, 1 if cz == 1 else LANES - 1, 1)
            for x in range(CX):
                if not inside(x + cx):
                    continue
                dst = out.at[i, x - low + 1 + cx, OY + y + cy : OY + y + cy + 1, :]
                if cz == 0:
                    dst[...] = val[x : x + 1]
                else:
                    keep = (not_first if cz == 1 else not_last)[0:1]
                    pltpu.store(dst, val[x : x + 1], mask=keep)
    for at, i, x, y in ((112, 7, -1, -1), (118, 9, -1, CY), (124, 10, CX, -1), (130, 8, CX, CY)):
        if not inside(x + DIRS[i][0]):
            continue
        part = [
            from_side(x < 0, pair_pts[at + k : at + k + 1, :], other_pts[at + k : at + k + 1, :])
            for k in range(6)
        ]
        held, rho, mom = part[0], part[1], part[2:5]
        solid = part[5] != 0.0
        frc = [force[c, x + 1, y + 1 : y + 2, :] for c in range(3)]
        hit = Collision(rho, mom, frc)
        put(i, x, y, jnp.where(solid, held, KEEP * held + hit.one(i)))

    def send(x):
        return pltpu.make_async_copy(
            out.at[:, x - low + 1, OY : OY + CY, :], out_hbm.at[:, x], out_sems.at[x]
        )

    def plane(x, carry):
        for yb in range(CY // 8):
            at = slice(yb * 8, yb * 8 + 8)
            g = [pops[i, x, at, :] for i in range(19)]
            solid = flags[x, at, :] != 0
            rho, mom = moments(g)
            hit = Collision(rho, mom, force_at(x, yb))
            put(0, x, yb * 8, jnp.where(solid, g[0], KEEP * g[0] + hit.base))
            for k in range(1, 19, 2):
                even, odd = hit.terms(k)
                ahead = jnp.where(solid, g[k + 1], KEEP * g[k] + (even + odd))
                back = jnp.where(solid, g[k], KEEP * g[k + 1] + (even - odd))
                put(k, x, yb * 8, ahead)
                put(k + 1, x, yb * 8, back)
                if DIRS[k][2] != 0:
                    up, down = (k, k + 1) if DIRS[k][2] == 1 else (k + 1, k)
                    rising, falling = (ahead, back) if up == k else (back, ahead)
                    rows = pl.ds(OY + yb * 8, 8)
                    pltpu.store(out.at[up, x - low + 1, rows, :], falling, mask=first)
                    pltpu.store(out.at[down, x - low + 1, rows, :], rising, mask=last)

        @pl.when(x > low)
        def _():
            send(x - 1).start()

        return carry

    lax.fori_loop(low, high, plane, 0)
    send(high - 1).start()
    for x in range(low, high):
        send(x).wait()


def exchanged(block, source):
    count_x, count_y = lax.axis_size("gx"), lax.axis_size("gy")
    pairs = []
    for x in range(count_x):
        for y in range(count_y):
            from_x, from_y = source(x, y)
            pairs.append(((from_x % count_x) * count_y + from_y % count_y, x * count_y + y))
    return lax.ppermute(block, ("gx", "gy"), pairs)


def swapped(block):
    return exchanged(block, lambda x, y: (x, y ^ 1))


def along_z(block, distance):
    def source(x, y):
        return x + 4 * distance * (1 if (x // 4 + y) % 2 == 0 else -1), y

    return exchanged(block, source)


def cost(flops):
    return pl.CostEstimate(flops=flops, bytes_accessed=0, transcendentals=0)


def local(populations, solid_flags, point_cells, point_turbine, blade_speed, chord, turbine_gain):
    points = point_cells.shape[1]
    total_x = CX * lax.axis_size("gx")
    total_y = CY * lax.axis_size("gy")
    sds = jax.ShapeDtypeStruct
    params = pltpu.CompilerParams(vmem_limit_bytes=24 * 1024 * 1024)
    light = pltpu.CompilerParams(vmem_limit_bytes=4 * 1024 * 1024)
    compact = [
        pltpu.VMEM((CHUNK, points), BF16),
        pltpu.VMEM((16, points), F32),
        pltpu.VMEM((LANES, LANES), F32),
        pltpu.VMEM((LANES, LANES), F32),
    ]
    sibling, across, paired, unpaired, held_pops = pl.pallas_call(
        sample_kernel,
        out_shape=(
            sds((192, LANES), F32),
            sds((192, LANES), F32),
            sds((10, CY, LANES), F32),
            sds((10, CY, LANES), F32),
            sds(populations.shape, F32),
        ),
        in_specs=[HBM] * 7,
        out_specs=(VMEM,) * 5,
        scratch_shapes=[
            pltpu.VMEM((3 * CX * CY, 2 * LANES), BF16),
            pltpu.VMEM((3 * CX * CY, LANES), BF16),
            *compact,
            pltpu.VMEM((16, CHUNK), F32),
            pltpu.SMEM(turbine_gain.shape, F32),
            pltpu.VMEM(solid_flags.shape, jnp.int32),
            pltpu.VMEM((3, points), jnp.int32),
            pltpu.VMEM((1, points), jnp.int32),
            pltpu.VMEM((1, points), F32),
            pltpu.VMEM((3, points), F32),
            pltpu.SemaphoreType.DMA((CX,)),
            pltpu.SemaphoreType.DMA((6,)),
        ],
        compiler_params=params,
        name="sample",
    )(
        *[
            pltpu.with_memory_space_constraint(arg, pltpu.HBM)
            for arg in (
                turbine_gain, populations, solid_flags, point_cells, point_turbine, chord,
                blade_speed,
            )
        ]
    )
    beside = swapped(sibling)
    beyond = exchanged(across, lambda x, y: (x, y + 1 if y % 2 else y - 1))
    paired = exchanged(paired, lambda x, y: (x ^ 1, y))
    unpaired = exchanged(unpaired, lambda x, y: (x + 1 if x % 2 else x - 1, y))
    joined = pl.pallas_call(
        join_kernel,
        out_shape=sds((136, LANES), F32),
        in_specs=[VMEM] * 3,
        out_specs=VMEM,
        compiler_params=light,
        name="join",
    )(sibling, beside, beyond)
    pair_pts = exchanged(joined, lambda x, y: (x ^ 1, y))
    other_pts = exchanged(joined, lambda x, y: (x + 1 if x % 2 else x - 1, y))
    other_half = exchanged(joined, lambda x, y: (x, y + 4))
    near = known(joined[:112], known(pair_pts[:112], other_pts[:112]))
    prepared = pl.pallas_call(
        functools.partial(prep_kernel, total_x=total_x, total_y=total_y),
        out_shape=(
            sds((READY + 1, 8, CHUNK), F32),
            sds((LANES, LANES), F32),
            sds((8, points), F32),
        ),
        in_specs=[VMEM],
        out_specs=(VMEM, VMEM, VMEM),
        scratch_shapes=[pltpu.VMEM((CHUNK, points), BF16), pltpu.VMEM((LANES, LANES), F32)],
        compiler_params=params,
        cost_estimate=cost(FORCE_FLOPS),
        name="prep",
    )(point_cells)
    force = pl.pallas_call(
        force_kernel,
        out_shape=sds((3, CX + 2, FY, LANES), F32),
        in_specs=[VMEM] * 4,
        out_specs=VMEM,
        scratch_shapes=[pltpu.VMEM((CHUNK, points), BF16), pltpu.VMEM((8, CHUNK), F32)],
        compiler_params=params,
        cost_estimate=cost(FORCE_FLOPS),
        name="force",
    )(*prepared, near)
    step_args = (held_pops, solid_flags, force)
    rest_args = (beside, beyond, pair_pts, other_pts)
    read = None
    for low, high in ((1, CX // 2 + 1), (CX // 2 + 1, CX), (0, 1)):
        extra = () if read is None else (read,)
        halos = (paired, unpaired) if low == 0 or high == CX else (pair_pts, other_pts)
        read = pl.pallas_call(
            functools.partial(step_kernel, low=low, high=high),
            out_shape=sds(populations.shape, F32),
            in_specs=[VMEM] * 9 + [HBM] * len(extra),
            out_specs=HBM,
            scratch_shapes=[
                pltpu.VMEM((19, high - low + 2, CY + 16, LANES), F32),
                pltpu.SemaphoreType.DMA((CX,)),
            ],
            input_output_aliases={9: 0} if extra else {},
            compiler_params=params,
            cost_estimate=cost(STEP_FLOPS),
        )(*step_args, *halos, *rest_args, *extra)
    have = known(near, other_half[:112])
    got = swapped(have)
    have = known(have, got)
    got = along_z(have, 1)
    have = known(have, got)
    got = swapped(have)
    have = known(have, got)
    got = along_z(have, 3)
    have = known(have, got)
    have = known(have, swapped(have))
    got = exchanged(
        have, lambda x, y: (x // 4 * 4 + (x + 2) % 4, y) if y % 2 else (x, y + 4)
    )
    have = known(have, got)
    last = swapped(have)
    point_force = pl.pallas_call(
        finish_kernel,
        out_shape=sds((3, points), F32),
        in_specs=[VMEM] * 2,
        out_specs=VMEM,
        compiler_params=light,
        name="finish",
    )(have, last)
    return read, point_force


def solution(mesh):
    in_specs = (P(None, "gx", "gy", None), P("gx", "gy", None), P(), P(), P(), P(), P())
    out_specs = (P(None, "gx", "gy", None), P())
    return jax.shard_map(local, mesh=mesh, in_specs=in_specs, out_specs=out_specs, check_vma=False)
```
